32 devices in a mesh: gp: 32 (over z, y, x, core).
Axes of the slice: x: 2, y: 2, z: 4, core: 2. Of those that a mesh axis runs over, the one named last changes fastest.
Arguments:
- features: bfloat16 [65536, 128], P('gp')
- labels: int32 [65536], P('gp')
- train_mask: float32 [65536], P('gp')
- send_idx: int32 [1024, 512], P('gp')
- src_idx: int32 [196608], P('gp')
- dst_idx: int32 [196608], P('gp')
- inv_deg: float32 [65536], P('gp')
- w_self_1: bfloat16 [128, 256], replicated
- w_neigh_1: bfloat16 [128, 256], replicated
- bias_1: float32 [256], replicated
- w_self_2: bfloat16 [256, 256], replicated
- w_neigh_2: bfloat16 [256, 256], replicated
- bias_2: float32 [256], replicated
- w_self_3: bfloat16 [256, 40], replicated
- w_neigh_3: bfloat16 [256, 40], replicated
- bias_3: float32 [40], replicated
Outputs:
- output 1: float32 [], replicated
- output 2: float32 [128, 256], replicated
- output 3: float32 [128, 256], replicated
- output 4: float32 [256], replicated
- output 5: float32 [256, 256], replicated
- output 6: float32 [256, 256], replicated
- output 7: float32 [256], replicated
- output 8: float32 [256, 40], replicated
- output 9: float32 [256, 40], replicated
- output 10: float32 [40], replicated
All inputs are finite; a program needn't handle non-finite values.
Results may differ from the reference program's by a relative error of at most 0.0106418.
Values are sent between devices in bfloat16 or wider.
A program may use at most 1 GiB of HBM per device.

```python
import jax
import jax.numpy as jnp
from jax import lax

GROUP = 32
N_DEV = 2048
HALO_DEV = 16384
DEG = 3
F_IN = 128
HIDDEN = 256
CLASSES = 40
SEND = HALO_DEV // GROUP
EDGES = N_DEV * DEG
NODES = GROUP * N_DEV
TABLE_ROWS = N_DEV + HALO_DEV


def draw_graph(key):
    keys = jax.random.split(key, 8)
    send_idx = jax.random.randint(keys[0], (GROUP * GROUP, SEND), 0, N_DEV, jnp.int32)
    hub_weight = jax.random.randint(keys[1], (GROUP, 1), 1, 5, jnp.int32)
    counts = jax.random.randint(keys[2], (GROUP, GROUP), 1, SEND + 1, jnp.int32)
    counts = jnp.clip((counts * hub_weight) // 4, 1, SEND)
    dst_idx = jnp.sort(jax.random.randint(keys[3], (GROUP, EDGES), 0, N_DEV, jnp.int32), axis=1)
    from_halo = jax.random.randint(keys[4], (GROUP, EDGES), 0, 2, jnp.int32)
    local_src = jax.random.randint(keys[5], (GROUP, EDGES), 0, N_DEV, jnp.int32)
    owner = jnp.arange(GROUP, dtype=jnp.int32)[:, None]
    peer = (owner + 1 + jax.random.randint(keys[6], (GROUP, EDGES), 0, GROUP - 1, jnp.int32)) % GROUP
    slot = jax.random.randint(keys[7], (GROUP, EDGES), 0, counts[peer, owner], jnp.int32)
    src_idx = jnp.where(from_halo == 1, N_DEV + peer * SEND + slot, local_src)
    ones_row = jnp.ones((EDGES,), jnp.float32)
    degree = jax.vmap(lambda dst_row: jax.ops.segment_sum(ones_row, dst_row, num_segments=N_DEV))(dst_idx)
    inv_deg = 1.0 / jnp.maximum(degree, 1.0)
    return send_idx, src_idx.reshape(-1), dst_idx.reshape(-1), inv_deg.reshape(-1)


def draw_weight(key, fan_in, fan_out):
    normal = jax.random.normal(key, (fan_in, fan_out), jnp.float32)
    return (normal * fan_in ** -0.5).astype(jnp.bfloat16)


def setup_inputs(seed: int = 0) -> dict:
    keys = jax.random.split(jax.random.key(seed), 13)
    send_idx, src_idx, dst_idx, inv_deg = draw_graph(keys[0])
    return {
        'features': jax.random.normal(keys[1], (NODES, F_IN), jnp.float32).astype(jnp.bfloat16),
        'labels': jax.random.randint(keys[2], (NODES,), 0, CLASSES, jnp.int32),
        'train_mask': jax.random.randint(keys[3], (NODES,), 0, 2, jnp.int32).astype(jnp.float32),
        'send_idx': send_idx,
        'src_idx': src_idx,
        'dst_idx': dst_idx,
        'inv_deg': inv_deg,
        'w_self_1': draw_weight(keys[4], F_IN, HIDDEN),
        'w_neigh_1': draw_weight(keys[5], F_IN, HIDDEN),
        'bias_1': 0.5 * jax.random.normal(keys[6], (HIDDEN,), jnp.float32),
        'w_self_2': draw_weight(keys[7], HIDDEN, HIDDEN),
        'w_neigh_2': draw_weight(keys[8], HIDDEN, HIDDEN),
        'bias_2': 0.5 * jax.random.normal(keys[9], (HIDDEN,), jnp.float32),
        'w_self_3': draw_weight(keys[10], HIDDEN, CLASSES),
        'w_neigh_3': draw_weight(keys[11], HIDDEN, CLASSES),
        'bias_3': 0.5 * jax.random.normal(keys[12], (CLASSES,), jnp.float32),
    }


def reference(features, labels, train_mask, send_idx, src_idx, dst_idx, inv_deg,
              w_self_1, w_neigh_1, bias_1, w_self_2, w_neigh_2, bias_2,
              w_self_3, w_neigh_3, bias_3):
    base = jnp.arange(GROUP, dtype=jnp.int32) * N_DEV
    halo_global = (send_idx.reshape(GROUP, GROUP, SEND) + base[:, None, None]).transpose(1, 0, 2).reshape(-1)
    src_groups = src_idx.reshape(GROUP, EDGES)
    dst_groups = dst_idx.reshape(GROUP, EDGES)
    inv_groups = inv_deg.reshape(GROUP, N_DEV, 1)

    def aggregate(hidden):
        width = hidden.shape[1]
        halo = hidden[halo_global].reshape(GROUP, HALO_DEV, width)

        def one_group(pieces):
            own_rows, halo_rows, src_row, dst_row, inv_row = pieces
            table = jnp.concatenate([own_rows, halo_rows], axis=0)
            summed = jax.ops.segment_sum(table[src_row].astype(jnp.float32), dst_row, num_segments=N_DEV)
            return (summed * inv_row).astype(jnp.bfloat16)

        pieces = (hidden.reshape(GROUP, N_DEV, width), halo, src_groups, dst_groups, inv_groups)
        return lax.map(one_group, pieces).reshape(NODES, width)

    def layer(hidden, w_self, w_neigh, bias):
        neigh_mean = aggregate(hidden)
        return (jnp.dot(hidden, w_self, preferred_element_type=jnp.float32)
                + jnp.dot(neigh_mean, w_neigh, preferred_element_type=jnp.float32) + bias)

    def loss_of(params):
        hidden_1 = jax.nn.relu(layer(features, params[0], params[1], params[2])).astype(jnp.bfloat16)
        hidden_2 = jax.nn.relu(layer(hidden_1, params[3], params[4], params[5])).astype(jnp.bfloat16)
        logits = layer(hidden_2, params[6], params[7], params[8])
        log_prob = jax.nn.log_softmax(logits, axis=-1)
        picked = jnp.take_along_axis(log_prob, labels[:, None], axis=1)[:, 0]
        return jnp.sum(train_mask * -picked) / jnp.sum(train_mask)

    params = (w_self_1, w_neigh_1, bias_1, w_self_2, w_neigh_2, bias_2, w_self_3, w_neigh_3, bias_3)
    loss, grads = jax.value_and_grad(loss_of)(params)
    return (loss,
            grads[0].astype(jnp.float32), grads[1].astype(jnp.float32), grads[2].astype(jnp.float32),
            grads[3].astype(jnp.float32), grads[4].astype(jnp.float32), grads[5].astype(jnp.float32),
            grads[6].astype(jnp.float32), grads[7].astype(jnp.float32), grads[8].astype(jnp.float32))
```

```python
import functools

import jax
import jax.numpy as jnp
from jax import lax
from jax.experimental import pallas as pl
from jax.experimental.pallas import tpu as pltpu
from jax.sharding import PartitionSpec as P

GROUP_AXIS = 'gp'
LANES = 128
DST_TILE = 256
CHUNK = 256
COLS = 512
BATCH = 8
VMEM_BYTES = 60 * 1024 * 1024
F32 = jnp.float32
BF16 = jnp.bfloat16


def as_columns(row):
    return jnp.broadcast_to(row, (LANES, LANES)).T


def adjacency_kernel(n_own, starts, parts, dst_ref, col_ref, own_ref, rec_ref, acc):
    part, tile = parts[0], pl.program_id(0)
    lo, hi = starts[tile], starts[tile + 1]
    own_blocks = n_own // COLS
    n_recv = rec_ref.shape[1]
    blocks = own_blocks + n_recv // COLS
    dst_iota = lax.broadcasted_iota(jnp.int32, (DST_TILE, CHUNK), 0) + tile * DST_TILE
    lane_iota = lax.broadcasted_iota(jnp.int32, (LANES, LANES), 1)
    lanes = jnp.concatenate([lane_iota] * (CHUNK // LANES), axis=0)

    def clear(b, carry):
        acc[b] = jnp.zeros((DST_TILE, COLS), F32)
        return carry

    lax.fori_loop(0, blocks, clear, 0)

    def chunk_step(c, carry):
        to_dst = (dst_iota == dst_ref[pl.ds(c, 1), :]).astype(BF16)
        row = col_ref[pl.ds(c, 1), :]
        row = jnp.where(row < n_own, row, jnp.where(
            (row >= n_own + part * n_recv) & (row < n_own + (part + 1) * n_recv), row - part * n_recv, -1))
        columns = jnp.concatenate(
            [as_columns(row[:, k * LANES:(k + 1) * LANES]) for k in range(CHUNK // LANES)], axis=0)

        def block_step(b, carry):
            shifted = columns - b * COLS
            hot = jnp.concatenate([(shifted == lanes + j * LANES).astype(BF16) for j in range(COLS // LANES)], axis=1)
            acc[b] += jnp.dot(to_dst, hot, preferred_element_type=F32)
            return carry

        return lax.fori_loop(0, blocks, block_step, carry)

    lax.fori_loop(lax.div(lo, CHUNK), lax.div(hi + CHUNK - 1, CHUNK), chunk_step, 0)
    for b in range(own_blocks):
        own_ref[:, b * COLS:(b + 1) * COLS] = acc[b].astype(BF16)
    for b in range(n_recv // COLS):
        rec_ref[:, b * COLS:(b + 1) * COLS] = acc[own_blocks + b].astype(BF16)


def adjacency(part, starts, dst_idx, columns, n_own, n_recv):
    edges = dst_idx.shape[0]
    grid_spec = pltpu.PrefetchScalarGridSpec(
        num_scalar_prefetch=2, grid=(n_own // DST_TILE,),
        in_specs=[pl.BlockSpec((edges // CHUNK, CHUNK), lambda i, *_: (0, 0))] * 2,
        out_specs=[pl.BlockSpec((DST_TILE, n_own), lambda i, *_: (i, 0)),
                   pl.BlockSpec((DST_TILE, n_recv), lambda i, *_: (i, 0))],
        scratch_shapes=[pltpu.VMEM(((n_own + n_recv) // COLS, DST_TILE, COLS), F32)])
    return pl.pallas_call(
        functools.partial(adjacency_kernel, n_own), grid_spec=grid_spec,
        out_shape=[jax.ShapeDtypeStruct((n_own, n_own), BF16), jax.ShapeDtypeStruct((n_own, n_recv), BF16)],
        compiler_params=pltpu.CompilerParams(vmem_limit_bytes=VMEM_BYTES),
        cost_estimate=pl.CostEstimate(flops=30 * 10**9, bytes_accessed=40 * 10**6, transcendentals=0),
        name='adjacency',
    )(starts, jnp.reshape(part, (1,)).astype(jnp.int32), dst_idx.reshape(-1, CHUNK), columns.reshape(-1, CHUNK))


def pick_kernel(list_ref, rows_ref, out_ref):
    n_rows = rows_ref.shape[0]
    lane_iota = lax.broadcasted_iota(jnp.int32, (LANES, LANES), 1)

    def hot(row):
        columns = as_columns(row)
        return jnp.concatenate(
            [(columns == lane_iota + j * LANES).astype(BF16) for j in range(n_rows // LANES)], axis=1)

    all_hot = jnp.concatenate([hot(list_ref[b:b + 1, :]) for b in range(BATCH)], axis=0)
    picked = jnp.dot(all_hot, rows_ref[...], preferred_element_type=F32).astype(BF16)
    for b in range(BATCH):
        out_ref[b] = picked[b * LANES:(b + 1) * LANES]


def pick(lists, rows):
    group, _ = lists.shape
    n_rows, width = rows.shape
    return pl.pallas_call(
        pick_kernel, grid=(group // BATCH,),
        in_specs=[pl.BlockSpec((BATCH, LANES), lambda i: (i, 0)),
                  pl.BlockSpec((n_rows, width), lambda i: (0, 0))],
        out_specs=pl.BlockSpec((BATCH, LANES, width), lambda i: (i, 0, 0)),
        out_shape=jax.ShapeDtypeStruct((group, LANES, width), BF16),
        compiler_params=pltpu.CompilerParams(vmem_limit_bytes=VMEM_BYTES),
        cost_estimate=pl.CostEstimate(flops=2 * group * LANES * n_rows * width, bytes_accessed=4 * 10**6,
                                      transcendentals=0),
        name='pick',
    )(lists, rows)


def put_back_kernel(list_ref, sent_ref, add_ref, out_ref):
    n_rows = out_ref.shape[0]
    row_iota = lax.broadcasted_iota(jnp.int32, (n_rows, LANES), 0)

    @pl.when(pl.program_id(0) == 0)
    def _():
        out_ref[...] = add_ref[...]

    hot = jnp.concatenate([(row_iota == list_ref[b:b + 1, :]).astype(BF16) for b in range(BATCH)], axis=1)
    rows = jnp.concatenate([sent_ref[b] for b in range(BATCH)], axis=0)
    out_ref[...] += jnp.dot(hot, rows, preferred_element_type=F32)


def put_back(lists, sent, add):
    group, _ = lists.shape
    n_rows, width = add.shape
    return pl.pallas_call(
        put_back_kernel, grid=(group // BATCH,),
        in_specs=[pl.BlockSpec((BATCH, LANES), lambda i: (i, 0)),
                  pl.BlockSpec((BATCH, LANES, width), lambda i: (i, 0, 0)),
                  pl.BlockSpec((n_rows, width), lambda i: (0, 0))],
        out_specs=pl.BlockSpec((n_rows, width), lambda i: (0, 0)),
        out_shape=jax.ShapeDtypeStruct((n_rows, width), F32),
        compiler_params=pltpu.CompilerParams(vmem_limit_bytes=VMEM_BYTES),
        cost_estimate=pl.CostEstimate(flops=2 * group * LANES * n_rows * width, bytes_accessed=8 * 10**6,
                                      transcendentals=0),
        name='put_back',
    )(lists, sent, add)


def gather_in_kernel(adj_ref, rows_ref, add_ref, out_ref):
    out_ref[...] = add_ref[...] + jnp.dot(adj_ref[...], rows_ref[...], preferred_element_type=F32)


def gather_in(adj_rec, rows, add):
    n_own, n_recv = adj_rec.shape
    width = rows.shape[1]
    return pl.pallas_call(
        gather_in_kernel, grid=(n_own // DST_TILE,),
        in_specs=[pl.BlockSpec((DST_TILE, n_recv), lambda i: (i, 0)),
                  pl.BlockSpec((n_recv, width), lambda i: (0, 0)),
                  pl.BlockSpec((DST_TILE, width), lambda i: (i, 0))],
        out_specs=pl.BlockSpec((DST_TILE, width), lambda i: (i, 0)),
        out_shape=jax.ShapeDtypeStruct((n_own, width), F32),
        compiler_params=pltpu.CompilerParams(vmem_limit_bytes=VMEM_BYTES),
        cost_estimate=pl.CostEstimate(flops=2 * n_own * n_recv * width, bytes_accessed=20 * 10**6, transcendentals=0),
        name='gather_in',
    )(adj_rec, rows, add)


def spread_out_kernel(adj_ref, rows_ref, out_ref):
    out_ref[...] = lax.dot_general(adj_ref[...], rows_ref[...], (((0,), (0,)), ((), ())),
                                   preferred_element_type=F32).astype(BF16)


def spread_out(adj_rec, rows):
    n_own, n_recv = adj_rec.shape
    width = rows.shape[1]
    return pl.pallas_call(
        spread_out_kernel, grid=(n_recv // COLS,),
        in_specs=[pl.BlockSpec((n_own, COLS), lambda i: (0, i)),
                  pl.BlockSpec((n_own, width), lambda i: (0, 0))],
        out_specs=pl.BlockSpec((COLS, width), lambda i: (i, 0)),
        out_shape=jax.ShapeDtypeStruct((n_recv, width), BF16),
        compiler_params=pltpu.CompilerParams(vmem_limit_bytes=VMEM_BYTES),
        cost_estimate=pl.CostEstimate(flops=2 * n_own * n_recv * width, bytes_accessed=20 * 10**6, transcendentals=0),
        name='spread_out',
    )(adj_rec, rows)


def before(count):
    index = jnp.arange(count, dtype=jnp.int32)
    return index[:, None] < index[None, :]


def rank_in_row(flags):
    tri = before(flags.shape[1]).astype(BF16)
    return jnp.dot(flags.astype(BF16), tri, preferred_element_type=F32).astype(jnp.int32)


def exchange_plan(send_idx, src_idx, n_own):
    group, slots = send_idx.shape
    halo = src_idx - n_own
    peer, slot = halo // slots, halo % slots
    from_peer = ((halo >= 0)[:, None] & (peer[:, None] == jnp.arange(group, dtype=jnp.int32)[None, :])).astype(BF16)
    at_slot = (slot[:, None] == jnp.arange(slots, dtype=jnp.int32)[None, :]).astype(BF16)
    needed = jnp.einsum('eg,es->gs', from_peer, at_slot, preferred_element_type=F32) > 0
    rank = rank_in_row(needed)
    my_rounds = (jnp.max(jnp.where(needed, rank, 0)) // LANES + 1).astype(jnp.int32)
    upper = rank // LANES * group + jnp.arange(group, dtype=jnp.int32)[:, None]
    split = jnp.concatenate([upper, rank % LANES], axis=1).astype(BF16)
    found = jnp.dot(from_peer, split, preferred_element_type=F32)
    found = jnp.sum((found[:, :slots] * LANES + found[:, slots:]) * at_slot.astype(F32), axis=1).astype(jnp.int32)
    columns = jnp.where(halo >= 0, n_own + found, src_idx)
    message = jnp.concatenate([jnp.where(needed, rank, -1), jnp.full((group, LANES), my_rounds)], axis=1)
    message = lax.all_to_all(message, GROUP_AXIS, 0, 0, tiled=True)
    asked, rounds = message[:, :slots], jnp.max(message[:, slots])
    k = jnp.arange(slots, dtype=jnp.int32)
    chosen = asked[:, None, :] == k[None, :, None]
    lists = jnp.sum(jnp.where(chosen, send_idx[:, None, :] + 1, 0), axis=2) - 1
    return columns, rounds, lists.reshape(group, slots // LANES, LANES).transpose(1, 0, 2)


def weight_grads(h_in, neigh_mean, d_pre, d_pre_bf):
    g_self = jnp.einsum('nd,ne->de', h_in, d_pre_bf, preferred_element_type=jnp.float32)
    g_neigh = jnp.einsum('nd,ne->de', neigh_mean, d_pre_bf, preferred_element_type=jnp.float32)
    return g_self, g_neigh, jnp.sum(d_pre, axis=0)


def input_grads(d_pre_bf, w_self, w_neigh):
    d_self = jnp.einsum('ne,de->nd', d_pre_bf, w_self, preferred_element_type=jnp.float32)
    d_mean = jnp.einsum('ne,de->nd', d_pre_bf, w_neigh, preferred_element_type=jnp.float32)
    return d_self, d_mean


def head_grad(logits, labels, train_mask):
    log_prob = jax.nn.log_softmax(logits, axis=-1)
    is_label = labels[:, None] == jnp.arange(logits.shape[1], dtype=jnp.int32)[None, :]
    picked = jnp.sum(jnp.where(is_label, log_prob, 0.0), axis=-1)
    d_logits = (jnp.exp(log_prob) - is_label.astype(jnp.float32)) * train_mask[:, None]
    return jnp.sum(train_mask * -picked), d_logits


def solution(mesh):
    def device_step(features, labels, train_mask, send_idx, src_idx, dst_idx, inv_deg,
                    w_self_1, w_neigh_1, bias_1, w_self_2, w_neigh_2, bias_2,
                    w_self_3, w_neigh_3, bias_3):
        n_own = features.shape[0]
        group, slots = send_idx.shape
        columns, rounds, lists = exchange_plan(send_idx, src_idx, n_own)
        n_recv = group * LANES
        starts = jnp.sum(dst_idx[None, :] < (jnp.arange(n_own // DST_TILE + 1) * DST_TILE)[:, None],
                         axis=1, dtype=jnp.int32)

        def adjacency_of(part):
            return adjacency(part, starts, dst_idx, columns, n_own, n_recv)

        adj_own, adj_first = adjacency_of(0)

        def swap(rows):
            return lax.all_to_all(rows, GROUP_AXIS, 0, 0, tiled=True)

        def aggregate(hidden):
            def one_round(part, adj_rec, total):
                received = swap(pick(lists[part], hidden))
                return gather_in(adj_rec, received.reshape(n_recv, -1), total)

            summed = one_round(0, adj_first, jnp.dot(adj_own, hidden, preferred_element_type=F32))
            summed = lax.fori_loop(1, rounds, lambda part, total: one_round(part, adjacency_of(part)[1], total), summed)
            return (summed * inv_deg[:, None]).astype(BF16)

        def layer(hidden, w_self, w_neigh, bias):
            neigh_mean = aggregate(hidden)
            pre_act = (jnp.dot(hidden, w_self, preferred_element_type=jnp.float32)
                       + jnp.dot(neigh_mean, w_neigh, preferred_element_type=jnp.float32) + bias)
            return neigh_mean, pre_act

        def back_to_owners(d_mean, d_self):
            d_sum = (d_mean * inv_deg[:, None]).astype(BF16)

            def one_round(part, adj_rec, total):
                returned = swap(spread_out(adj_rec, d_sum).reshape(group, LANES, -1))
                return put_back(lists[part], returned, total)

            d_own = d_self + jnp.einsum('nt,nd->td', adj_own, d_sum, preferred_element_type=F32)
            return lax.fori_loop(1, rounds, lambda part, total: one_round(part, adjacency_of(part)[1], total),
                                 one_round(0, adj_first, d_own))

        mean_1, pre_1 = layer(features, w_self_1, w_neigh_1, bias_1)
        hidden_1 = jax.nn.relu(pre_1).astype(jnp.bfloat16)
        mean_2, pre_2 = layer(hidden_1, w_self_2, w_neigh_2, bias_2)
        hidden_2 = jax.nn.relu(pre_2).astype(jnp.bfloat16)
        mean_3, logits = layer(hidden_2, w_self_3, w_neigh_3, bias_3)
        loss_sum, d_logits = head_grad(logits, labels, train_mask)
        totals = lax.psum(jnp.stack([loss_sum, jnp.sum(train_mask)]), GROUP_AXIS)

        d_pre_3 = d_logits / totals[1]
        d_bf_3 = d_pre_3.astype(jnp.bfloat16)
        g_self_3, g_neigh_3, g_bias_3 = weight_grads(hidden_2, mean_3, d_pre_3, d_bf_3)
        d_self_3, d_mean_3 = input_grads(d_bf_3, w_self_3, w_neigh_3)
        d_pre_2 = jnp.where(pre_2 > 0, back_to_owners(d_mean_3, d_self_3), 0.0)
        d_bf_2 = d_pre_2.astype(jnp.bfloat16)
        g_self_2, g_neigh_2, g_bias_2 = weight_grads(hidden_1, mean_2, d_pre_2, d_bf_2)
        d_self_2, d_mean_2 = input_grads(d_bf_2, w_self_2, w_neigh_2)
        d_pre_1 = jnp.where(pre_1 > 0, back_to_owners(d_mean_2, d_self_2), 0.0)
        d_bf_1 = d_pre_1.astype(jnp.bfloat16)
        g_self_1, g_neigh_1, g_bias_1 = weight_grads(features, mean_1, d_pre_1, d_bf_1)

        grads = lax.psum((g_self_1, g_neigh_1, g_bias_1, g_self_2, g_neigh_2, g_bias_2,
                          g_self_3, g_neigh_3, g_bias_3), GROUP_AXIS)
        return (totals[0] / totals[1],) + tuple(grads)

    sharded = P(GROUP_AXIS)
    whole = P()
    return jax.shard_map(device_step, mesh=mesh,
                         in_specs=(sharded,) * 7 + (whole,) * 9,
                         out_specs=(whole,) * 10, check_vma=False)
```

```python
import functools

import jax
import jax.numpy as jnp
from jax import lax
from jax.experimental import pallas as pl
from jax.experimental.pallas import tpu as pltpu
from jax.sharding import PartitionSpec as P

GROUP_AXIS = 'gp'
LANES = 128
DST_TILE = 256
WINDOW = 8
COLS = 512
BATCH = 8
VMEM_BYTES = 60 * 1024 * 1024
MESH = pl.DeviceIdType.MESH
F32 = jnp.float32
IDX = jnp.int16
BF16 = jnp.bfloat16


def as_columns(row):
    return jnp.broadcast_to(row, (LANES, LANES)).T


def adjacency_kernel(n_own, starts, parts, dst_ref, col_ref, own_ref, rec_ref):
    part, tile = parts[0], pl.program_id(0)
    first = lax.div(starts[tile], LANES)
    last = lax.div(starts[tile + 1] + LANES - 1, LANES)
    n_recv = rec_ref.shape[1]
    dst_iota = lax.broadcasted_iota(jnp.int32, (DST_TILE, LANES), 0) + tile * DST_TILE
    lanes = lax.broadcasted_iota(jnp.int32, (WINDOW * LANES, LANES), 1).astype(IDX)

    def window_step(w, carry):
        rows = first + w * WINDOW
        dst = dst_ref[pl.ds(rows, WINDOW), :]
        col = col_ref[pl.ds(rows, WINDOW), :]
        mine = (col >= n_own + part * n_recv) & (col < n_own + (part + 1) * n_recv)
        col = jnp.where(col < n_own, col, jnp.where(mine, col - part * n_recv, -1))
        to_dst = jnp.concatenate([(dst_iota == dst[k:k + 1, :]).astype(BF16) for k in range(WINDOW)], axis=1)
        columns = jnp.concatenate([as_columns(col[k:k + 1, :]) for k in range(WINDOW)], axis=0).astype(IDX)

        def fill(out_ref, base):
            def block_step(b, carry):
                offset = pl.multiple_of(b * COLS, COLS)
                shifted = columns - (base + offset).astype(IDX)
                hot = jnp.concatenate([jnp.where(shifted == lanes + IDX(j * LANES), BF16(1), BF16(0))
                                       for j in range(COLS // LANES)], axis=1)
                counts = jnp.dot(to_dst, hot, preferred_element_type=F32)
                at = (slice(None), pl.ds(offset, COLS))

                @pl.when(w == 0)
                def _():
                    out_ref[at] = counts.astype(BF16)

                @pl.when(w > 0)
                def _():
                    out_ref[at] = (out_ref[at].astype(F32) + counts).astype(BF16)

                return carry

            lax.fori_loop(0, out_ref.shape[1] // COLS, block_step, 0)

        fill(own_ref, 0)
        fill(rec_ref, n_own)
        return carry

    windows = jnp.maximum(lax.div(last - first + WINDOW - 1, WINDOW), 1)
    lax.fori_loop(0, windows, window_step, 0)


def adjacency(part, starts, dst_idx, columns, n_own, n_recv):
    def rows_of(index):
        padding = jnp.full((WINDOW * LANES,), -1, jnp.int32)
        return jnp.concatenate([index, padding]).reshape(-1, LANES)

    rows = dst_idx.shape[0] // LANES + WINDOW
    grid_spec = pltpu.PrefetchScalarGridSpec(
        num_scalar_prefetch=2, grid=(n_own // DST_TILE,),
        in_specs=[pl.BlockSpec((rows, LANES), lambda i, *_: (0, 0))] * 2,
        out_specs=[pl.BlockSpec((DST_TILE, n_own), lambda i, *_: (i, 0)),
                   pl.BlockSpec((DST_TILE, n_recv), lambda i, *_: (i, 0))])
    return pl.pallas_call(
        functools.partial(adjacency_kernel, n_own), grid_spec=grid_spec,
        out_shape=[jax.ShapeDtypeStruct((n_own, n_own), BF16), jax.ShapeDtypeStruct((n_own, n_recv), BF16)],
        compiler_params=pltpu.CompilerParams(vmem_limit_bytes=VMEM_BYTES),
        cost_estimate=pl.CostEstimate(flops=30 * 10**9, bytes_accessed=40 * 10**6, transcendentals=0),
        name='adjacency',
    )(starts, jnp.reshape(part, (1,)).astype(jnp.int32), rows_of(dst_idx), rows_of(columns))


def pick_kernel(list_ref, rows_ref, out_ref):
    n_rows = rows_ref.shape[0]
    lane_iota = lax.broadcasted_iota(jnp.int32, (LANES, LANES), 1)

    def hot(row):
        columns = as_columns(row)
        return jnp.concatenate(
            [(columns == lane_iota + j * LANES).astype(BF16) for j in range(n_rows // LANES)], axis=1)

    all_hot = jnp.concatenate([hot(list_ref[b:b + 1, :]) for b in range(BATCH)], axis=0)
    picked = jnp.dot(all_hot, rows_ref[...], preferred_element_type=F32).astype(BF16)
    for b in range(BATCH):
        out_ref[b] = picked[b * LANES:(b + 1) * LANES]


def pick(lists, rows):
    group, _ = lists.shape
    n_rows, width = rows.shape
    return pl.pallas_call(
        pick_kernel, grid=(group // BATCH,),
        in_specs=[pl.BlockSpec((BATCH, LANES), lambda i: (i, 0)),
                  pl.BlockSpec((n_rows, width), lambda i: (0, 0))],
        out_specs=pl.BlockSpec((BATCH, LANES, width), lambda i: (i, 0, 0)),
        out_shape=jax.ShapeDtypeStruct((group, LANES, width), BF16),
        compiler_params=pltpu.CompilerParams(vmem_limit_bytes=VMEM_BYTES),
        cost_estimate=pl.CostEstimate(flops=2 * group * LANES * n_rows * width, bytes_accessed=4 * 10**6,
                                      transcendentals=0),
        name='pick',
    )(lists, rows)


def put_back_kernel(list_ref, sent_ref, add_ref, out_ref):
    n_rows = out_ref.shape[0]
    row_iota = lax.broadcasted_iota(jnp.int32, (n_rows, LANES), 0)

    @pl.when(pl.program_id(0) == 0)
    def _():
        out_ref[...] = add_ref[...]

    hot = jnp.concatenate([(row_iota == list_ref[b:b + 1, :]).astype(BF16) for b in range(BATCH)], axis=1)
    rows = jnp.concatenate([sent_ref[b] for b in range(BATCH)], axis=0)
    out_ref[...] += jnp.dot(hot, rows, preferred_element_type=F32)


def put_back(lists, sent, add):
    group, _ = lists.shape
    n_rows, width = add.shape
    return pl.pallas_call(
        put_back_kernel, grid=(group // BATCH,),
        in_specs=[pl.BlockSpec((BATCH, LANES), lambda i: (i, 0)),
                  pl.BlockSpec((BATCH, LANES, width), lambda i: (i, 0, 0)),
                  pl.BlockSpec((n_rows, width), lambda i: (0, 0))],
        out_specs=pl.BlockSpec((n_rows, width), lambda i: (0, 0)),
        out_shape=jax.ShapeDtypeStruct((n_rows, width), F32),
        compiler_params=pltpu.CompilerParams(vmem_limit_bytes=VMEM_BYTES),
        cost_estimate=pl.CostEstimate(flops=2 * group * LANES * n_rows * width, bytes_accessed=8 * 10**6,
                                      transcendentals=0),
        name='put_back',
    )(lists, sent, add)


def gather_in_kernel(adj_ref, rows_ref, add_ref, out_ref):
    out_ref[...] = add_ref[...] + jnp.dot(adj_ref[...], rows_ref[...], preferred_element_type=F32)


def gather_in(adj_rec, rows, add):
    n_own, n_recv = adj_rec.shape
    width = rows.shape[1]
    return pl.pallas_call(
        gather_in_kernel, grid=(n_own // DST_TILE,),
        in_specs=[pl.BlockSpec((DST_TILE, n_recv), lambda i: (i, 0)),
                  pl.BlockSpec((n_recv, width), lambda i: (0, 0)),
                  pl.BlockSpec((DST_TILE, width), lambda i: (i, 0))],
        out_specs=pl.BlockSpec((DST_TILE, width), lambda i: (i, 0)),
        out_shape=jax.ShapeDtypeStruct((n_own, width), F32),
        compiler_params=pltpu.CompilerParams(vmem_limit_bytes=VMEM_BYTES),
        cost_estimate=pl.CostEstimate(flops=2 * n_own * n_recv * width, bytes_accessed=20 * 10**6, transcendentals=0),
        name='gather_in',
    )(adj_rec, rows, add)


def spread_out_kernel(adj_ref, rows_ref, out_ref):
    out_ref[...] = lax.dot_general(adj_ref[...], rows_ref[...], (((0,), (0,)), ((), ())),
                                   preferred_element_type=F32).astype(BF16)


def spread_out(adj_rec, rows):
    n_own, n_recv = adj_rec.shape
    width = rows.shape[1]
    return pl.pallas_call(
        spread_out_kernel, grid=(n_recv // COLS,),
        in_specs=[pl.BlockSpec((n_own, COLS), lambda i: (0, i)),
                  pl.BlockSpec((n_own, width), lambda i: (0, 0))],
        out_specs=pl.BlockSpec((COLS, width), lambda i: (i, 0)),
        out_shape=jax.ShapeDtypeStruct((n_recv, width), BF16),
        compiler_params=pltpu.CompilerParams(vmem_limit_bytes=VMEM_BYTES),
        cost_estimate=pl.CostEstimate(flops=2 * n_own * n_recv * width, bytes_accessed=20 * 10**6, transcendentals=0),
        name='spread_out',
    )(adj_rec, rows)


def add_up_kernel(n_chips, rows, *refs):
    parts, (out_ref, packed, partner_half, mine, inbox, total, gathered, send, recv) = refs[:-9], refs[-9:]
    me = lax.axis_index(GROUP_AXIS)
    core, chip = lax.rem(me, 2), lax.div(me, 2)
    partner = me + 1 - 2 * core

    def twin(step):
        return 2 * lax.rem(chip + step, n_chips) + core

    barrier = pltpu.get_barrier_semaphore()
    pl.semaphore_signal(barrier, inc=1, device_id=(partner,), device_id_type=MESH)
    for step in range(1, n_chips):
        pl.semaphore_signal(barrier, inc=1, device_id=(twin(step),), device_id_type=MESH)

    at = 0
    for ref in parts:
        count, width = ref.shape
        for j in range(width // LANES):
            packed[at:at + count, :] = ref[:, j * LANES:(j + 1) * LANES]
            at += count
    packed[at:, :] = jnp.zeros((packed.shape[0] - at, LANES), F32)
    half = n_chips * rows

    def half_of(which):
        return pl.ds(pl.multiple_of(which * half, 8), half)

    def copy(src, dst, slot, device):
        return pltpu.make_async_remote_copy(
            src_ref=src, dst_ref=dst, send_sem=send.at[slot], recv_sem=recv.at[slot],
            device_id=(device,), device_id_type=MESH)

    pl.semaphore_wait(barrier, n_chips)
    first = copy(packed.at[half_of(1 - core)], partner_half, 0, partner)
    first.start()
    first.wait()
    mine[...] = (packed[half_of(core), :] + partner_half[...]).reshape(n_chips, rows, LANES)
    sends = []
    for step in range(1, n_chips):
        sends.append(copy(mine.at[lax.rem(chip + step, n_chips)], inbox.at[step], step, twin(step)))
        sends[-1].start()
    value = mine[chip]
    for step in range(1, n_chips):
        sends[step - 1].wait_recv()
        value = value + inbox[step]
    total[...] = value
    for item in sends:
        item.wait_send()
    spread = []
    for step in range(1, n_chips):
        spread.append(copy(total, gathered.at[core, chip], n_chips + step, twin(step)))
        spread[-1].start()
    gathered[core, chip] = value
    for item in spread:
        item.wait()
    last = copy(gathered.at[core], gathered.at[core], 2 * n_chips, partner)
    last.start()
    last.wait()
    out_ref[...] = gathered[...].reshape(2 * half, LANES)


def add_up(parts, group):
    n_chips = group // 2
    used = sum(p.size for p in parts) // LANES
    rows = -(-used // (group * 8)) * 8
    total = group * rows
    chunk = (rows, LANES)
    return pl.pallas_call(
        functools.partial(add_up_kernel, n_chips, rows),
        in_specs=[pl.BlockSpec(memory_space=pltpu.VMEM)] * len(parts),
        out_specs=pl.BlockSpec(memory_space=pltpu.VMEM),
        out_shape=jax.ShapeDtypeStruct((total, LANES), F32),
        scratch_shapes=[pltpu.VMEM((total, LANES), F32), pltpu.VMEM((total // 2, LANES), F32),
                        pltpu.VMEM((n_chips,) + chunk, F32), pltpu.VMEM((n_chips,) + chunk, F32),
                        pltpu.VMEM(chunk, F32), pltpu.VMEM((2, n_chips) + chunk, F32),
                        pltpu.SemaphoreType.DMA((2 * n_chips + 1,)), pltpu.SemaphoreType.DMA((2 * n_chips + 1,))],
        compiler_params=pltpu.CompilerParams(collective_id=0, has_side_effects=True),
        name='add_up',
    )(*parts)


def unpack_kernel(flipped, packed_ref, *out_refs):
    at = 0
    for ref, flip in zip(out_refs[:-1], flipped):
        count, width = ref.shape[::-1] if flip else ref.shape
        pieces = []
        for j in range(width // LANES):
            pieces.append(packed_ref[at:at + count, :])
            at += count
        if flip:
            short = jnp.zeros((LANES - count, LANES), F32)
            for j, piece in enumerate(pieces):
                ref[j * LANES:(j + 1) * LANES, :] = jnp.concatenate([piece, short], axis=0).T[:, :count]
        else:
            ref[...] = jnp.concatenate(pieces, axis=1)
    out_refs[-1][...] = packed_ref[at:at + out_refs[-1].shape[0], :]


def unpack(packed, shapes, flipped):
    return pl.pallas_call(
        functools.partial(unpack_kernel, flipped),
        in_specs=[pl.BlockSpec(memory_space=pltpu.VMEM)],
        out_specs=[pl.BlockSpec(memory_space=pltpu.VMEM)] * (len(shapes) + 1),
        out_shape=[jax.ShapeDtypeStruct(shape, F32) for shape in shapes + ((8, LANES),)],
        name='unpack',
    )(packed)


def before(count):
    index = jnp.arange(count, dtype=jnp.int32)
    return index[:, None] < index[None, :]


def rank_in_row(flags):
    tri = before(flags.shape[1]).astype(BF16)
    return jnp.dot(flags.astype(BF16), tri, preferred_element_type=F32).astype(jnp.int32)


def exchange_plan(send_idx, src_idx, train_mask, n_own):
    group, slots = send_idx.shape
    halo = src_idx - n_own
    peer, slot = halo // slots, halo % slots
    from_peer = ((halo >= 0)[:, None] & (peer[:, None] == jnp.arange(group, dtype=jnp.int32)[None, :])).astype(BF16)
    at_slot = (slot[:, None] == jnp.arange(slots, dtype=jnp.int32)[None, :]).astype(BF16)
    needed = jnp.einsum('eg,es->gs', from_peer, at_slot, preferred_element_type=F32) > 0
    rank = rank_in_row(needed)
    my_rounds = (jnp.max(jnp.where(needed, rank, 0)) // LANES + 1).astype(jnp.int32)
    upper = rank // LANES * group + jnp.arange(group, dtype=jnp.int32)[:, None]
    split = jnp.concatenate([upper, rank % LANES], axis=1).astype(BF16)
    found = jnp.dot(from_peer, split, preferred_element_type=F32)
    found = jnp.sum((found[:, :slots] * LANES + found[:, slots:]) * at_slot.astype(F32), axis=1).astype(jnp.int32)
    columns = jnp.where(halo >= 0, n_own + found, src_idx)
    my_count = jnp.sum(train_mask).astype(jnp.int32)
    extras = jnp.where(jnp.arange(LANES) == 0, my_rounds, my_count)
    message = jnp.concatenate([jnp.where(needed, rank, -1), jnp.broadcast_to(extras, (group, LANES))], axis=1)
    message = lax.all_to_all(message, GROUP_AXIS, 0, 0, tiled=True)
    asked, rounds = message[:, :slots], jnp.max(message[:, slots])
    count = jnp.sum(message[:, slots + 1]).astype(F32)
    k = jnp.arange(slots, dtype=jnp.int32)
    chosen = asked[:, None, :] == k[None, :, None]
    lists = jnp.sum(jnp.where(chosen, send_idx[:, None, :] + 1, 0), axis=2) - 1
    return columns, rounds, count, lists.reshape(group, slots // LANES, LANES).transpose(1, 0, 2)


def weight_grads(h_in, neigh_mean, d_pre, d_pre_bf):
    g_self = jnp.einsum('nd,ne->de', h_in, d_pre_bf, preferred_element_type=jnp.float32)
    g_neigh = jnp.einsum('nd,ne->de', neigh_mean, d_pre_bf, preferred_element_type=jnp.float32)
    return g_self, g_neigh, jnp.sum(d_pre, axis=0)


def input_grads(d_pre_bf, w_self, w_neigh):
    d_self = jnp.einsum('ne,de->nd', d_pre_bf, w_self, preferred_element_type=jnp.float32)
    d_mean = jnp.einsum('ne,de->nd', d_pre_bf, w_neigh, preferred_element_type=jnp.float32)
    return d_self, d_mean


def head_grad(logits, labels, train_mask):
    log_prob = jax.nn.log_softmax(logits, axis=-1)
    is_label = labels[:, None] == jnp.arange(logits.shape[1], dtype=jnp.int32)[None, :]
    picked = jnp.sum(jnp.where(is_label, log_prob, 0.0), axis=-1)
    d_logits = (jnp.exp(log_prob) - is_label.astype(jnp.float32)) * train_mask[:, None]
    return jnp.sum(train_mask * -picked), d_logits


def solution(mesh):
    def device_step(features, labels, train_mask, send_idx, src_idx, dst_idx, inv_deg,
                    w_self_1, w_neigh_1, bias_1, w_self_2, w_neigh_2, bias_2,
                    w_self_3, w_neigh_3, bias_3):
        n_own = features.shape[0]
        group, slots = send_idx.shape
        columns, rounds, count, lists = exchange_plan(send_idx, src_idx, train_mask, n_own)
        n_recv = group * LANES
        starts = jnp.sum(dst_idx[None, :] < (jnp.arange(n_own // DST_TILE + 1) * DST_TILE)[:, None],
                         axis=1, dtype=jnp.int32)

        def adjacency_of(part):
            return adjacency(part, starts, dst_idx, columns, n_own, n_recv)

        adj_own, adj_first = adjacency_of(0)

        def swap(rows):
            return lax.all_to_all(rows, GROUP_AXIS, 0, 0, tiled=True)

        def aggregate(hidden):
            def one_round(part, adj_rec, total):
                received = swap(pick(lists[part], hidden))
                return gather_in(adj_rec, received.reshape(n_recv, -1), total)

            summed = one_round(0, adj_first, jnp.dot(adj_own, hidden, preferred_element_type=F32))
            summed = lax.fori_loop(1, rounds, lambda part, total: one_round(part, adjacency_of(part)[1], total), summed)
            return (summed * inv_deg[:, None]).astype(BF16)

        def layer(hidden, w_self, w_neigh, bias):
            neigh_mean = aggregate(hidden)
            pre_act = (jnp.dot(hidden, w_self, preferred_element_type=jnp.float32)
                       + jnp.dot(neigh_mean, w_neigh, preferred_element_type=jnp.float32) + bias)
            return neigh_mean, pre_act

        def back_to_owners(d_mean, d_self):
            d_sum = (d_mean * inv_deg[:, None]).astype(BF16)

            def one_round(part, adj_rec, total):
                returned = swap(spread_out(adj_rec, d_sum).reshape(group, LANES, -1))
                return put_back(lists[part], returned, total)

            d_own = d_self + jnp.einsum('nt,nd->td', adj_own, d_sum, preferred_element_type=F32)
            return lax.fori_loop(1, rounds, lambda part, total: one_round(part, adjacency_of(part)[1], total),
                                 one_round(0, adj_first, d_own))

        mean_1, pre_1 = layer(features, w_self_1, w_neigh_1, bias_1)
        hidden_1 = jax.nn.relu(pre_1).astype(jnp.bfloat16)
        mean_2, pre_2 = layer(hidden_1, w_self_2, w_neigh_2, bias_2)
        hidden_2 = jax.nn.relu(pre_2).astype(jnp.bfloat16)
        mean_3, logits = layer(hidden_2, w_self_3, w_neigh_3, bias_3)
        loss_sum, d_logits = head_grad(logits, labels, train_mask)

        d_pre_3 = d_logits / count
        d_bf_3 = d_pre_3.astype(jnp.bfloat16)
        g_self_3 = jnp.einsum('ne,nd->ed', d_bf_3, hidden_2, preferred_element_type=F32)
        g_neigh_3 = jnp.einsum('ne,nd->ed', d_bf_3, mean_3, preferred_element_type=F32)
        g_bias_3 = jnp.sum(d_pre_3, axis=0)
        d_self_3, d_mean_3 = input_grads(d_bf_3, w_self_3, w_neigh_3)
        d_pre_2 = jnp.where(pre_2 > 0, back_to_owners(d_mean_3, d_self_3), 0.0)
        d_bf_2 = d_pre_2.astype(jnp.bfloat16)
        g_self_2, g_neigh_2, g_bias_2 = weight_grads(hidden_1, mean_2, d_pre_2, d_bf_2)
        d_self_2, d_mean_2 = input_grads(d_bf_2, w_self_2, w_neigh_2)
        d_pre_1 = jnp.where(pre_1 > 0, back_to_owners(d_mean_2, d_self_2), 0.0)
        d_bf_1 = d_pre_1.astype(jnp.bfloat16)
        g_self_1, g_neigh_1, g_bias_1 = weight_grads(features, mean_1, d_pre_1, d_bf_1)

        classes = g_bias_3.shape[0]
        small = jnp.concatenate([g_bias_1, g_bias_2, jnp.pad(g_bias_3, (0, LANES - classes)),
                                 jnp.full((LANES,), loss_sum / count)]).reshape(-1, LANES)
        small = jnp.pad(small, ((0, 8 - small.shape[0]), (0, 0)))
        summed = add_up((g_self_1, g_neigh_1, g_self_2, g_neigh_2, g_self_3, g_neigh_3, small), group)
        outs = unpack(summed, (g_self_1.shape, g_neigh_1.shape, g_self_2.shape, g_neigh_2.shape,
                               w_self_3.shape, w_neigh_3.shape), (False,) * 4 + (True,) * 2)
        gs_1, gn_1, gs_2, gn_2, gs_3, gn_3, small = outs
        small = small.reshape(-1)
        n_1, n_2 = g_bias_1.shape[0], g_bias_2.shape[0]
        return (small[n_1 + n_2 + LANES], gs_1, gn_1, small[:n_1], gs_2, gn_2, small[n_1:n_1 + n_2],
                gs_3, gn_3, small[n_1 + n_2:n_1 + n_2 + classes])

    sharded = P(GROUP_AXIS)
    whole = P()
    return jax.shard_map(device_step, mesh=mesh,
                         in_specs=(sharded,) * 7 + (whole,) * 9,
                         out_specs=(whole,) * 10, check_vma=False)
```

```python
import functools

import jax
import jax.numpy as jnp
from jax import lax
from jax.experimental import pallas as pl
from jax.experimental.pallas import tpu as pltpu
from jax.sharding import PartitionSpec as P

GROUP_AXIS = 'gp'
LANES = 128
DST_TILE = 256
WINDOW = 8
COLS = 512
BATCH = 8
PLANE = 8
ROWS = 512
VMEM_BYTES = 60 * 1024 * 1024
MESH = pl.DeviceIdType.MESH
F32 = jnp.float32
IDX = jnp.int16
BF16 = jnp.bfloat16


def as_columns(row):
    return jnp.broadcast_to(row, (LANES, LANES)).T


def adjacency_kernel(n_own, starts, parts, dst_ref, col_ref, own_ref, rec_ref):
    part, tile = parts[0], pl.program_id(0)
    first = lax.div(starts[tile], LANES)
    last = lax.div(starts[tile + 1] + LANES - 1, LANES)
    n_recv = rec_ref.shape[1]
    dst_iota = lax.broadcasted_iota(jnp.int32, (DST_TILE, LANES), 0) + tile * DST_TILE
    lanes = lax.broadcasted_iota(jnp.int32, (WINDOW * LANES, LANES), 1).astype(IDX)

    def window_step(w, carry):
        rows = first + w * WINDOW
        dst = dst_ref[pl.ds(rows, WINDOW), :]
        col = col_ref[pl.ds(rows, WINDOW), :]
        mine = (col >= n_own + part * n_recv) & (col < n_own + (part + 1) * n_recv)
        col = jnp.where(col < n_own, col, jnp.where(mine, col - part * n_recv, -1))
        to_dst = jnp.concatenate([(dst_iota == dst[k:k + 1, :]).astype(BF16) for k in range(WINDOW)], axis=1)
        columns = jnp.concatenate([as_columns(col[k:k + 1, :]) for k in range(WINDOW)], axis=0).astype(IDX)

        def fill(out_ref, base):
            def block_step(b, carry):
                offset = pl.multiple_of(b * COLS, COLS)
                shifted = columns - (base + offset).astype(IDX)
                hot = jnp.concatenate([jnp.where(shifted == lanes + IDX(j * LANES), BF16(1), BF16(0))
                                       for j in range(COLS // LANES)], axis=1)
                counts = jnp.dot(to_dst, hot, preferred_element_type=F32)
                at = (slice(None), pl.ds(offset, COLS))

                @pl.when(w == 0)
                def _():
                    out_ref[at] = counts.astype(BF16)

                @pl.when(w > 0)
                def _():
                    out_ref[at] = (out_ref[at].astype(F32) + counts).astype(BF16)

                return carry

            lax.fori_loop(0, out_ref.shape[1] // COLS, block_step, 0)

        fill(own_ref, 0)
        fill(rec_ref, n_own)
        return carry

    windows = jnp.maximum(lax.div(last - first + WINDOW - 1, WINDOW), 1)
    lax.fori_loop(0, windows, window_step, 0)


def adjacency(part, starts, dst_idx, columns, n_own, n_recv):
    def rows_of(index):
        padding = jnp.full((WINDOW * LANES,), -1, jnp.int32)
        return jnp.concatenate([index, padding]).reshape(-1, LANES)

    rows = dst_idx.shape[0] // LANES + WINDOW
    grid_spec = pltpu.PrefetchScalarGridSpec(
        num_scalar_prefetch=2, grid=(n_own // DST_TILE,),
        in_specs=[pl.BlockSpec((rows, LANES), lambda i, *_: (0, 0))] * 2,
        out_specs=[pl.BlockSpec((DST_TILE, n_own), lambda i, *_: (i, 0)),
                   pl.BlockSpec((DST_TILE, n_recv), lambda i, *_: (i, 0))])
    return pl.pallas_call(
        functools.partial(adjacency_kernel, n_own), grid_spec=grid_spec,
        out_shape=[jax.ShapeDtypeStruct((n_own, n_own), BF16), jax.ShapeDtypeStruct((n_own, n_recv), BF16)],
        compiler_params=pltpu.CompilerParams(vmem_limit_bytes=VMEM_BYTES),
        cost_estimate=pl.CostEstimate(flops=30 * 10**9, bytes_accessed=40 * 10**6, transcendentals=0),
        name='adjacency',
    )(starts, jnp.reshape(part, (1,)).astype(jnp.int32), rows_of(dst_idx), rows_of(columns))


def pick_kernel(list_ref, rows_ref, out_ref):
    n_rows = rows_ref.shape[0]
    lane_iota = lax.broadcasted_iota(jnp.int32, (LANES, LANES), 1)

    def hot(row):
        columns = as_columns(row)
        return jnp.concatenate(
            [(columns == lane_iota + j * LANES).astype(BF16) for j in range(n_rows // LANES)], axis=1)

    all_hot = jnp.concatenate([hot(list_ref[b:b + 1, :]) for b in range(BATCH)], axis=0)
    picked = jnp.dot(all_hot, rows_ref[...], preferred_element_type=F32).astype(BF16)
    for b in range(BATCH):
        out_ref[b] = picked[b * LANES:(b + 1) * LANES]


def pick(lists, rows):
    group, _ = lists.shape
    n_rows, width = rows.shape
    return pl.pallas_call(
        pick_kernel, grid=(group // BATCH,),
        in_specs=[pl.BlockSpec((BATCH, LANES), lambda i: (i, 0)),
                  pl.BlockSpec((n_rows, width), lambda i: (0, 0))],
        out_specs=pl.BlockSpec((BATCH, LANES, width), lambda i: (i, 0, 0)),
        out_shape=jax.ShapeDtypeStruct((group, LANES, width), BF16),
        compiler_params=pltpu.CompilerParams(vmem_limit_bytes=VMEM_BYTES),
        cost_estimate=pl.CostEstimate(flops=2 * group * LANES * n_rows * width, bytes_accessed=4 * 10**6,
                                      transcendentals=0),
        name='pick',
    )(lists, rows)


def put_back_kernel(list_ref, sent_ref, add_ref, out_ref):
    n_rows = out_ref.shape[0]
    row_iota = lax.broadcasted_iota(jnp.int32, (n_rows, LANES), 0)

    @pl.when(pl.program_id(0) == 0)
    def _():
        out_ref[...] = add_ref[...]

    hot = jnp.concatenate([(row_iota == list_ref[b:b + 1, :]).astype(BF16) for b in range(BATCH)], axis=1)
    rows = jnp.concatenate([sent_ref[b] for b in range(BATCH)], axis=0)
    out_ref[...] += jnp.dot(hot, rows, preferred_element_type=F32)


def put_back(lists, sent, add):
    group, _ = lists.shape
    n_rows, width = add.shape
    return pl.pallas_call(
        put_back_kernel, grid=(group // BATCH,),
        in_specs=[pl.BlockSpec((BATCH, LANES), lambda i: (i, 0)),
                  pl.BlockSpec((BATCH, LANES, width), lambda i: (i, 0, 0)),
                  pl.BlockSpec((n_rows, width), lambda i: (0, 0))],
        out_specs=pl.BlockSpec((n_rows, width), lambda i: (0, 0)),
        out_shape=jax.ShapeDtypeStruct((n_rows, width), F32),
        compiler_params=pltpu.CompilerParams(vmem_limit_bytes=VMEM_BYTES),
        cost_estimate=pl.CostEstimate(flops=2 * group * LANES * n_rows * width, bytes_accessed=8 * 10**6,
                                      transcendentals=0),
        name='put_back',
    )(lists, sent, add)


def gather_in_kernel(adj_ref, rows_ref, add_ref, out_ref):
    out_ref[...] = add_ref[...] + jnp.dot(adj_ref[...], rows_ref[...], preferred_element_type=F32)


def gather_in(adj_rec, rows, add):
    n_own, n_recv = adj_rec.shape
    width = rows.shape[1]
    return pl.pallas_call(
        gather_in_kernel, grid=(n_own // DST_TILE,),
        in_specs=[pl.BlockSpec((DST_TILE, n_recv), lambda i: (i, 0)),
                  pl.BlockSpec((n_recv, width), lambda i: (0, 0)),
                  pl.BlockSpec((DST_TILE, width), lambda i: (i, 0))],
        out_specs=pl.BlockSpec((DST_TILE, width), lambda i: (i, 0)),
        out_shape=jax.ShapeDtypeStruct((n_own, width), F32),
        compiler_params=pltpu.CompilerParams(vmem_limit_bytes=VMEM_BYTES),
        cost_estimate=pl.CostEstimate(flops=2 * n_own * n_recv * width, bytes_accessed=20 * 10**6, transcendentals=0),
        name='gather_in',
    )(adj_rec, rows, add)


def spread_out_kernel(adj_ref, rows_ref, out_ref):
    out_ref[...] = lax.dot_general(adj_ref[...], rows_ref[...], (((0,), (0,)), ((), ())),
                                   preferred_element_type=F32).astype(BF16)


def spread_out(adj_rec, rows):
    n_own, n_recv = adj_rec.shape
    width = rows.shape[1]
    return pl.pallas_call(
        spread_out_kernel, grid=(n_recv // COLS,),
        in_specs=[pl.BlockSpec((n_own, COLS), lambda i: (0, i)),
                  pl.BlockSpec((n_own, width), lambda i: (0, 0))],
        out_specs=pl.BlockSpec((COLS, width), lambda i: (i, 0)),
        out_shape=jax.ShapeDtypeStruct((n_recv, width), BF16),
        compiler_params=pltpu.CompilerParams(vmem_limit_bytes=VMEM_BYTES),
        cost_estimate=pl.CostEstimate(flops=2 * n_own * n_recv * width, bytes_accessed=20 * 10**6, transcendentals=0),
        name='spread_out',
    )(adj_rec, rows)


def plane_order(me, planes):
    z = lax.div(me, PLANE)
    if planes == 4:
        return [lax.rem(z + 2, 4), 3 - z, z + 1 - 2 * lax.rem(z, 2), z]
    return [lax.rem(z + step, planes) for step in range(1, planes + 1)]


def meet_all(barrier, me, group):
    def signal(step, carry):
        pl.semaphore_signal(barrier, inc=1, device_id=(lax.rem(me + step, group),), device_id_type=MESH)
        return carry

    lax.fori_loop(1, group, signal, 0)


class Swap:
    def __init__(self, me, outbox, inbox, send, recv):
        self.me, self.outbox, self.inbox, self.send, self.recv = me, outbox, inbox, send, recv

    def copy(self, peer, slot):
        return pltpu.make_async_remote_copy(
            src_ref=self.outbox.at[peer], dst_ref=self.inbox.at[slot], send_sem=self.send.at[peer],
            recv_sem=self.recv.at[slot], device_id=(peer,), device_id_type=MESH)

    def others(self, plane, own):
        if own:
            return [plane * PLANE + lax.rem(self.me + step, PLANE) for step in range(1, PLANE)]
        return [plane * PLANE + step for step in range(PLANE)]

    def send_plane(self, plane, own):
        for peer in self.others(plane, own):
            self.copy(peer, self.me).start()
        if own:
            self.inbox[self.me] = self.outbox[self.me]

    def receive_plane(self, plane, own):
        for peer in self.others(plane, own):
            self.copy(peer, peer).wait_recv()
        block = self.inbox[pl.ds(plane * PLANE, PLANE)]
        return block.reshape(block.shape[0] * block.shape[1], block.shape[2])

    def finish(self, planes):
        for k, plane in enumerate(planes):
            for peer in self.others(plane, k == len(planes) - 1):
                self.copy(peer, self.me).wait_send()


def fetch_adjacency(own_hbm, rec_hbm, own_ref, rec_ref, planes, sems):
    span = rec_ref.shape[2]
    own = pltpu.make_async_copy(own_hbm, own_ref, sems.at[len(planes)])
    recs = [pltpu.make_async_copy(rec_hbm.at[:, pl.ds(pl.multiple_of(plane * span, span), span)], rec_ref.at[k],
                                  sems.at[k]) for k, plane in enumerate(planes)]
    return own, recs


def exchange_in_kernel(group, list_ref, rows_ref, own_hbm, rec_hbm, out_ref,
                       outbox, inbox, own_ref, rec_ref, send, recv, sems):
    me = lax.axis_index(GROUP_AXIS)
    planes = plane_order(me, group // PLANE)
    barrier = pltpu.get_barrier_semaphore()
    meet_all(barrier, me, group)
    own_copy, rec_copies = fetch_adjacency(own_hbm, rec_hbm, own_ref, rec_ref, planes, sems)
    for item in [own_copy] + rec_copies[::-1]:
        item.start()
    swap = Swap(me, outbox, inbox, send, recv)
    n_rows = rows_ref.shape[0]
    lanes = lax.broadcasted_iota(jnp.int32, (LANES, LANES), 1).astype(IDX)
    met = False
    for k, plane in enumerate(planes):
        def pick_one(b, carry):
            columns = as_columns(list_ref[pl.ds(plane * PLANE + b, 1), :]).astype(IDX)
            hot = jnp.concatenate([jnp.where(columns == lanes + IDX(j * LANES), BF16(1), BF16(0))
                                   for j in range(n_rows // LANES)], axis=1)
            return hot

        hot = jnp.concatenate([pick_one(b, 0) for b in range(PLANE)], axis=0)
        picked = jnp.dot(hot, rows_ref[...], preferred_element_type=F32).astype(BF16)
        outbox[pl.ds(plane * PLANE, PLANE)] = picked.reshape(PLANE, LANES, picked.shape[1])
        if not met:
            pl.semaphore_wait(barrier, group - 1)
            met = True
        swap.send_plane(plane, k == len(planes) - 1)
    own_copy.wait()

    def own_step(i, carry):
        at = pl.ds(pl.multiple_of(i * ROWS, ROWS), ROWS)
        out_ref[at, :] = jnp.dot(own_ref[at, :], rows_ref[...], preferred_element_type=F32)
        return carry

    lax.fori_loop(0, n_rows // ROWS, own_step, 0)
    for k in [3, 2, 0, 1] if len(planes) == 4 else range(len(planes))[::-1]:
        rec_copies[k].wait()
        block = swap.receive_plane(planes[k], k == len(planes) - 1)

        def rec_step(i, carry):
            at = pl.ds(pl.multiple_of(i * ROWS, ROWS), ROWS)
            out_ref[at, :] += jnp.dot(rec_ref[k, at, :], block, preferred_element_type=F32)
            return carry

        lax.fori_loop(0, n_rows // ROWS, rec_step, 0)
    swap.finish(planes)


def exchange_back_kernel(group, list_ref, grad_ref, add_ref, own_hbm, rec_hbm, out_ref,
                         outbox, inbox, own_ref, rec_ref, send, recv, sems):
    me = lax.axis_index(GROUP_AXIS)
    planes = plane_order(me, group // PLANE)
    barrier = pltpu.get_barrier_semaphore()
    meet_all(barrier, me, group)
    own_copy, rec_copies = fetch_adjacency(own_hbm, rec_hbm, own_ref, rec_ref, planes, sems)
    for item in rec_copies + [own_copy]:
        item.start()
    swap = Swap(me, outbox, inbox, send, recv)
    n_rows, width = grad_ref.shape
    met = False
    for k, plane in enumerate(planes):
        rec_copies[k].wait()
        part = lax.dot_general(rec_ref[k], grad_ref[...], (((0,), (0,)), ((), ())), preferred_element_type=F32)
        outbox[pl.ds(plane * PLANE, PLANE)] = part.astype(BF16).reshape(PLANE, LANES, width)
        if not met:
            pl.semaphore_wait(barrier, group - 1)
            met = True
        swap.send_plane(plane, k == len(planes) - 1)
    own_copy.wait()

    def own_step(i, carry):
        at = pl.ds(pl.multiple_of(i * ROWS, ROWS), ROWS)
        out_ref[at, :] = add_ref[at, :] + lax.dot_general(
            own_ref[:, at], grad_ref[...], (((0,), (0,)), ((), ())), preferred_element_type=F32)
        return carry

    lax.fori_loop(0, n_rows // ROWS, own_step, 0)
    row_iota = lax.broadcasted_iota(jnp.int32, (ROWS, LANES), 0)
    for k in [3, 2, 0, 1] if len(planes) == 4 else range(len(planes))[::-1]:
        block = swap.receive_plane(planes[k], k == len(planes) - 1)
        names = list_ref[pl.ds(pl.multiple_of(planes[k] * PLANE, PLANE), PLANE), :]

        def rec_step(i, carry):
            at = pl.ds(pl.multiple_of(i * ROWS, ROWS), ROWS)
            rows = (row_iota + i * ROWS).astype(IDX)
            hot = jnp.concatenate(
                [jnp.where(rows == jnp.broadcast_to(names[b:b + 1, :], (ROWS, LANES)).astype(IDX), BF16(1), BF16(0))
                 for b in range(PLANE)], axis=1)
            out_ref[at, :] += jnp.dot(hot, block, preferred_element_type=F32)
            return carry

        lax.fori_loop(0, n_rows // ROWS, rec_step, 0)
    swap.finish(planes)


def exchange(body, which, name, lists, arrays, adj_own, adj_rec):
    group = lists.shape[0]
    n_rows, width = arrays[0].shape
    planes = group // PLANE
    vmem, anywhere = pl.BlockSpec(memory_space=pltpu.VMEM), pl.BlockSpec(memory_space=pl.ANY)
    box = pltpu.VMEM((group, LANES, width), BF16)
    return pl.pallas_call(
        functools.partial(body, group),
        in_specs=[vmem] * (1 + len(arrays)) + [anywhere] * 2, out_specs=vmem,
        out_shape=jax.ShapeDtypeStruct((n_rows, width), F32),
        scratch_shapes=[box, box, pltpu.VMEM(adj_own.shape, BF16),
                        pltpu.VMEM((planes, n_rows, adj_rec.shape[1] // planes), BF16),
                        pltpu.SemaphoreType.DMA((group,)), pltpu.SemaphoreType.DMA((group,)),
                        pltpu.SemaphoreType.DMA((planes + 1,))],
        compiler_params=pltpu.CompilerParams(collective_id=which, has_side_effects=True, vmem_limit_bytes=VMEM_BYTES),
        cost_estimate=pl.CostEstimate(flops=2 * 2 * n_rows * adj_rec.shape[1] * width, bytes_accessed=30 * 10**6,
                                      transcendentals=0),
        name=name,
    )(lists, *arrays, adj_own, adj_rec)


def add_up_kernel(n_chips, rows, *refs):
    parts, (out_ref, packed, partner_half, mine, inbox, total, gathered, send, recv) = refs[:-9], refs[-9:]
    me = lax.axis_index(GROUP_AXIS)
    core, chip = lax.rem(me, 2), lax.div(me, 2)
    partner = me + 1 - 2 * core

    def twin(step):
        return 2 * lax.rem(chip + step, n_chips) + core

    barrier = pltpu.get_barrier_semaphore()
    pl.semaphore_signal(barrier, inc=1, device_id=(partner,), device_id_type=MESH)
    for step in range(1, n_chips):
        pl.semaphore_signal(barrier, inc=1, device_id=(twin(step),), device_id_type=MESH)

    at = 0
    for ref in parts:
        count, width = ref.shape
        for j in range(width // LANES):
            packed[at:at + count, :] = ref[:, j * LANES:(j + 1) * LANES]
            at += count
    packed[at:, :] = jnp.zeros((packed.shape[0] - at, LANES), F32)
    half = n_chips * rows

    def half_of(which):
        return pl.ds(pl.multiple_of(which * half, 8), half)

    def copy(src, dst, slot, device):
        return pltpu.make_async_remote_copy(
            src_ref=src, dst_ref=dst, send_sem=send.at[slot], recv_sem=recv.at[slot],
            device_id=(device,), device_id_type=MESH)

    pl.semaphore_wait(barrier, n_chips)
    first = copy(packed.at[half_of(1 - core)], partner_half, 0, partner)
    first.start()
    first.wait()
    mine[...] = (packed[half_of(core), :] + partner_half[...]).reshape(n_chips, rows, LANES)
    sends = []
    for step in range(1, n_chips):
        sends.append(copy(mine.at[lax.rem(chip + step, n_chips)], inbox.at[step], step, twin(step)))
        sends[-1].start()
    value = mine[chip]
    for step in range(1, n_chips):
        sends[step - 1].wait_recv()
        value = value + inbox[step]
    total[...] = value
    for item in sends:
        item.wait_send()
    spread = []
    for step in range(1, n_chips):
        spread.append(copy(total, gathered.at[core, chip], n_chips + step, twin(step)))
        spread[-1].start()
    gathered[core, chip] = value
    for item in spread:
        item.wait()
    last = copy(gathered.at[core], gathered.at[core], 2 * n_chips, partner)
    last.start()
    last.wait()
    out_ref[...] = gathered[...].reshape(2 * half, LANES)


def add_up(parts, group):
    n_chips = group // 2
    used = sum(p.size for p in parts) // LANES
    rows = -(-used // (group * 8)) * 8
    total = group * rows
    chunk = (rows, LANES)
    return pl.pallas_call(
        functools.partial(add_up_kernel, n_chips, rows),
        in_specs=[pl.BlockSpec(memory_space=pltpu.VMEM)] * len(parts),
        out_specs=pl.BlockSpec(memory_space=pltpu.VMEM),
        out_shape=jax.ShapeDtypeStruct((total, LANES), F32),
        scratch_shapes=[pltpu.VMEM((total, LANES), F32), pltpu.VMEM((total // 2, LANES), F32),
                        pltpu.VMEM((n_chips,) + chunk, F32), pltpu.VMEM((n_chips,) + chunk, F32),
                        pltpu.VMEM(chunk, F32), pltpu.VMEM((2, n_chips) + chunk, F32),
                        pltpu.SemaphoreType.DMA((2 * n_chips + 1,)), pltpu.SemaphoreType.DMA((2 * n_chips + 1,))],
        compiler_params=pltpu.CompilerParams(collective_id=0, has_side_effects=True),
        name='add_up',
    )(*parts)


def unpack_kernel(flipped, packed_ref, *out_refs):
    at = 0
    for ref, flip in zip(out_refs[:-1], flipped):
        count, width = ref.shape[::-1] if flip else ref.shape
        pieces = []
        for j in range(width // LANES):
            pieces.append(packed_ref[at:at + count, :])
            at += count
        if flip:
            short = jnp.zeros((LANES - count, LANES), F32)
            for j, piece in enumerate(pieces):
                ref[j * LANES:(j + 1) * LANES, :] = jnp.concatenate([piece, short], axis=0).T[:, :count]
        else:
            ref[...] = jnp.concatenate(pieces, axis=1)
    out_refs[-1][...] = packed_ref[at:at + out_refs[-1].shape[0], :]


def unpack(packed, shapes, flipped):
    return pl.pallas_call(
        functools.partial(unpack_kernel, flipped),
        in_specs=[pl.BlockSpec(memory_space=pltpu.VMEM)],
        out_specs=[pl.BlockSpec(memory_space=pltpu.VMEM)] * (len(shapes) + 1),
        out_shape=[jax.ShapeDtypeStruct(shape, F32) for shape in shapes + ((8, LANES),)],
        name='unpack',
    )(packed)


def before(count):
    index = jnp.arange(count, dtype=jnp.int32)
    return index[:, None] < index[None, :]


def rank_in_row(flags):
    tri = before(flags.shape[1]).astype(BF16)
    return jnp.dot(flags.astype(BF16), tri, preferred_element_type=F32).astype(jnp.int32)


def exchange_plan(send_idx, src_idx, train_mask, n_own):
    group, slots = send_idx.shape
    halo = src_idx - n_own
    peer, slot = halo // slots, halo % slots
    from_peer = ((halo >= 0)[:, None] & (peer[:, None] == jnp.arange(group, dtype=jnp.int32)[None, :])).astype(BF16)
    at_slot = (slot[:, None] == jnp.arange(slots, dtype=jnp.int32)[None, :]).astype(BF16)
    needed = jnp.einsum('eg,es->gs', from_peer, at_slot, preferred_element_type=F32) > 0
    rank = rank_in_row(needed)
    my_rounds = (jnp.max(jnp.where(needed, rank, 0)) // LANES + 1).astype(jnp.int32)
    upper = rank // LANES * group + jnp.arange(group, dtype=jnp.int32)[:, None]
    split = jnp.concatenate([upper, rank % LANES], axis=1).astype(BF16)
    found = jnp.dot(from_peer, split, preferred_element_type=F32)
    found = jnp.sum((found[:, :slots] * LANES + found[:, slots:]) * at_slot.astype(F32), axis=1).astype(jnp.int32)
    columns = jnp.where(halo >= 0, n_own + found, src_idx)
    my_count = jnp.sum(train_mask).astype(jnp.int32)
    extras = jnp.where(jnp.arange(LANES) == 0, my_rounds, my_count)
    message = jnp.concatenate([jnp.where(needed, rank, -1), jnp.broadcast_to(extras, (group, LANES))], axis=1)
    message = lax.all_to_all(message, GROUP_AXIS, 0, 0, tiled=True)
    asked, rounds = message[:, :slots], jnp.max(message[:, slots])
    count = jnp.sum(message[:, slots + 1]).astype(F32)
    k = jnp.arange(slots, dtype=jnp.int32)
    chosen = asked[:, None, :] == k[None, :, None]
    lists = jnp.sum(jnp.where(chosen, send_idx[:, None, :] + 1, 0), axis=2) - 1
    return columns, rounds, count, lists.reshape(group, slots // LANES, LANES).transpose(1, 0, 2)


def weight_grads(h_in, neigh_mean, d_pre, d_pre_bf):
    g_self = jnp.einsum('nd,ne->de', h_in, d_pre_bf, preferred_element_type=jnp.float32)
    g_neigh = jnp.einsum('nd,ne->de', neigh_mean, d_pre_bf, preferred_element_type=jnp.float32)
    return g_self, g_neigh, jnp.sum(d_pre, axis=0)


def input_grads(d_pre_bf, w_self, w_neigh):
    d_self = jnp.einsum('ne,de->nd', d_pre_bf, w_self, preferred_element_type=jnp.float32)
    d_mean = jnp.einsum('ne,de->nd', d_pre_bf, w_neigh, preferred_element_type=jnp.float32)
    return d_self, d_mean


def head_grad(logits, labels, train_mask):
    log_prob = jax.nn.log_softmax(logits, axis=-1)
    is_label = labels[:, None] == jnp.arange(logits.shape[1], dtype=jnp.int32)[None, :]
    picked = jnp.sum(jnp.where(is_label, log_prob, 0.0), axis=-1)
    d_logits = (jnp.exp(log_prob) - is_label.astype(jnp.float32)) * train_mask[:, None]
    return jnp.sum(train_mask * -picked), d_logits


def solution(mesh):
    def device_step(features, labels, train_mask, send_idx, src_idx, dst_idx, inv_deg,
                    w_self_1, w_neigh_1, bias_1, w_self_2, w_neigh_2, bias_2,
                    w_self_3, w_neigh_3, bias_3):
        n_own = features.shape[0]
        group, slots = send_idx.shape
        columns, rounds, count, lists = exchange_plan(send_idx, src_idx, train_mask, n_own)
        n_recv = group * LANES
        starts = jnp.sum(dst_idx[None, :] < (jnp.arange(n_own // DST_TILE + 1) * DST_TILE)[:, None],
                         axis=1, dtype=jnp.int32)

        def adjacency_of(part):
            return adjacency(part, starts, dst_idx, columns, n_own, n_recv)

        adj_own, adj_first = adjacency_of(0)

        def swap(rows):
            return lax.all_to_all(rows, GROUP_AXIS, 0, 0, tiled=True)

        def aggregate(hidden, which):
            def more(part, total):
                received = swap(pick(lists[part], hidden))
                return gather_in(adjacency_of(part)[1], received.reshape(n_recv, -1), total)

            summed = exchange(exchange_in_kernel, which, 'exchange_in', lists[0], (hidden,), adj_own, adj_first)
            summed = lax.fori_loop(1, rounds, more, summed)
            return (summed * inv_deg[:, None]).astype(BF16)

        def layer(hidden, w_self, w_neigh, bias, which):
            neigh_mean = aggregate(hidden, which)
            pre_act = (jnp.dot(hidden, w_self, preferred_element_type=jnp.float32)
                       + jnp.dot(neigh_mean, w_neigh, preferred_element_type=jnp.float32) + bias)
            return neigh_mean, pre_act

        def back_to_owners(d_mean, d_self, which):
            d_sum = (d_mean * inv_deg[:, None]).astype(BF16)

            def more(part, total):
                returned = swap(spread_out(adjacency_of(part)[1], d_sum).reshape(group, LANES, -1))
                return put_back(lists[part], returned, total)

            d_hidden = exchange(exchange_back_kernel, which, 'exchange_back', lists[0], (d_sum, d_self),
                                adj_own, adj_first)
            return lax.fori_loop(1, rounds, more, d_hidden)

        mean_1, pre_1 = layer(features, w_self_1, w_neigh_1, bias_1, 1)
        hidden_1 = jax.nn.relu(pre_1).astype(jnp.bfloat16)
        mean_2, pre_2 = layer(hidden_1, w_self_2, w_neigh_2, bias_2, 2)
        hidden_2 = jax.nn.relu(pre_2).astype(jnp.bfloat16)
        mean_3, logits = layer(hidden_2, w_self_3, w_neigh_3, bias_3, 3)
        loss_sum, d_logits = head_grad(logits, labels, train_mask)

        d_pre_3 = d_logits / count
        d_bf_3 = d_pre_3.astype(jnp.bfloat16)
        g_self_3 = jnp.einsum('ne,nd->ed', d_bf_3, hidden_2, preferred_element_type=F32)
        g_neigh_3 = jnp.einsum('ne,nd->ed', d_bf_3, mean_3, preferred_element_type=F32)
        g_bias_3 = jnp.sum(d_pre_3, axis=0)
        d_self_3, d_mean_3 = input_grads(d_bf_3, w_self_3, w_neigh_3)
        d_pre_2 = jnp.where(pre_2 > 0, back_to_owners(d_mean_3, d_self_3, 4), 0.0)
        d_bf_2 = d_pre_2.astype(jnp.bfloat16)
        g_self_2, g_neigh_2, g_bias_2 = weight_grads(hidden_1, mean_2, d_pre_2, d_bf_2)
        d_self_2, d_mean_2 = input_grads(d_bf_2, w_self_2, w_neigh_2)
        d_pre_1 = jnp.where(pre_1 > 0, back_to_owners(d_mean_2, d_self_2, 5), 0.0)
        d_bf_1 = d_pre_1.astype(jnp.bfloat16)
        g_self_1, g_neigh_1, g_bias_1 = weight_grads(features, mean_1, d_pre_1, d_bf_1)

        classes = g_bias_3.shape[0]
        small = jnp.concatenate([g_bias_1, g_bias_2, jnp.pad(g_bias_3, (0, LANES - classes)),
                                 jnp.full((LANES,), loss_sum / count)]).reshape(-1, LANES)
        small = jnp.pad(small, ((0, 8 - small.shape[0]), (0, 0)))
        summed = add_up((g_self_1, g_neigh_1, g_self_2, g_neigh_2, g_self_3, g_neigh_3, small), group)
        outs = unpack(summed, (g_self_1.shape, g_neigh_1.shape, g_self_2.shape, g_neigh_2.shape,
                               w_self_3.shape, w_neigh_3.shape), (False,) * 4 + (True,) * 2)
        gs_1, gn_1, gs_2, gn_2, gs_3, gn_3, small = outs
        small = small.reshape(-1)
        n_1, n_2 = g_bias_1.shape[0], g_bias_2.shape[0]
        return (small[n_1 + n_2 + LANES], gs_1, gn_1, small[:n_1], gs_2, gn_2, small[n_1:n_1 + n_2],
                gs_3, gn_3, small[n_1 + n_2:n_1 + n_2 + classes])

    sharded = P(GROUP_AXIS)
    whole = P()
    return jax.shard_map(device_step, mesh=mesh,
                         in_specs=(sharded,) * 7 + (whole,) * 9,
                         out_specs=(whole,) * 10, check_vma=False)
```

```python
import functools

import jax
import jax.numpy as jnp
from jax import lax
from jax.experimental import pallas as pl
from jax.experimental.pallas import tpu as pltpu
from jax.sharding import PartitionSpec as P

GROUP_AXIS = 'gp'
LANES = 128
DST_TILE = 256
WINDOW = 8
COLS = 1024
BATCH = 8
PLANE = 8
ROWS = 512
VMEM_BYTES = 60 * 1024 * 1024
MESH = pl.DeviceIdType.MESH
F32 = jnp.float32
IDX = jnp.int16
BF16 = jnp.bfloat16


def as_columns(row):
    return jnp.broadcast_to(row, (LANES, LANES)).T


def adjacency_kernel(n_own, starts, parts, dst_ref, col_ref, own_ref, rec_ref):
    part, tile = parts[0], pl.program_id(0)
    first = lax.div(starts[tile], LANES)
    last = lax.div(starts[tile + 1] + LANES - 1, LANES)
    n_recv = rec_ref.shape[1]
    dst_iota = lax.broadcasted_iota(jnp.int32, (DST_TILE, LANES), 0) + tile * DST_TILE
    lanes = lax.broadcasted_iota(jnp.int32, (WINDOW * LANES, LANES), 1).astype(IDX)

    def window_step(w, add):
        rows = first + w * WINDOW
        dst = dst_ref[pl.ds(rows, WINDOW), :]
        col = col_ref[pl.ds(rows, WINDOW), :]
        mine = (col >= n_own + part * n_recv) & (col < n_own + (part + 1) * n_recv)
        col = jnp.where(col < n_own, col, jnp.where(mine, col - part * n_recv, -1))
        to_dst = jnp.concatenate([(dst_iota == dst[k:k + 1, :]).astype(BF16) for k in range(WINDOW)], axis=1)
        columns = jnp.concatenate([as_columns(col[k:k + 1, :]) for k in range(WINDOW)], axis=0).astype(IDX)

        def fill(out_ref, base):
            def block_step(b, carry):
                offset = b * COLS
                shifted = columns - (base + offset).astype(IDX)
                for c in range(0, COLS, 2 * LANES):
                    hot = jnp.concatenate([jnp.where(shifted == lanes + IDX(c + j * LANES), BF16(1), BF16(0))
                                           for j in range(2)], axis=1)
                    counts = jnp.dot(to_dst, hot, preferred_element_type=F32)
                    at = (slice(None), pl.ds(pl.multiple_of(offset + c, 2 * LANES), 2 * LANES))
                    if add:
                        counts = counts + out_ref[at].astype(F32)
                    out_ref[at] = counts.astype(BF16)
                return carry

            lax.fori_loop(0, out_ref.shape[1] // COLS, block_step, 0)

        fill(own_ref, 0)
        fill(rec_ref, n_own)

    window_step(0, False)

    def more(w, carry):
        window_step(w, True)
        return carry

    lax.fori_loop(1, lax.div(last - first + WINDOW - 1, WINDOW), more, 0)


def adjacency(part, starts, dst_idx, columns, n_own, n_recv):
    def rows_of(index):
        padding = jnp.full((WINDOW * LANES,), -1, jnp.int32)
        return jnp.concatenate([index, padding]).reshape(-1, LANES)

    rows = dst_idx.shape[0] // LANES + WINDOW
    grid_spec = pltpu.PrefetchScalarGridSpec(
        num_scalar_prefetch=2, grid=(n_own // DST_TILE,),
        in_specs=[pl.BlockSpec((rows, LANES), lambda i, *_: (0, 0))] * 2,
        out_specs=[pl.BlockSpec((DST_TILE, n_own), lambda i, *_: (i, 0)),
                   pl.BlockSpec((DST_TILE, n_recv), lambda i, *_: (i, 0))])
    return pl.pallas_call(
        functools.partial(adjacency_kernel, n_own), grid_spec=grid_spec,
        out_shape=[jax.ShapeDtypeStruct((n_own, n_own), BF16), jax.ShapeDtypeStruct((n_own, n_recv), BF16)],
        compiler_params=pltpu.CompilerParams(vmem_limit_bytes=VMEM_BYTES),
        cost_estimate=pl.CostEstimate(flops=30 * 10**9, bytes_accessed=40 * 10**6, transcendentals=0),
        name='adjacency',
    )(starts, jnp.reshape(part, (1,)).astype(jnp.int32), rows_of(dst_idx), rows_of(columns))


def pick_kernel(list_ref, rows_ref, out_ref):
    n_rows = rows_ref.shape[0]
    lane_iota = lax.broadcasted_iota(jnp.int32, (LANES, LANES), 1)

    def hot(row):
        columns = as_columns(row)
        return jnp.concatenate(
            [(columns == lane_iota + j * LANES).astype(BF16) for j in range(n_rows // LANES)], axis=1)

    all_hot = jnp.concatenate([hot(list_ref[b:b + 1, :]) for b in range(BATCH)], axis=0)
    picked = jnp.dot(all_hot, rows_ref[...], preferred_element_type=F32).astype(BF16)
    for b in range(BATCH):
        out_ref[b] = picked[b * LANES:(b + 1) * LANES]


def pick(lists, rows):
    group, _ = lists.shape
    n_rows, width = rows.shape
    return pl.pallas_call(
        pick_kernel, grid=(group // BATCH,),
        in_specs=[pl.BlockSpec((BATCH, LANES), lambda i: (i, 0)),
                  pl.BlockSpec((n_rows, width), lambda i: (0, 0))],
        out_specs=pl.BlockSpec((BATCH, LANES, width), lambda i: (i, 0, 0)),
        out_shape=jax.ShapeDtypeStruct((group, LANES, width), BF16),
        compiler_params=pltpu.CompilerParams(vmem_limit_bytes=VMEM_BYTES),
        cost_estimate=pl.CostEstimate(flops=2 * group * LANES * n_rows * width, bytes_accessed=4 * 10**6,
                                      transcendentals=0),
        name='pick',
    )(lists, rows)


def put_back_kernel(list_ref, sent_ref, add_ref, out_ref):
    n_rows = out_ref.shape[0]
    row_iota = lax.broadcasted_iota(jnp.int32, (n_rows, LANES), 0)

    @pl.when(pl.program_id(0) == 0)
    def _():
        out_ref[...] = add_ref[...]

    hot = jnp.concatenate([(row_iota == list_ref[b:b + 1, :]).astype(BF16) for b in range(BATCH)], axis=1)
    rows = jnp.concatenate([sent_ref[b] for b in range(BATCH)], axis=0)
    out_ref[...] += jnp.dot(hot, rows, preferred_element_type=F32)


def put_back(lists, sent, add):
    group, _ = lists.shape
    n_rows, width = add.shape
    return pl.pallas_call(
        put_back_kernel, grid=(group // BATCH,),
        in_specs=[pl.BlockSpec((BATCH, LANES), lambda i: (i, 0)),
                  pl.BlockSpec((BATCH, LANES, width), lambda i: (i, 0, 0)),
                  pl.BlockSpec((n_rows, width), lambda i: (0, 0))],
        out_specs=pl.BlockSpec((n_rows, width), lambda i: (0, 0)),
        out_shape=jax.ShapeDtypeStruct((n_rows, width), F32),
        compiler_params=pltpu.CompilerParams(vmem_limit_bytes=VMEM_BYTES),
        cost_estimate=pl.CostEstimate(flops=2 * group * LANES * n_rows * width, bytes_accessed=8 * 10**6,
                                      transcendentals=0),
        name='put_back',
    )(lists, sent, add)


def gather_in_kernel(adj_ref, rows_ref, add_ref, out_ref):
    out_ref[...] = add_ref[...] + jnp.dot(adj_ref[...], rows_ref[...], preferred_element_type=F32)


def gather_in(adj_rec, rows, add):
    n_own, n_recv = adj_rec.shape
    width = rows.shape[1]
    return pl.pallas_call(
        gather_in_kernel, grid=(n_own // DST_TILE,),
        in_specs=[pl.BlockSpec((DST_TILE, n_recv), lambda i: (i, 0)),
                  pl.BlockSpec((n_recv, width), lambda i: (0, 0)),
                  pl.BlockSpec((DST_TILE, width), lambda i: (i, 0))],
        out_specs=pl.BlockSpec((DST_TILE, width), lambda i: (i, 0)),
        out_shape=jax.ShapeDtypeStruct((n_own, width), F32),
        compiler_params=pltpu.CompilerParams(vmem_limit_bytes=VMEM_BYTES),
        cost_estimate=pl.CostEstimate(flops=2 * n_own * n_recv * width, bytes_accessed=20 * 10**6, transcendentals=0),
        name='gather_in',
    )(adj_rec, rows, add)


def spread_out_kernel(adj_ref, rows_ref, out_ref):
    out_ref[...] = lax.dot_general(adj_ref[...], rows_ref[...], (((0,), (0,)), ((), ())),
                                   preferred_element_type=F32).astype(BF16)


def spread_out(adj_rec, rows):
    n_own, n_recv = adj_rec.shape
    width = rows.shape[1]
    return pl.pallas_call(
        spread_out_kernel, grid=(n_recv // 512,),
        in_specs=[pl.BlockSpec((n_own, 512), lambda i: (0, i)),
                  pl.BlockSpec((n_own, width), lambda i: (0, 0))],
        out_specs=pl.BlockSpec((512, width), lambda i: (i, 0)),
        out_shape=jax.ShapeDtypeStruct((n_recv, width), BF16),
        compiler_params=pltpu.CompilerParams(vmem_limit_bytes=VMEM_BYTES),
        cost_estimate=pl.CostEstimate(flops=2 * n_own * n_recv * width, bytes_accessed=20 * 10**6, transcendentals=0),
        name='spread_out',
    )(adj_rec, rows)


def plane_order(me):
    z = lax.div(me, PLANE)
    near, far, mirror = z + 1 - 2 * lax.rem(z, 2), lax.rem(z + 2, 4), 3 - z
    inner = lax.div(lax.rem(z, 3) + 1, 2)
    sending = [inner * far + (1 - inner) * near, inner * mirror + (1 - inner) * far,
               inner * near + (1 - inner) * mirror, z]
    return sending, [z, near, far, mirror]


def meet_all(barrier, me, group):
    def signal(step, carry):
        pl.semaphore_signal(barrier, inc=1, device_id=(lax.rem(me + step, group),), device_id_type=MESH)
        return carry

    lax.fori_loop(1, group, signal, 0)


class Swap:
    def __init__(self, me, outbox, inbox, send, recv):
        self.me, self.outbox, self.inbox, self.send, self.recv = me, outbox, inbox, send, recv

    def copy(self, peer, slot):
        return pltpu.make_async_remote_copy(
            src_ref=self.outbox.at[peer], dst_ref=self.inbox.at[slot], send_sem=self.send.at[peer],
            recv_sem=self.recv.at[slot], device_id=(peer,), device_id_type=MESH)

    def others(self, plane, own):
        if own:
            return [plane * PLANE + lax.rem(self.me + step, PLANE) for step in range(1, PLANE)]
        return [plane * PLANE + step for step in range(PLANE)]

    def send_plane(self, plane, own):
        for peer in self.others(plane, own):
            self.copy(peer, self.me).start()
        if own:
            self.inbox[self.me] = self.outbox[self.me]

    def receive_plane(self, plane, own):
        for peer in self.others(plane, own):
            self.copy(peer, peer).wait_recv()
        block = self.inbox[pl.ds(plane * PLANE, PLANE)]
        return block.reshape(block.shape[0] * block.shape[1], block.shape[2])

    def finish(self, planes):
        for k, plane in enumerate(planes):
            for peer in self.others(plane, k == len(planes) - 1):
                self.copy(peer, self.me).wait_send()


def fetch_adjacency(own_hbm, rec_hbm, own_ref, rec_ref, planes, sems):
    span = rec_ref.shape[2]
    own = pltpu.make_async_copy(own_hbm, own_ref, sems.at[len(planes)])
    recs = [pltpu.make_async_copy(rec_hbm.at[:, pl.ds(pl.multiple_of(plane * span, span), span)], rec_ref.at[k],
                                  sems.at[k]) for k, plane in enumerate(planes)]
    return own, recs


def exchange_in_kernel(group, list_ref, rows_ref, own_hbm, rec_hbm, out_ref,
                       outbox, inbox, own_ref, rec_ref, send, recv, sems):
    me = lax.axis_index(GROUP_AXIS)
    planes, arriving = plane_order(me)
    barrier = pltpu.get_barrier_semaphore()
    meet_all(barrier, me, group)
    own_copy, rec_copies = fetch_adjacency(own_hbm, rec_hbm, own_ref, rec_ref, arriving, sems)
    for item in [own_copy] + rec_copies:
        item.start()
    swap = Swap(me, outbox, inbox, send, recv)
    n_rows = rows_ref.shape[0]
    lanes = lax.broadcasted_iota(jnp.int32, (LANES, LANES), 1).astype(IDX)
    met = False
    for k, plane in enumerate(planes):
        def pick_one(b, carry):
            columns = as_columns(list_ref[pl.ds(plane * PLANE + b, 1), :]).astype(IDX)
            hot = jnp.concatenate([jnp.where(columns == lanes + IDX(j * LANES), BF16(1), BF16(0))
                                   for j in range(n_rows // LANES)], axis=1)
            return hot

        hot = jnp.concatenate([pick_one(b, 0) for b in range(PLANE)], axis=0)
        picked = jnp.dot(hot, rows_ref[...], preferred_element_type=F32).astype(BF16)
        outbox[pl.ds(plane * PLANE, PLANE)] = picked.reshape(PLANE, LANES, picked.shape[1])
        if not met:
            pl.semaphore_wait(barrier, group - 1)
            met = True
        swap.send_plane(plane, k == len(planes) - 1)
    own_copy.wait()

    def own_step(i, carry):
        at = pl.ds(pl.multiple_of(i * ROWS, ROWS), ROWS)
        out_ref[at, :] = jnp.dot(own_ref[at, :], rows_ref[...], preferred_element_type=F32)
        return carry

    lax.fori_loop(0, n_rows // ROWS, own_step, 0)
    for k, plane in enumerate(arriving):
        rec_copies[k].wait()
        block = swap.receive_plane(plane, k == 0)

        def rec_step(i, carry):
            at = pl.ds(pl.multiple_of(i * ROWS, ROWS), ROWS)
            out_ref[at, :] += jnp.dot(rec_ref[k, at, :], block, preferred_element_type=F32)
            return carry

        lax.fori_loop(0, n_rows // ROWS, rec_step, 0)
    swap.finish(planes)


def exchange_back_kernel(group, list_ref, grad_ref, add_ref, own_hbm, rec_hbm, out_ref,
                         outbox, inbox, own_ref, rec_ref, send, recv, sems):
    me = lax.axis_index(GROUP_AXIS)
    planes, arriving = plane_order(me)
    barrier = pltpu.get_barrier_semaphore()
    meet_all(barrier, me, group)
    own_copy, rec_copies = fetch_adjacency(own_hbm, rec_hbm, own_ref, rec_ref, planes, sems)
    for item in rec_copies + [own_copy]:
        item.start()
    swap = Swap(me, outbox, inbox, send, recv)
    n_rows, width = grad_ref.shape
    met = False
    for k, plane in enumerate(planes):
        rec_copies[k].wait()
        part = lax.dot_general(rec_ref[k], grad_ref[...], (((0,), (0,)), ((), ())), preferred_element_type=F32)
        outbox[pl.ds(plane * PLANE, PLANE)] = part.astype(BF16).reshape(PLANE, LANES, width)
        if not met:
            pl.semaphore_wait(barrier, group - 1)
            met = True
        swap.send_plane(plane, k == len(planes) - 1)
    own_copy.wait()

    def own_step(i, carry):
        at = pl.ds(pl.multiple_of(i * ROWS, ROWS), ROWS)
        out_ref[at, :] = add_ref[at, :] + lax.dot_general(
            own_ref[:, at], grad_ref[...], (((0,), (0,)), ((), ())), preferred_element_type=F32)
        return carry

    lax.fori_loop(0, n_rows // ROWS, own_step, 0)
    row_iota = lax.broadcasted_iota(jnp.int32, (ROWS, LANES), 0)
    for k, plane in enumerate(arriving):
        block = swap.receive_plane(plane, k == 0)
        names = list_ref[pl.ds(pl.multiple_of(plane * PLANE, PLANE), PLANE), :]

        def rec_step(i, carry):
            at = pl.ds(pl.multiple_of(i * ROWS, ROWS), ROWS)
            rows = (row_iota + i * ROWS).astype(IDX)
            hot = jnp.concatenate(
                [jnp.where(rows == jnp.broadcast_to(names[b:b + 1, :], (ROWS, LANES)).astype(IDX), BF16(1), BF16(0))
                 for b in range(PLANE)], axis=1)
            out_ref[at, :] += jnp.dot(hot, block, preferred_element_type=F32)
            return carry

        lax.fori_loop(0, n_rows // ROWS, rec_step, 0)
    swap.finish(planes)


def exchange(body, which, name, lists, arrays, adj_own, adj_rec):
    group = lists.shape[0]
    n_rows, width = arrays[0].shape
    planes = group // PLANE
    vmem, anywhere = pl.BlockSpec(memory_space=pltpu.VMEM), pl.BlockSpec(memory_space=pl.ANY)
    box = pltpu.VMEM((group, LANES, width), BF16)
    return pl.pallas_call(
        functools.partial(body, group),
        in_specs=[vmem] * (1 + len(arrays)) + [anywhere] * 2, out_specs=vmem,
        out_shape=jax.ShapeDtypeStruct((n_rows, width), F32),
        scratch_shapes=[box, box, pltpu.VMEM(adj_own.shape, BF16),
                        pltpu.VMEM((planes, n_rows, adj_rec.shape[1] // planes), BF16),
                        pltpu.SemaphoreType.DMA((group,)), pltpu.SemaphoreType.DMA((group,)),
                        pltpu.SemaphoreType.DMA((planes + 1,))],
        compiler_params=pltpu.CompilerParams(collective_id=which, has_side_effects=True, vmem_limit_bytes=VMEM_BYTES),
        cost_estimate=pl.CostEstimate(flops=2 * 2 * n_rows * adj_rec.shape[1] * width, bytes_accessed=30 * 10**6,
                                      transcendentals=0),
        name=name,
    )(lists, *arrays, adj_own, adj_rec)


def add_up_kernel(n_chips, rows, *refs):
    parts, (out_ref, packed, partner_half, mine, inbox, total, gathered, send, recv) = refs[:-9], refs[-9:]
    me = lax.axis_index(GROUP_AXIS)
    core, chip = lax.rem(me, 2), lax.div(me, 2)
    partner = me + 1 - 2 * core

    def twin(step):
        return 2 * lax.rem(chip + step, n_chips) + core

    barrier = pltpu.get_barrier_semaphore()
    pl.semaphore_signal(barrier, inc=1, device_id=(partner,), device_id_type=MESH)
    for step in range(1, n_chips):
        pl.semaphore_signal(barrier, inc=1, device_id=(twin(step),), device_id_type=MESH)

    at = 0
    for ref in parts:
        count, width = ref.shape
        for j in range(width // LANES):
            packed[at:at + count, :] = ref[:, j * LANES:(j + 1) * LANES]
            at += count
    packed[at:, :] = jnp.zeros((packed.shape[0] - at, LANES), F32)
    half = n_chips * rows

    def half_of(which):
        return pl.ds(pl.multiple_of(which * half, 8), half)

    def copy(src, dst, slot, device):
        return pltpu.make_async_remote_copy(
            src_ref=src, dst_ref=dst, send_sem=send.at[slot], recv_sem=recv.at[slot],
            device_id=(device,), device_id_type=MESH)

    pl.semaphore_wait(barrier, n_chips)
    first = copy(packed.at[half_of(1 - core)], partner_half, 0, partner)
    first.start()
    first.wait()
    mine[...] = (packed[half_of(core), :] + partner_half[...]).reshape(n_chips, rows, LANES)
    sends = []
    for step in range(1, n_chips):
        sends.append(copy(mine.at[lax.rem(chip + step, n_chips)], inbox.at[step], step, twin(step)))
        sends[-1].start()
    value = mine[chip]
    for step in range(1, n_chips):
        sends[step - 1].wait_recv()
        value = value + inbox[step]
    total[...] = value
    for item in sends:
        item.wait_send()
    spread = []
    for step in range(1, n_chips):
        spread.append(copy(total, gathered.at[core, chip], n_chips + step, twin(step)))
        spread[-1].start()
    gathered[core, chip] = value
    for item in spread:
        item.wait()
    last = copy(gathered.at[core], gathered.at[core], 2 * n_chips, partner)
    last.start()
    last.wait()
    out_ref[...] = gathered[...].reshape(2 * half, LANES)


def add_up(parts, group):
    n_chips = group // 2
    used = sum(p.size for p in parts) // LANES
    rows = -(-used // (group * 8)) * 8
    total = group * rows
    chunk = (rows, LANES)
    return pl.pallas_call(
        functools.partial(add_up_kernel, n_chips, rows),
        in_specs=[pl.BlockSpec(memory_space=pltpu.VMEM)] * len(parts),
        out_specs=pl.BlockSpec(memory_space=pltpu.VMEM),
        out_shape=jax.ShapeDtypeStruct((total, LANES), F32),
        scratch_shapes=[pltpu.VMEM((total, LANES), F32), pltpu.VMEM((total // 2, LANES), F32),
                        pltpu.VMEM((n_chips,) + chunk, F32), pltpu.VMEM((n_chips,) + chunk, F32),
                        pltpu.VMEM(chunk, F32), pltpu.VMEM((2, n_chips) + chunk, F32),
                        pltpu.SemaphoreType.DMA((2 * n_chips + 1,)), pltpu.SemaphoreType.DMA((2 * n_chips + 1,))],
        compiler_params=pltpu.CompilerParams(collective_id=0, has_side_effects=True),
        name='add_up',
    )(*parts)


def unpack_kernel(flipped, packed_ref, *out_refs):
    at = 0
    for ref, flip in zip(out_refs[:-1], flipped):
        count, width = ref.shape[::-1] if flip else ref.shape
        pieces = []
        for j in range(width // LANES):
            pieces.append(packed_ref[at:at + count, :])
            at += count
        if flip:
            short = jnp.zeros((LANES - count, LANES), F32)
            for j, piece in enumerate(pieces):
                ref[j * LANES:(j + 1) * LANES, :] = jnp.concatenate([piece, short], axis=0).T[:, :count]
        else:
            ref[...] = jnp.concatenate(pieces, axis=1)
    out_refs[-1][...] = packed_ref[at:at + out_refs[-1].shape[0], :]


def unpack(packed, shapes, flipped):
    return pl.pallas_call(
        functools.partial(unpack_kernel, flipped),
        in_specs=[pl.BlockSpec(memory_space=pltpu.VMEM)],
        out_specs=[pl.BlockSpec(memory_space=pltpu.VMEM)] * (len(shapes) + 1),
        out_shape=[jax.ShapeDtypeStruct(shape, F32) for shape in shapes + ((8, LANES),)],
        name='unpack',
    )(packed)


def before(count):
    index = jnp.arange(count, dtype=jnp.int32)
    return index[:, None] < index[None, :]


def rank_in_row(flags):
    tri = before(flags.shape[1]).astype(BF16)
    return jnp.dot(flags.astype(BF16), tri, preferred_element_type=F32).astype(jnp.int32)


def exchange_plan(send_idx, src_idx, train_mask, n_own):
    group, slots = send_idx.shape
    halo = src_idx - n_own
    peer, slot = halo // slots, halo % slots
    from_peer = ((halo >= 0)[:, None] & (peer[:, None] == jnp.arange(group, dtype=jnp.int32)[None, :])).astype(BF16)
    at_slot = (slot[:, None] == jnp.arange(slots, dtype=jnp.int32)[None, :]).astype(BF16)
    needed = jnp.einsum('eg,es->gs', from_peer, at_slot, preferred_element_type=F32) > 0
    rank = rank_in_row(needed)
    my_rounds = (jnp.max(jnp.where(needed, rank, 0)) // LANES + 1).astype(jnp.int32)
    upper = rank // LANES * group + jnp.arange(group, dtype=jnp.int32)[:, None]
    split = jnp.concatenate([upper, rank % LANES], axis=1).astype(BF16)
    found = jnp.dot(from_peer, split, preferred_element_type=F32)
    found = jnp.sum((found[:, :slots] * LANES + found[:, slots:]) * at_slot.astype(F32), axis=1).astype(jnp.int32)
    columns = jnp.where(halo >= 0, n_own + found, src_idx)
    my_count = jnp.sum(train_mask).astype(jnp.int32)
    extras = jnp.where(jnp.arange(LANES) == 0, my_rounds, my_count)
    message = jnp.concatenate([jnp.where(needed, rank, -1), jnp.broadcast_to(extras, (group, LANES))], axis=1)
    message = lax.all_to_all(message, GROUP_AXIS, 0, 0, tiled=True)
    asked, rounds = message[:, :slots], jnp.max(message[:, slots])
    count = jnp.sum(message[:, slots + 1]).astype(F32)
    k = jnp.arange(slots, dtype=jnp.int32)
    chosen = asked[:, None, :] == k[None, :, None]
    lists = jnp.sum(jnp.where(chosen, send_idx[:, None, :] + 1, 0), axis=2) - 1
    return columns, rounds, count, lists.reshape(group, slots // LANES, LANES).transpose(1, 0, 2)


def weight_grads(h_in, neigh_mean, d_pre, d_pre_bf):
    g_self = jnp.einsum('nd,ne->de', h_in, d_pre_bf, preferred_element_type=jnp.float32)
    g_neigh = jnp.einsum('nd,ne->de', neigh_mean, d_pre_bf, preferred_element_type=jnp.float32)
    return g_self, g_neigh, jnp.sum(d_pre, axis=0)


def input_grads(d_pre_bf, w_self, w_neigh):
    d_self = jnp.einsum('ne,de->nd', d_pre_bf, w_self, preferred_element_type=jnp.float32)
    d_mean = jnp.einsum('ne,de->nd', d_pre_bf, w_neigh, preferred_element_type=jnp.float32)
    return d_self, d_mean


def head_grad(logits, labels, train_mask):
    log_prob = jax.nn.log_softmax(logits, axis=-1)
    is_label = labels[:, None] == jnp.arange(logits.shape[1], dtype=jnp.int32)[None, :]
    picked = jnp.sum(jnp.where(is_label, log_prob, 0.0), axis=-1)
    d_logits = (jnp.exp(log_prob) - is_label.astype(jnp.float32)) * train_mask[:, None]
    return jnp.sum(train_mask * -picked), d_logits


def solution(mesh):
    def device_step(features, labels, train_mask, send_idx, src_idx, dst_idx, inv_deg,
                    w_self_1, w_neigh_1, bias_1, w_self_2, w_neigh_2, bias_2,
                    w_self_3, w_neigh_3, bias_3):
        n_own = features.shape[0]
        group, slots = send_idx.shape
        columns, rounds, count, lists = exchange_plan(send_idx, src_idx, train_mask, n_own)
        n_recv = group * LANES
        starts = jnp.sum(dst_idx[None, :] < (jnp.arange(n_own // DST_TILE + 1) * DST_TILE)[:, None],
                         axis=1, dtype=jnp.int32)

        def adjacency_of(part):
            return adjacency(part, starts, dst_idx, columns, n_own, n_recv)

        adj_own, adj_first = adjacency_of(0)

        def swap(rows):
            return lax.all_to_all(rows, GROUP_AXIS, 0, 0, tiled=True)

        def aggregate(hidden, which):
            def more(part, total):
                received = swap(pick(lists[part], hidden))
                return gather_in(adjacency_of(part)[1], received.reshape(n_recv, -1), total)

            summed = exchange(exchange_in_kernel, which, 'exchange_in', lists[0], (hidden,), adj_own, adj_first)
            summed = lax.fori_loop(1, rounds, more, summed)
            return (summed * inv_deg[:, None]).astype(BF16)

        def layer(hidden, w_self, w_neigh, bias, which):
            neigh_mean = aggregate(hidden, which)
            pre_act = (jnp.dot(hidden, w_self, preferred_element_type=jnp.float32)
                       + jnp.dot(neigh_mean, w_neigh, preferred_element_type=jnp.float32) + bias)
            return neigh_mean, pre_act

        def back_to_owners(d_mean, d_self, which):
            d_sum = (d_mean * inv_deg[:, None]).astype(BF16)

            def more(part, total):
                returned = swap(spread_out(adjacency_of(part)[1], d_sum).reshape(group, LANES, -1))
                return put_back(lists[part], returned, total)

            d_hidden = exchange(exchange_back_kernel, which, 'exchange_back', lists[0], (d_sum, d_self),
                                adj_own, adj_first)
            return lax.fori_loop(1, rounds, more, d_hidden)

        mean_1, pre_1 = layer(features, w_self_1, w_neigh_1, bias_1, 1)
        hidden_1 = jax.nn.relu(pre_1).astype(jnp.bfloat16)
        mean_2, pre_2 = layer(hidden_1, w_self_2, w_neigh_2, bias_2, 2)
        hidden_2 = jax.nn.relu(pre_2).astype(jnp.bfloat16)
        mean_3, logits = layer(hidden_2, w_self_3, w_neigh_3, bias_3, 3)
        loss_sum, d_logits = head_grad(logits, labels, train_mask)

        d_pre_3 = d_logits / count
        d_bf_3 = d_pre_3.astype(jnp.bfloat16)
        g_self_3 = jnp.einsum('ne,nd->ed', d_bf_3, hidden_2, preferred_element_type=F32)
        g_neigh_3 = jnp.einsum('ne,nd->ed', d_bf_3, mean_3, preferred_element_type=F32)
        g_bias_3 = jnp.sum(d_pre_3, axis=0)
        d_self_3, d_mean_3 = input_grads(d_bf_3, w_self_3, w_neigh_3)
        d_pre_2 = jnp.where(pre_2 > 0, back_to_owners(d_mean_3, d_self_3, 4), 0.0)
        d_bf_2 = d_pre_2.astype(jnp.bfloat16)
        g_self_2, g_neigh_2, g_bias_2 = weight_grads(hidden_1, mean_2, d_pre_2, d_bf_2)
        d_self_2, d_mean_2 = input_grads(d_bf_2, w_self_2, w_neigh_2)
        d_pre_1 = jnp.where(pre_1 > 0, back_to_owners(d_mean_2, d_self_2, 5), 0.0)
        d_bf_1 = d_pre_1.astype(jnp.bfloat16)
        g_self_1, g_neigh_1, g_bias_1 = weight_grads(features, mean_1, d_pre_1, d_bf_1)

        classes = g_bias_3.shape[0]
        small = jnp.concatenate([g_bias_1, g_bias_2, jnp.pad(g_bias_3, (0, LANES - classes)),
                                 jnp.full((LANES,), loss_sum / count)]).reshape(-1, LANES)
        small = jnp.pad(small, ((0, 8 - small.shape[0]), (0, 0)))
        summed = add_up((g_self_1, g_neigh_1, g_self_2, g_neigh_2, g_self_3, g_neigh_3, small), group)
        outs = unpack(summed, (g_self_1.shape, g_neigh_1.shape, g_self_2.shape, g_neigh_2.shape,
                               w_self_3.shape, w_neigh_3.shape), (False,) * 4 + (True,) * 2)
        gs_1, gn_1, gs_2, gn_2, gs_3, gn_3, small = outs
        small = small.reshape(-1)
        n_1, n_2 = g_bias_1.shape[0], g_bias_2.shape[0]
        return (small[n_1 + n_2 + LANES], gs_1, gn_1, small[:n_1], gs_2, gn_2, small[n_1:n_1 + n_2],
                gs_3, gn_3, small[n_1 + n_2:n_1 + n_2 + classes])

    sharded = P(GROUP_AXIS)
    whole = P()
    return jax.shard_map(device_step, mesh=mesh,
                         in_specs=(sharded,) * 7 + (whole,) * 9,
                         out_specs=(whole,) * 10, check_vma=False)
```

```python
import functools

import jax
import jax.numpy as jnp
from jax import lax
from jax.experimental import pallas as pl
from jax.experimental.pallas import tpu as pltpu
from jax.sharding import PartitionSpec as P

GROUP_AXIS = 'gp'
LANES = 128
HALF = 64
DST_TILE = 256
WINDOW = 8
COLS = 1024
BATCH = 8
PLANE = 8
ROWS = 512
VMEM_BYTES = 60 * 1024 * 1024
MESH = pl.DeviceIdType.MESH
F32 = jnp.float32
IDX = jnp.int16
BF16 = jnp.bfloat16


def as_columns(row):
    return jnp.broadcast_to(row, (LANES, LANES)).T


def adjacency_kernel(n_own, starts, parts, dst_ref, col_ref, own_ref, rec_ref):
    part, tile = parts[0], pl.program_id(0)
    first = lax.div(starts[tile], LANES)
    last = lax.div(starts[tile + 1] + LANES - 1, LANES)
    n_recv = rec_ref.shape[1]
    dst_iota = lax.broadcasted_iota(jnp.int32, (DST_TILE, LANES), 0) + tile * DST_TILE
    lanes = lax.broadcasted_iota(jnp.int32, (WINDOW * LANES, LANES), 1).astype(IDX)

    def window_step(w, add):
        rows = first + w * WINDOW
        dst = dst_ref[pl.ds(rows, WINDOW), :]
        col = col_ref[pl.ds(rows, WINDOW), :]
        mine = (col >= n_own + part * n_recv) & (col < n_own + (part + 1) * n_recv)
        col = jnp.where(col < n_own, col, jnp.where(mine, col - part * n_recv, -1))
        to_dst = jnp.concatenate([(dst_iota == dst[k:k + 1, :]).astype(BF16) for k in range(WINDOW)], axis=1)
        columns = jnp.concatenate([as_columns(col[k:k + 1, :]) for k in range(WINDOW)], axis=0).astype(IDX)

        def fill(out_ref, base):
            def block_step(b, carry):
                offset = b * COLS
                shifted = columns - (base + offset).astype(IDX)
                for c in range(0, COLS, 2 * LANES):
                    hot = jnp.concatenate([jnp.where(shifted == lanes + IDX(c + j * LANES), BF16(1), BF16(0))
                                           for j in range(2)], axis=1)
                    counts = jnp.dot(to_dst, hot, preferred_element_type=F32)
                    at = (slice(None), pl.ds(pl.multiple_of(offset + c, 2 * LANES), 2 * LANES))
                    if add:
                        counts = counts + out_ref[at].astype(F32)
                    out_ref[at] = counts.astype(BF16)
                return carry

            lax.fori_loop(0, out_ref.shape[1] // COLS, block_step, 0)

        fill(own_ref, 0)
        fill(rec_ref, n_own)

    window_step(0, False)

    def more(w, carry):
        window_step(w, True)
        return carry

    lax.fori_loop(1, lax.div(last - first + WINDOW - 1, WINDOW), more, 0)


def adjacency(part, starts, dst_idx, columns, n_own, n_recv):
    def rows_of(index):
        padding = jnp.full((WINDOW * LANES,), -1, jnp.int32)
        return jnp.concatenate([index, padding]).reshape(-1, LANES)

    rows = dst_idx.shape[0] // LANES + WINDOW
    grid_spec = pltpu.PrefetchScalarGridSpec(
        num_scalar_prefetch=2, grid=(n_own // DST_TILE,),
        in_specs=[pl.BlockSpec((rows, LANES), lambda i, *_: (0, 0))] * 2,
        out_specs=[pl.BlockSpec((DST_TILE, n_own), lambda i, *_: (i, 0)),
                   pl.BlockSpec((DST_TILE, n_recv), lambda i, *_: (i, 0))])
    return pl.pallas_call(
        functools.partial(adjacency_kernel, n_own), grid_spec=grid_spec,
        out_shape=[jax.ShapeDtypeStruct((n_own, n_own), BF16), jax.ShapeDtypeStruct((n_own, n_recv), BF16)],
        compiler_params=pltpu.CompilerParams(vmem_limit_bytes=VMEM_BYTES),
        cost_estimate=pl.CostEstimate(flops=30 * 10**9, bytes_accessed=40 * 10**6, transcendentals=0),
        name='adjacency',
    )(starts, jnp.reshape(part, (1,)).astype(jnp.int32), rows_of(dst_idx), rows_of(columns))


def pick_kernel(list_ref, rows_ref, out_ref):
    n_rows = rows_ref.shape[0]
    lane_iota = lax.broadcasted_iota(jnp.int32, (LANES, LANES), 1)

    def hot(row):
        columns = as_columns(row)
        return jnp.concatenate(
            [(columns == lane_iota + j * LANES).astype(BF16) for j in range(n_rows // LANES)], axis=1)

    all_hot = jnp.concatenate([hot(list_ref[b:b + 1, :]) for b in range(BATCH)], axis=0)
    picked = jnp.dot(all_hot, rows_ref[...], preferred_element_type=F32).astype(BF16)
    for b in range(BATCH):
        out_ref[b] = picked[b * LANES:(b + 1) * LANES]


def pick(lists, rows):
    group, _ = lists.shape
    n_rows, width = rows.shape
    return pl.pallas_call(
        pick_kernel, grid=(group // BATCH,),
        in_specs=[pl.BlockSpec((BATCH, LANES), lambda i: (i, 0)),
                  pl.BlockSpec((n_rows, width), lambda i: (0, 0))],
        out_specs=pl.BlockSpec((BATCH, LANES, width), lambda i: (i, 0, 0)),
        out_shape=jax.ShapeDtypeStruct((group, LANES, width), BF16),
        compiler_params=pltpu.CompilerParams(vmem_limit_bytes=VMEM_BYTES),
        cost_estimate=pl.CostEstimate(flops=2 * group * LANES * n_rows * width, bytes_accessed=4 * 10**6,
                                      transcendentals=0),
        name='pick',
    )(lists, rows)


def put_back_kernel(list_ref, sent_ref, add_ref, out_ref):
    n_rows = out_ref.shape[0]
    row_iota = lax.broadcasted_iota(jnp.int32, (n_rows, LANES), 0)

    @pl.when(pl.program_id(0) == 0)
    def _():
        out_ref[...] = add_ref[...]

    hot = jnp.concatenate([(row_iota == list_ref[b:b + 1, :]).astype(BF16) for b in range(BATCH)], axis=1)
    rows = jnp.concatenate([sent_ref[b] for b in range(BATCH)], axis=0)
    out_ref[...] += jnp.dot(hot, rows, preferred_element_type=F32)


def put_back(lists, sent, add):
    group, _ = lists.shape
    n_rows, width = add.shape
    return pl.pallas_call(
        put_back_kernel, grid=(group // BATCH,),
        in_specs=[pl.BlockSpec((BATCH, LANES), lambda i: (i, 0)),
                  pl.BlockSpec((BATCH, LANES, width), lambda i: (i, 0, 0)),
                  pl.BlockSpec((n_rows, width), lambda i: (0, 0))],
        out_specs=pl.BlockSpec((n_rows, width), lambda i: (0, 0)),
        out_shape=jax.ShapeDtypeStruct((n_rows, width), F32),
        compiler_params=pltpu.CompilerParams(vmem_limit_bytes=VMEM_BYTES),
        cost_estimate=pl.CostEstimate(flops=2 * group * LANES * n_rows * width, bytes_accessed=8 * 10**6,
                                      transcendentals=0),
        name='put_back',
    )(lists, sent, add)


def gather_in_kernel(adj_ref, rows_ref, add_ref, out_ref):
    out_ref[...] = add_ref[...] + jnp.dot(adj_ref[...], rows_ref[...], preferred_element_type=F32)


def gather_in(adj_rec, rows, add):
    n_own, n_recv = adj_rec.shape
    width = rows.shape[1]
    return pl.pallas_call(
        gather_in_kernel, grid=(n_own // DST_TILE,),
        in_specs=[pl.BlockSpec((DST_TILE, n_recv), lambda i: (i, 0)),
                  pl.BlockSpec((n_recv, width), lambda i: (0, 0)),
                  pl.BlockSpec((DST_TILE, width), lambda i: (i, 0))],
        out_specs=pl.BlockSpec((DST_TILE, width), lambda i: (i, 0)),
        out_shape=jax.ShapeDtypeStruct((n_own, width), F32),
        compiler_params=pltpu.CompilerParams(vmem_limit_bytes=VMEM_BYTES),
        cost_estimate=pl.CostEstimate(flops=2 * n_own * n_recv * width, bytes_accessed=20 * 10**6, transcendentals=0),
        name='gather_in',
    )(adj_rec, rows, add)


def spread_out_kernel(adj_ref, rows_ref, out_ref):
    out_ref[...] = lax.dot_general(adj_ref[...], rows_ref[...], (((0,), (0,)), ((), ())),
                                   preferred_element_type=F32).astype(BF16)


def spread_out(adj_rec, rows):
    n_own, n_recv = adj_rec.shape
    width = rows.shape[1]
    return pl.pallas_call(
        spread_out_kernel, grid=(n_recv // 512,),
        in_specs=[pl.BlockSpec((n_own, 512), lambda i: (0, i)),
                  pl.BlockSpec((n_own, width), lambda i: (0, 0))],
        out_specs=pl.BlockSpec((512, width), lambda i: (i, 0)),
        out_shape=jax.ShapeDtypeStruct((n_recv, width), BF16),
        compiler_params=pltpu.CompilerParams(vmem_limit_bytes=VMEM_BYTES),
        cost_estimate=pl.CostEstimate(flops=2 * n_own * n_recv * width, bytes_accessed=20 * 10**6, transcendentals=0),
        name='spread_out',
    )(adj_rec, rows)


def plane_order(me):
    z = lax.div(me, PLANE)
    near, far, mirror = z + 1 - 2 * lax.rem(z, 2), lax.rem(z + 2, 4), 3 - z
    inner = lax.div(lax.rem(z, 3) + 1, 2)
    sending = [inner * far + (1 - inner) * near, inner * mirror + (1 - inner) * far,
               inner * near + (1 - inner) * mirror, z]
    return sending, [z, near, far, mirror]


def meet_all(barrier, me, group):
    def signal(step, carry):
        pl.semaphore_signal(barrier, inc=1, device_id=(lax.rem(me + step, group),), device_id_type=MESH)
        return carry

    lax.fori_loop(1, group, signal, 0)


class Swap:
    def __init__(self, me, outbox, inbox, send, recv):
        self.me, self.outbox, self.inbox, self.send, self.recv = me, outbox, inbox, send, recv

    def copy(self, peer, slot):
        return pltpu.make_async_remote_copy(
            src_ref=self.outbox.at[peer], dst_ref=self.inbox.at[slot], send_sem=self.send.at[peer],
            recv_sem=self.recv.at[slot], device_id=(peer,), device_id_type=MESH)

    def others(self, plane, own):
        if own:
            return [plane * PLANE + lax.rem(self.me + step, PLANE) for step in range(1, PLANE)]
        return [plane * PLANE + step for step in range(PLANE)]

    def send_plane(self, plane, own):
        for peer in self.others(plane, own):
            self.copy(peer, self.me).start()
        if own:
            self.inbox[self.me] = self.outbox[self.me]

    def receive_plane(self, plane, own):
        for peer in self.others(plane, own):
            self.copy(peer, peer).wait_recv()
        block = self.inbox[pl.ds(plane * PLANE, PLANE)]
        return block.reshape(block.shape[0] * block.shape[1], block.shape[2])

    def finish(self, planes):
        for k, plane in enumerate(planes):
            for peer in self.others(plane, k == len(planes) - 1):
                self.copy(peer, self.me).wait_send()


def fetch_adjacency(own_hbm, rec_hbm, own_ref, rec_ref, planes, sems):
    span = rec_ref.shape[2]
    own = pltpu.make_async_copy(own_hbm, own_ref, sems.at[len(planes)])
    recs = [pltpu.make_async_copy(rec_hbm.at[:, pl.ds(pl.multiple_of(plane * span, span), span)], rec_ref.at[k],
                                  sems.at[k]) for k, plane in enumerate(planes)]
    return own, recs


def exchange_in_kernel(group, list_ref, rows_ref, own_hbm, rec_hbm, out_ref,
                       outbox, inbox, own_ref, rec_ref, send, recv, sems):
    me = lax.axis_index(GROUP_AXIS)
    planes, arriving = plane_order(me)
    barrier = pltpu.get_barrier_semaphore()
    meet_all(barrier, me, group)
    own_copy, rec_copies = fetch_adjacency(own_hbm, rec_hbm, own_ref, rec_ref, arriving, sems)
    for item in [own_copy] + rec_copies:
        item.start()
    swap = Swap(me, outbox, inbox, send, recv)
    n_rows = rows_ref.shape[0]
    lanes = lax.broadcasted_iota(jnp.int32, (LANES, LANES), 1).astype(IDX)
    met = False
    for k, plane in enumerate(planes):
        def pick_one(b, carry):
            columns = as_columns(list_ref[pl.ds(plane * PLANE + b, 1), :]).astype(IDX)
            hot = jnp.concatenate([jnp.where(columns == lanes + IDX(j * LANES), BF16(1), BF16(0))
                                   for j in range(n_rows // LANES)], axis=1)
            return hot

        hot = jnp.concatenate([pick_one(b, 0) for b in range(PLANE)], axis=0)
        picked = jnp.dot(hot, rows_ref[...], preferred_element_type=F32).astype(BF16)
        outbox[pl.ds(plane * PLANE, PLANE)] = picked.reshape(PLANE, LANES, picked.shape[1])
        if not met:
            pl.semaphore_wait(barrier, group - 1)
            met = True
        swap.send_plane(plane, k == len(planes) - 1)
    own_copy.wait()

    def own_step(i, carry):
        at = pl.ds(pl.multiple_of(i * ROWS, ROWS), ROWS)
        out_ref[at, :] = jnp.dot(own_ref[at, :], rows_ref[...], preferred_element_type=F32)
        return carry

    lax.fori_loop(0, n_rows // ROWS, own_step, 0)
    for k, plane in enumerate(arriving):
        rec_copies[k].wait()
        block = swap.receive_plane(plane, k == 0)

        def rec_step(i, carry):
            at = pl.ds(pl.multiple_of(i * ROWS, ROWS), ROWS)
            out_ref[at, :] += jnp.dot(rec_ref[k, at, :], block, preferred_element_type=F32)
            return carry

        lax.fori_loop(0, n_rows // ROWS, rec_step, 0)
    swap.finish(planes)


def exchange_back_kernel(group, list_ref, grad_ref, add_ref, own_hbm, rec_hbm, out_ref,
                         outbox, inbox, own_ref, rec_ref, send, recv, sems):
    me = lax.axis_index(GROUP_AXIS)
    planes, arriving = plane_order(me)
    barrier = pltpu.get_barrier_semaphore()
    meet_all(barrier, me, group)
    own_copy, rec_copies = fetch_adjacency(own_hbm, rec_hbm, own_ref, rec_ref, planes, sems)
    for item in rec_copies + [own_copy]:
        item.start()
    swap = Swap(me, outbox, inbox, send, recv)
    n_rows, width = grad_ref.shape
    met = False
    for k, plane in enumerate(planes):
        rec_copies[k].wait()
        part = lax.dot_general(rec_ref[k], grad_ref[...], (((0,), (0,)), ((), ())), preferred_element_type=F32)
        outbox[pl.ds(plane * PLANE, PLANE)] = part.astype(BF16).reshape(PLANE, LANES, width)
        if not met:
            pl.semaphore_wait(barrier, group - 1)
            met = True
        swap.send_plane(plane, k == len(planes) - 1)
    own_copy.wait()

    def own_step(i, carry):
        at = pl.ds(pl.multiple_of(i * ROWS, ROWS), ROWS)
        out_ref[at, :] = add_ref[at, :] + lax.dot_general(
            own_ref[:, at], grad_ref[...], (((0,), (0,)), ((), ())), preferred_element_type=F32)
        return carry

    lax.fori_loop(0, n_rows // ROWS, own_step, 0)
    row_iota = lax.broadcasted_iota(jnp.int32, (ROWS, LANES), 0)
    for k, plane in enumerate(arriving):
        block = swap.receive_plane(plane, k == 0)
        names = list_ref[pl.ds(pl.multiple_of(plane * PLANE, PLANE), PLANE), :]

        def rec_step(i, carry):
            at = pl.ds(pl.multiple_of(i * ROWS, ROWS), ROWS)
            rows = (row_iota + i * ROWS).astype(IDX)
            hot = jnp.concatenate(
                [jnp.where(rows == jnp.broadcast_to(names[b:b + 1, :], (ROWS, LANES)).astype(IDX), BF16(1), BF16(0))
                 for b in range(PLANE)], axis=1)
            out_ref[at, :] += jnp.dot(hot, block, preferred_element_type=F32)
            return carry

        lax.fori_loop(0, n_rows // ROWS, rec_step, 0)
    swap.finish(planes)


def exchange(body, which, name, lists, arrays, adj_own, adj_rec):
    group = lists.shape[0]
    n_rows, width = arrays[0].shape
    planes = group // PLANE
    vmem, anywhere = pl.BlockSpec(memory_space=pltpu.VMEM), pl.BlockSpec(memory_space=pl.ANY)
    box = pltpu.VMEM((group, LANES, width), BF16)
    return pl.pallas_call(
        functools.partial(body, group),
        in_specs=[vmem] * (1 + len(arrays)) + [anywhere] * 2, out_specs=vmem,
        out_shape=jax.ShapeDtypeStruct((n_rows, width), F32),
        scratch_shapes=[box, box, pltpu.VMEM(adj_own.shape, BF16),
                        pltpu.VMEM((planes, n_rows, adj_rec.shape[1] // planes), BF16),
                        pltpu.SemaphoreType.DMA((group,)), pltpu.SemaphoreType.DMA((group,)),
                        pltpu.SemaphoreType.DMA((planes + 1,))],
        compiler_params=pltpu.CompilerParams(collective_id=which, has_side_effects=True, vmem_limit_bytes=VMEM_BYTES),
        cost_estimate=pl.CostEstimate(flops=2 * 2 * n_rows * adj_rec.shape[1] * width, bytes_accessed=30 * 10**6,
                                      transcendentals=0),
        name=name,
    )(lists, *arrays, adj_own, adj_rec)


def add_up_kernel(n_chips, rows, *refs):
    parts, (out_ref, packed, partner_half, mine, inbox, total, gathered, send, recv) = refs[:-9], refs[-9:]
    me = lax.axis_index(GROUP_AXIS)
    core, chip = lax.rem(me, 2), lax.div(me, 2)
    partner = me + 1 - 2 * core

    def twin(step):
        return 2 * lax.rem(chip + step, n_chips) + core

    barrier = pltpu.get_barrier_semaphore()
    pl.semaphore_signal(barrier, inc=1, device_id=(partner,), device_id_type=MESH)
    for step in range(1, n_chips):
        pl.semaphore_signal(barrier, inc=1, device_id=(twin(step),), device_id_type=MESH)

    at = 0
    for ref in parts:
        count, width = ref.shape
        for j in range(width // LANES):
            packed[at:at + count, :] = ref[:, j * LANES:(j + 1) * LANES]
            at += count
    packed[at:, :] = jnp.zeros((packed.shape[0] - at, LANES), F32)
    half = n_chips * rows

    def half_of(which):
        return pl.ds(pl.multiple_of(which * half, 8), half)

    def copy(src, dst, slot, device):
        return pltpu.make_async_remote_copy(
            src_ref=src, dst_ref=dst, send_sem=send.at[slot], recv_sem=recv.at[slot],
            device_id=(device,), device_id_type=MESH)

    pl.semaphore_wait(barrier, n_chips)
    first = copy(packed.at[half_of(1 - core)], partner_half, 0, partner)
    first.start()
    first.wait()
    mine[...] = (packed[half_of(core), :] + partner_half[...]).reshape(n_chips, rows, LANES)
    sends = []
    for step in range(1, n_chips):
        sends.append(copy(mine.at[lax.rem(chip + step, n_chips)], inbox.at[step], step, twin(step)))
        sends[-1].start()
    value = mine[chip]
    for step in range(1, n_chips):
        sends[step - 1].wait_recv()
        value = value + inbox[step]
    total[...] = value
    for item in sends:
        item.wait_send()
    spread = []
    for step in range(1, n_chips):
        spread.append(copy(total, gathered.at[core, chip], n_chips + step, twin(step)))
        spread[-1].start()
    gathered[core, chip] = value
    for item in spread:
        item.wait()
    last = copy(gathered.at[core], gathered.at[core], 2 * n_chips, partner)
    last.start()
    last.wait()
    out_ref[...] = gathered[...].reshape(2 * half, LANES)


def add_up(parts, group):
    n_chips = group // 2
    used = sum(p.size for p in parts) // LANES
    rows = -(-used // (group * 8)) * 8
    total = group * rows
    chunk = (rows, LANES)
    return pl.pallas_call(
        functools.partial(add_up_kernel, n_chips, rows),
        in_specs=[pl.BlockSpec(memory_space=pltpu.VMEM)] * len(parts),
        out_specs=pl.BlockSpec(memory_space=pltpu.VMEM),
        out_shape=jax.ShapeDtypeStruct((total, LANES), F32),
        scratch_shapes=[pltpu.VMEM((total, LANES), F32), pltpu.VMEM((total // 2, LANES), F32),
                        pltpu.VMEM((n_chips,) + chunk, F32), pltpu.VMEM((n_chips,) + chunk, F32),
                        pltpu.VMEM(chunk, F32), pltpu.VMEM((2, n_chips) + chunk, F32),
                        pltpu.SemaphoreType.DMA((2 * n_chips + 1,)), pltpu.SemaphoreType.DMA((2 * n_chips + 1,))],
        compiler_params=pltpu.CompilerParams(collective_id=0, has_side_effects=True),
        name='add_up',
    )(*parts)


def unpack_kernel(flipped, packed_ref, *out_refs):
    at = 0
    for ref, flip in zip(out_refs[:-1], flipped):
        count, width = ref.shape[::-1] if flip else ref.shape
        pieces = []
        for j in range(width // LANES):
            pieces.append(packed_ref[at:at + count, :])
            at += count
        if flip:
            short = jnp.zeros((LANES - count, LANES), F32)
            for j, piece in enumerate(pieces):
                ref[j * LANES:(j + 1) * LANES, :] = jnp.concatenate([piece, short], axis=0).T[:, :count]
        else:
            ref[...] = jnp.concatenate(pieces, axis=1)
    out_refs[-1][...] = packed_ref[at:at + out_refs[-1].shape[0], :]


def unpack(packed, shapes, flipped):
    return pl.pallas_call(
        functools.partial(unpack_kernel, flipped),
        in_specs=[pl.BlockSpec(memory_space=pltpu.VMEM)],
        out_specs=[pl.BlockSpec(memory_space=pltpu.VMEM)] * (len(shapes) + 1),
        out_shape=[jax.ShapeDtypeStruct(shape, F32) for shape in shapes + ((8, LANES),)],
        name='unpack',
    )(packed)


def before(count):
    index = jnp.arange(count, dtype=jnp.int32)
    return index[:, None] < index[None, :]


def rank_in_row(flags):
    tri = before(flags.shape[1]).astype(BF16)
    return jnp.dot(flags.astype(BF16), tri, preferred_element_type=F32).astype(jnp.int32)


def exchange_plan(send_idx, src_idx, train_mask, n_own):
    group, slots = send_idx.shape
    halo = src_idx - n_own
    peer, slot = halo // slots, halo % slots
    from_peer = ((halo >= 0)[:, None] & (peer[:, None] == jnp.arange(group, dtype=jnp.int32)[None, :])).astype(BF16)
    at_slot = (slot[:, None] == jnp.arange(slots, dtype=jnp.int32)[None, :]).astype(BF16)
    needed = jnp.einsum('eg,es->gs', from_peer, at_slot, preferred_element_type=F32) > 0
    rank = rank_in_row(needed)
    my_rounds = (jnp.max(jnp.where(needed, rank, 0)) // LANES + 1).astype(jnp.int32)
    upper = rank // LANES * group + jnp.arange(group, dtype=jnp.int32)[:, None]
    split = jnp.concatenate([upper, rank % LANES], axis=1).astype(BF16)
    found = jnp.dot(from_peer, split, preferred_element_type=F32)
    found = jnp.sum((found[:, :slots] * LANES + found[:, slots:]) * at_slot.astype(F32), axis=1).astype(jnp.int32)
    columns = jnp.where(halo >= 0, n_own + found, src_idx)
    my_count = jnp.sum(train_mask).astype(jnp.int32)
    extras = jnp.where(jnp.arange(LANES) == 0, my_rounds, my_count)
    message = jnp.concatenate([jnp.where(needed, rank, -1), jnp.broadcast_to(extras, (group, LANES))], axis=1)
    message = lax.all_to_all(message, GROUP_AXIS, 0, 0, tiled=True)
    asked, rounds = message[:, :slots], jnp.max(message[:, slots])
    count = jnp.sum(message[:, slots + 1]).astype(F32)
    k = jnp.arange(slots, dtype=jnp.int32)
    chosen = asked[:, None, :] == k[None, :, None]
    lists = jnp.sum(jnp.where(chosen, send_idx[:, None, :] + 1, 0), axis=2) - 1
    return columns, rounds, count, lists.reshape(group, slots // LANES, LANES).transpose(1, 0, 2)


def weight_grads(h_in, neigh_mean, d_pre, d_pre_bf):
    g_self = jnp.einsum('nd,ne->de', h_in, d_pre_bf, preferred_element_type=jnp.float32)
    g_neigh = jnp.einsum('nd,ne->de', neigh_mean, d_pre_bf, preferred_element_type=jnp.float32)
    return g_self, g_neigh, jnp.sum(d_pre, axis=0)


def input_grads(d_pre_bf, w_self, w_neigh):
    d_self = jnp.einsum('ne,de->nd', d_pre_bf, w_self, preferred_element_type=jnp.float32)
    d_mean = jnp.einsum('ne,de->nd', d_pre_bf, w_neigh, preferred_element_type=jnp.float32)
    return d_self, d_mean


def head_grad(logits, labels, train_mask):
    log_prob = jax.nn.log_softmax(logits, axis=-1)
    is_label = labels[:, None] == jnp.arange(logits.shape[1], dtype=jnp.int32)[None, :]
    picked = jnp.sum(jnp.where(is_label, log_prob, 0.0), axis=-1)
    d_logits = (jnp.exp(log_prob) - is_label.astype(jnp.float32)) * train_mask[:, None]
    return jnp.sum(train_mask * -picked), d_logits


def solution(mesh):
    def device_step(features, labels, train_mask, send_idx, src_idx, dst_idx, inv_deg,
                    w_self_1, w_neigh_1, bias_1, w_self_2, w_neigh_2, bias_2,
                    w_self_3, w_neigh_3, bias_3):
        n_own = features.shape[0]
        group, slots = send_idx.shape
        columns, rounds, count, lists = exchange_plan(send_idx, src_idx, train_mask, n_own)
        n_recv = group * LANES
        starts = jnp.sum(dst_idx[None, :] < (jnp.arange(n_own // DST_TILE + 1) * DST_TILE)[:, None],
                         axis=1, dtype=jnp.int32)

        def adjacency_of(part):
            return adjacency(part, starts, dst_idx, columns, n_own, n_recv)

        adj_own, adj_first = adjacency_of(0)

        def swap(rows):
            return lax.all_to_all(rows, GROUP_AXIS, 0, 0, tiled=True)

        def edge_sum(hidden, which):
            def more(part, total):
                received = swap(pick(lists[part], hidden))
                return gather_in(adjacency_of(part)[1], received.reshape(n_recv, -1), total)

            summed = exchange(exchange_in_kernel, which, 'exchange_in', lists[0], (hidden,), adj_own, adj_first)
            return lax.fori_loop(1, rounds, more, summed)

        def layer(hidden, w_self, w_neigh, bias, which):
            neigh_mean = (edge_sum(hidden, which) * inv_deg[:, None]).astype(BF16)
            pre_act = (jnp.dot(hidden, w_self, preferred_element_type=jnp.float32)
                       + jnp.dot(neigh_mean, w_neigh, preferred_element_type=jnp.float32) + bias)
            return neigh_mean, pre_act

        def back_to_owners(d_sum, d_self, which):
            def more(part, total):
                returned = swap(spread_out(adjacency_of(part)[1], d_sum).reshape(group, LANES, -1))
                return put_back(lists[part], returned, total)

            d_hidden = exchange(exchange_back_kernel, which, 'exchange_back', lists[0], (d_sum, d_self),
                                adj_own, adj_first)
            return lax.fori_loop(1, rounds, more, d_hidden)

        mean_1, pre_1 = layer(features, w_self_1, w_neigh_1, bias_1, 1)
        hidden_1 = jax.nn.relu(pre_1).astype(jnp.bfloat16)
        mean_2, pre_2 = layer(hidden_1, w_self_2, w_neigh_2, bias_2, 2)
        hidden_2 = jax.nn.relu(pre_2).astype(jnp.bfloat16)
        classes = w_neigh_3.shape[1]

        def split(x):
            high = x.astype(BF16)
            low = (x - high.astype(F32)).astype(BF16)
            pad = ((0, 0), (0, HALF - classes))
            return jnp.concatenate([jnp.pad(high, pad), jnp.pad(low, pad)], axis=1)

        def join(x):
            return x[:, :classes] + x[:, HALF:HALF + classes]

        projected = split(jnp.dot(hidden_2, w_neigh_3, preferred_element_type=F32))
        logits = (jnp.dot(hidden_2, w_self_3, preferred_element_type=F32)
                  + join(edge_sum(projected, 3)) * inv_deg[:, None] + bias_3)
        loss_sum, d_logits = head_grad(logits, labels, train_mask)

        d_pre_3 = d_logits / count
        d_bf_3 = d_pre_3.astype(jnp.bfloat16)
        g_self_3 = jnp.einsum('ne,nd->ed', d_bf_3, hidden_2, preferred_element_type=F32)
        g_bias_3 = jnp.sum(d_pre_3, axis=0)
        d_projected = join(back_to_owners(split(d_bf_3.astype(F32) * inv_deg[:, None]),
                                          jnp.zeros((n_own, 2 * HALF), F32), 4)).astype(BF16)
        g_neigh_3 = jnp.einsum('ne,nd->ed', d_projected, hidden_2, preferred_element_type=F32)
        d_hidden_2 = (jnp.einsum('ne,de->nd', d_bf_3, w_self_3, preferred_element_type=F32)
                      + jnp.einsum('ne,de->nd', d_projected, w_neigh_3, preferred_element_type=F32))
        d_pre_2 = jnp.where(pre_2 > 0, d_hidden_2, 0.0)
        d_bf_2 = d_pre_2.astype(jnp.bfloat16)
        g_self_2, g_neigh_2, g_bias_2 = weight_grads(hidden_1, mean_2, d_pre_2, d_bf_2)
        d_self_2, d_mean_2 = input_grads(d_bf_2, w_self_2, w_neigh_2)
        d_pre_1 = jnp.where(pre_1 > 0, back_to_owners((d_mean_2 * inv_deg[:, None]).astype(BF16), d_self_2, 5), 0.0)
        d_bf_1 = d_pre_1.astype(jnp.bfloat16)
        g_self_1, g_neigh_1, g_bias_1 = weight_grads(features, mean_1, d_pre_1, d_bf_1)

        small = jnp.concatenate([g_bias_1, g_bias_2, jnp.pad(g_bias_3, (0, LANES - classes)),
                                 jnp.full((LANES,), loss_sum / count)]).reshape(-1, LANES)
        small = jnp.pad(small, ((0, 8 - small.shape[0]), (0, 0)))
        summed = add_up((g_self_1, g_neigh_1, g_self_2, g_neigh_2, g_self_3, g_neigh_3, small), group)
        outs = unpack(summed, (g_self_1.shape, g_neigh_1.shape, g_self_2.shape, g_neigh_2.shape,
                               w_self_3.shape, w_neigh_3.shape), (False,) * 4 + (True,) * 2)
        gs_1, gn_1, gs_2, gn_2, gs_3, gn_3, small = outs
        small = small.reshape(-1)
        n_1, n_2 = g_bias_1.shape[0], g_bias_2.shape[0]
        return (small[n_1 + n_2 + LANES], gs_1, gn_1, small[:n_1], gs_2, gn_2, small[n_1:n_1 + n_2],
                gs_3, gn_3, small[n_1 + n_2:n_1 + n_2 + classes])

    sharded = P(GROUP_AXIS)
    whole = P()
    return jax.shard_map(device_step, mesh=mesh,
                         in_specs=(sharded,) * 7 + (whole,) * 9,
                         out_specs=(whole,) * 10, check_vma=False)
```

```python
import functools

import jax
import jax.numpy as jnp
from jax import lax
from jax.experimental import pallas as pl
from jax.experimental.pallas import tpu as pltpu
from jax.sharding import PartitionSpec as P

GROUP_AXIS = 'gp'
LANES = 128
HALF = 64
DST_TILE = 256
WINDOW = 8
COLS = 1024
BATCH = 8
PLANE = 8
ROWS = 512
VMEM_BYTES = 60 * 1024 * 1024
MESH = pl.DeviceIdType.MESH
F32 = jnp.float32
IDX = jnp.int16
BF16 = jnp.bfloat16


def as_columns(row):
    return jnp.broadcast_to(row, (LANES, LANES)).T


def adjacency_kernel(n_own, starts, parts, dst_ref, col_ref, own_ref, rec_ref):
    part, tile = parts[0], pl.program_id(0)
    first = lax.div(starts[tile], LANES)
    last = lax.div(starts[tile + 1] + LANES - 1, LANES)
    n_recv = rec_ref.shape[1]
    dst_iota = lax.broadcasted_iota(jnp.int32, (DST_TILE, LANES), 0) + tile * DST_TILE
    lanes = lax.broadcasted_iota(jnp.int32, (WINDOW * LANES, LANES), 1).astype(IDX)

    def window_step(w, add):
        rows = first + w * WINDOW
        dst = dst_ref[pl.ds(rows, WINDOW), :]
        col = col_ref[pl.ds(rows, WINDOW), :]
        mine = (col >= n_own + part * n_recv) & (col < n_own + (part + 1) * n_recv)
        col = jnp.where(col < n_own, col, jnp.where(mine, col - part * n_recv, -1))
        to_dst = jnp.concatenate([(dst_iota == dst[k:k + 1, :]).astype(BF16) for k in range(WINDOW)], axis=1)
        columns = jnp.concatenate([as_columns(col[k:k + 1, :]) for k in range(WINDOW)], axis=0).astype(IDX)

        def fill(out_ref, base):
            def block_step(b, carry):
                offset = b * COLS
                shifted = columns - (base + offset).astype(IDX)
                for c in range(0, COLS, 2 * LANES):
                    hot = jnp.concatenate([jnp.where(shifted == lanes + IDX(c + j * LANES), BF16(1), BF16(0))
                                           for j in range(2)], axis=1)
                    counts = jnp.dot(to_dst, hot, preferred_element_type=F32)
                    at = (slice(None), pl.ds(pl.multiple_of(offset + c, 2 * LANES), 2 * LANES))
                    if add:
                        counts = counts + out_ref[at].astype(F32)
                    out_ref[at] = counts.astype(BF16)
                return carry

            lax.fori_loop(0, out_ref.shape[1] // COLS, block_step, 0)

        fill(own_ref, 0)
        fill(rec_ref, n_own)

    window_step(0, False)

    def more(w, carry):
        window_step(w, True)
        return carry

    lax.fori_loop(1, lax.div(last - first + WINDOW - 1, WINDOW), more, 0)


def adjacency(part, starts, dst_idx, columns, n_own, n_recv):
    def rows_of(index):
        padding = jnp.full((WINDOW * LANES,), -1, jnp.int32)
        return jnp.concatenate([index, padding]).reshape(-1, LANES)

    rows = dst_idx.shape[0] // LANES + WINDOW
    grid_spec = pltpu.PrefetchScalarGridSpec(
        num_scalar_prefetch=2, grid=(n_own // DST_TILE,),
        in_specs=[pl.BlockSpec((rows, LANES), lambda i, *_: (0, 0))] * 2,
        out_specs=[pl.BlockSpec((DST_TILE, n_own), lambda i, *_: (i, 0)),
                   pl.BlockSpec((DST_TILE, n_recv), lambda i, *_: (i, 0))])
    return pl.pallas_call(
        functools.partial(adjacency_kernel, n_own), grid_spec=grid_spec,
        out_shape=[jax.ShapeDtypeStruct((n_own, n_own), BF16), jax.ShapeDtypeStruct((n_own, n_recv), BF16)],
        compiler_params=pltpu.CompilerParams(vmem_limit_bytes=VMEM_BYTES),
        cost_estimate=pl.CostEstimate(flops=30 * 10**9, bytes_accessed=40 * 10**6, transcendentals=0),
        name='adjacency',
    )(starts, jnp.reshape(part, (1,)).astype(jnp.int32), rows_of(dst_idx), rows_of(columns))


def pick_kernel(list_ref, rows_ref, out_ref):
    n_rows = rows_ref.shape[0]
    lane_iota = lax.broadcasted_iota(jnp.int32, (LANES, LANES), 1)

    def hot(row):
        columns = as_columns(row)
        return jnp.concatenate(
            [(columns == lane_iota + j * LANES).astype(BF16) for j in range(n_rows // LANES)], axis=1)

    all_hot = jnp.concatenate([hot(list_ref[b:b + 1, :]) for b in range(BATCH)], axis=0)
    picked = jnp.dot(all_hot, rows_ref[...], preferred_element_type=F32).astype(BF16)
    for b in range(BATCH):
        out_ref[b] = picked[b * LANES:(b + 1) * LANES]


def pick(lists, rows):
    group, _ = lists.shape
    n_rows, width = rows.shape
    return pl.pallas_call(
        pick_kernel, grid=(group // BATCH,),
        in_specs=[pl.BlockSpec((BATCH, LANES), lambda i: (i, 0)),
                  pl.BlockSpec((n_rows, width), lambda i: (0, 0))],
        out_specs=pl.BlockSpec((BATCH, LANES, width), lambda i: (i, 0, 0)),
        out_shape=jax.ShapeDtypeStruct((group, LANES, width), BF16),
        compiler_params=pltpu.CompilerParams(vmem_limit_bytes=VMEM_BYTES),
        cost_estimate=pl.CostEstimate(flops=2 * group * LANES * n_rows * width, bytes_accessed=4 * 10**6,
                                      transcendentals=0),
        name='pick',
    )(lists, rows)


def put_back_kernel(list_ref, sent_ref, add_ref, out_ref):
    n_rows = out_ref.shape[0]
    row_iota = lax.broadcasted_iota(jnp.int32, (n_rows, LANES), 0)

    @pl.when(pl.program_id(0) == 0)
    def _():
        out_ref[...] = add_ref[...]

    hot = jnp.concatenate([(row_iota == list_ref[b:b + 1, :]).astype(BF16) for b in range(BATCH)], axis=1)
    rows = jnp.concatenate([sent_ref[b] for b in range(BATCH)], axis=0)
    out_ref[...] += jnp.dot(hot, rows, preferred_element_type=F32)


def put_back(lists, sent, add):
    group, _ = lists.shape
    n_rows, width = add.shape
    return pl.pallas_call(
        put_back_kernel, grid=(group // BATCH,),
        in_specs=[pl.BlockSpec((BATCH, LANES), lambda i: (i, 0)),
                  pl.BlockSpec((BATCH, LANES, width), lambda i: (i, 0, 0)),
                  pl.BlockSpec((n_rows, width), lambda i: (0, 0))],
        out_specs=pl.BlockSpec((n_rows, width), lambda i: (0, 0)),
        out_shape=jax.ShapeDtypeStruct((n_rows, width), F32),
        compiler_params=pltpu.CompilerParams(vmem_limit_bytes=VMEM_BYTES),
        cost_estimate=pl.CostEstimate(flops=2 * group * LANES * n_rows * width, bytes_accessed=8 * 10**6,
                                      transcendentals=0),
        name='put_back',
    )(lists, sent, add)


def gather_in_kernel(adj_ref, rows_ref, add_ref, out_ref):
    out_ref[...] = add_ref[...] + jnp.dot(adj_ref[...], rows_ref[...], preferred_element_type=F32)


def gather_in(adj_rec, rows, add):
    n_own, n_recv = adj_rec.shape
    width = rows.shape[1]
    return pl.pallas_call(
        gather_in_kernel, grid=(n_own // DST_TILE,),
        in_specs=[pl.BlockSpec((DST_TILE, n_recv), lambda i: (i, 0)),
                  pl.BlockSpec((n_recv, width), lambda i: (0, 0)),
                  pl.BlockSpec((DST_TILE, width), lambda i: (i, 0))],
        out_specs=pl.BlockSpec((DST_TILE, width), lambda i: (i, 0)),
        out_shape=jax.ShapeDtypeStruct((n_own, width), F32),
        compiler_params=pltpu.CompilerParams(vmem_limit_bytes=VMEM_BYTES),
        cost_estimate=pl.CostEstimate(flops=2 * n_own * n_recv * width, bytes_accessed=20 * 10**6, transcendentals=0),
        name='gather_in',
    )(adj_rec, rows, add)


def spread_out_kernel(adj_ref, rows_ref, out_ref):
    out_ref[...] = lax.dot_general(adj_ref[...], rows_ref[...], (((0,), (0,)), ((), ())),
                                   preferred_element_type=F32).astype(BF16)


def spread_out(adj_rec, rows):
    n_own, n_recv = adj_rec.shape
    width = rows.shape[1]
    return pl.pallas_call(
        spread_out_kernel, grid=(n_recv // 512,),
        in_specs=[pl.BlockSpec((n_own, 512), lambda i: (0, i)),
                  pl.BlockSpec((n_own, width), lambda i: (0, 0))],
        out_specs=pl.BlockSpec((512, width), lambda i: (i, 0)),
        out_shape=jax.ShapeDtypeStruct((n_recv, width), BF16),
        compiler_params=pltpu.CompilerParams(vmem_limit_bytes=VMEM_BYTES),
        cost_estimate=pl.CostEstimate(flops=2 * n_own * n_recv * width, bytes_accessed=20 * 10**6, transcendentals=0),
        name='spread_out',
    )(adj_rec, rows)


def plane_order(me):
    z = lax.div(me, PLANE)
    near, far, mirror = z + 1 - 2 * lax.rem(z, 2), lax.rem(z + 2, 4), 3 - z
    inner = lax.div(lax.rem(z, 3) + 1, 2)
    sending = [inner * far + (1 - inner) * near, inner * mirror + (1 - inner) * far,
               inner * near + (1 - inner) * mirror, z]
    return sending, [z, near, far, mirror]


def meet_all(barrier, me, group):
    def signal(step, carry):
        pl.semaphore_signal(barrier, inc=1, device_id=(lax.rem(me + step, group),), device_id_type=MESH)
        return carry

    lax.fori_loop(1, group, signal, 0)


class Swap:
    def __init__(self, me, outbox, inbox, send, recv):
        self.me, self.outbox, self.inbox, self.send, self.recv = me, outbox, inbox, send, recv

    def copy(self, peer, slot):
        return pltpu.make_async_remote_copy(
            src_ref=self.outbox.at[peer], dst_ref=self.inbox.at[slot], send_sem=self.send.at[peer],
            recv_sem=self.recv.at[slot], device_id=(peer,), device_id_type=MESH)

    def others(self, plane, own):
        if own:
            return [plane * PLANE + lax.rem(self.me + step, PLANE) for step in range(1, PLANE)]
        return [plane * PLANE + step for step in range(PLANE)]

    def send_plane(self, plane, own):
        for peer in self.others(plane, own):
            self.copy(peer, self.me).start()
        if own:
            self.inbox[self.me] = self.outbox[self.me]

    def receive_plane(self, plane, own):
        for peer in self.others(plane, own):
            self.copy(peer, peer).wait_recv()
        block = self.inbox[pl.ds(plane * PLANE, PLANE)]
        return block.reshape(block.shape[0] * block.shape[1], block.shape[2])

    def finish(self, planes):
        for k, plane in enumerate(planes):
            for peer in self.others(plane, k == len(planes) - 1):
                self.copy(peer, self.me).wait_send()


def rows_at(i):
    return pl.ds(pl.multiple_of(i * ROWS, ROWS), ROWS)


def over_rows(n_rows, step, carry=0):
    return lax.fori_loop(0, n_rows // ROWS, step, carry)


def dot(a, b):
    return jnp.dot(a, b, preferred_element_type=F32)


def dot_t(a, b):
    return lax.dot_general(a, b, (((1,), (1,)), ((), ())), preferred_element_type=F32)


def t_dot(a, b):
    return lax.dot_general(a, b, (((0,), (0,)), ((), ())), preferred_element_type=F32)


def split_halves(twice):
    high = twice.astype(BF16)
    low = (twice - high.astype(F32)).astype(BF16)
    return jnp.where(lax.broadcasted_iota(jnp.int32, twice.shape, 1) < HALF, high, low)


def join_halves(x):
    return x + pltpu.roll(x, HALF, 1)


class Exchange:
    def __init__(self, group, list_ref, own_hbm, rec_hbm, outbox, inbox, own_ref, rec_ref, send, recv, sems, back):
        self.me = lax.axis_index(GROUP_AXIS)
        self.group, self.list_ref, self.own_ref, self.rec_ref, self.outbox = group, list_ref, own_ref, rec_ref, outbox
        self.planes, self.arriving = plane_order(self.me)
        self.barrier = pltpu.get_barrier_semaphore()
        meet_all(self.barrier, self.me, group)
        order = self.planes if back else self.arriving
        span = rec_ref.shape[2]
        self.own_copy = pltpu.make_async_copy(own_hbm, own_ref, sems.at[len(order)])
        self.rec_copies = [
            pltpu.make_async_copy(rec_hbm.at[:, pl.ds(pl.multiple_of(plane * span, span), span)], rec_ref.at[k],
                                  sems.at[k]) for k, plane in enumerate(order)]
        for item in self.rec_copies + [self.own_copy] if back else [self.own_copy] + self.rec_copies:
            item.start()
        self.swap = Swap(self.me, outbox, inbox, send, recv)

    def fill(self, k, plane, rows):
        self.outbox[pl.ds(plane * PLANE, PLANE)] = rows.astype(BF16).reshape(PLANE, LANES, rows.shape[1])
        if k == 0:
            pl.semaphore_wait(self.barrier, self.group - 1)
        self.swap.send_plane(plane, k == len(self.planes) - 1)

    def send_picked(self, rows_ref):
        n_rows = rows_ref.shape[0]
        lanes = lax.broadcasted_iota(jnp.int32, (LANES, LANES), 1).astype(IDX)
        for k, plane in enumerate(self.planes):
            hot = []
            for b in range(PLANE):
                columns = as_columns(self.list_ref[pl.ds(plane * PLANE + b, 1), :]).astype(IDX)
                hot.append(jnp.concatenate([jnp.where(columns == lanes + IDX(j * LANES), BF16(1), BF16(0))
                                            for j in range(n_rows // LANES)], axis=1))
            self.fill(k, plane, dot(jnp.concatenate(hot, axis=0), rows_ref[...]))

    def send_spread(self, grad_ref):
        for k, plane in enumerate(self.planes):
            self.rec_copies[k].wait()
            self.fill(k, plane, t_dot(self.rec_ref[k], grad_ref[...]))

    def own_in(self, rows_ref, out_ref):
        self.own_copy.wait()

        def step(i, carry):
            out_ref[rows_at(i), :] = dot(self.own_ref[rows_at(i), :], rows_ref[...])
            return carry

        over_rows(out_ref.shape[0], step)

    def own_back(self, grad_ref, out_ref):
        self.own_copy.wait()

        def step(i, carry):
            out_ref[rows_at(i), :] = t_dot(self.own_ref[:, rows_at(i)], grad_ref[...])
            return carry

        over_rows(out_ref.shape[0], step)

    def arrive_in(self, out_ref):
        for k, plane in enumerate(self.arriving):
            self.rec_copies[k].wait()
            block = self.swap.receive_plane(plane, k == 0)

            def step(i, carry):
                out_ref[rows_at(i), :] += dot(self.rec_ref[k, rows_at(i), :], block)
                return carry

            over_rows(out_ref.shape[0], step)
        self.swap.finish(self.planes)

    def arrive_back(self, out_ref):
        row_iota = lax.broadcasted_iota(jnp.int32, (ROWS, LANES), 0)
        for k, plane in enumerate(self.arriving):
            block = self.swap.receive_plane(plane, k == 0)
            names = self.list_ref[pl.ds(pl.multiple_of(plane * PLANE, PLANE), PLANE), :]

            def step(i, carry):
                rows = (row_iota + i * ROWS).astype(IDX)
                hot = jnp.concatenate(
                    [jnp.where(rows == jnp.broadcast_to(names[b:b + 1, :], (ROWS, LANES)).astype(IDX),
                               BF16(1), BF16(0)) for b in range(PLANE)], axis=1)
                out_ref[rows_at(i), :] += dot(hot, block)
                return carry

            over_rows(out_ref.shape[0], step)
        self.swap.finish(self.planes)


def edges_1_kernel(group, list_ref, x_ref, own_hbm, rec_hbm, out_ref, *scratch):
    exchange = Exchange(group, list_ref, own_hbm, rec_hbm, *scratch, back=False)
    exchange.send_picked(x_ref)
    exchange.own_in(x_ref, out_ref)
    exchange.arrive_in(out_ref)


def layer_step(sums, x, inv, w_self, w_neigh, bias):
    mean = (sums * inv).astype(BF16)
    pre_act = dot(x, w_self) + dot(mean, w_neigh) + bias
    return mean, jnp.maximum(pre_act, 0.0).astype(BF16)


def edges_2_kernel(group, list_ref, sums_ref, x_ref, inv_ref, w_self_ref, w_neigh_ref, bias_ref, own_hbm, rec_hbm,
                   mean_ref, h_ref, out_ref, *scratch):
    exchange = Exchange(group, list_ref, own_hbm, rec_hbm, *scratch, back=False)

    def step(i, carry):
        at = rows_at(i)
        mean_ref[at, :], h_ref[at, :] = layer_step(sums_ref[at, :], x_ref[at, :], inv_ref[at, :], w_self_ref[...],
                                                   w_neigh_ref[...], bias_ref[...])
        return carry

    over_rows(x_ref.shape[0], step)
    exchange.send_picked(h_ref)
    exchange.own_in(h_ref, out_ref)
    exchange.arrive_in(out_ref)


def edges_3_kernel(group, list_ref, sums_ref, x_ref, inv_ref, w_self_ref, w_neigh_ref, bias_ref, w_twice_ref,
                   own_hbm, rec_hbm, mean_ref, h_ref, y_ref, out_ref, *scratch):
    exchange = Exchange(group, list_ref, own_hbm, rec_hbm, *scratch, back=False)

    def step(i, carry):
        at = rows_at(i)
        mean, h = layer_step(sums_ref[at, :], x_ref[at, :], inv_ref[at, :], w_self_ref[...], w_neigh_ref[...],
                             bias_ref[...])
        mean_ref[at, :], h_ref[at, :] = mean, h
        y_ref[at, :] = split_halves(dot_t(h, w_twice_ref[...]))
        return carry

    over_rows(x_ref.shape[0], step)
    exchange.send_picked(y_ref)
    exchange.own_in(y_ref, out_ref)
    exchange.arrive_in(out_ref)


def back_3_kernel(classes, group, list_ref, sums_ref, h_ref, inv_ref, w_self_ref, bias_ref, label_ref, mask_ref,
                  count_ref, own_hbm, rec_hbm, d_ref, weighted_ref, g_self_ref, small_ref, out_ref, *scratch):
    exchange = Exchange(group, list_ref, own_hbm, rec_hbm, *scratch, back=True)
    lane = lax.broadcasted_iota(jnp.int32, (ROWS, LANES), 1)

    def step(i, carry):
        loss, d_bias = carry
        at = rows_at(i)
        inv = inv_ref[at, :]
        logits = dot_t(h_ref[at, :], w_self_ref[...]) + join_halves(sums_ref[at, :]) * inv + bias_ref[...]
        logits = jnp.where(lane < classes, logits, -1e30)
        shifted = logits - jnp.max(logits, axis=1, keepdims=True)
        log_prob = shifted - jnp.log(jnp.sum(jnp.exp(shifted), axis=1, keepdims=True))
        is_label = lane == label_ref[at, :]
        picked = jnp.sum(jnp.where(is_label, log_prob, 0.0), axis=1, keepdims=True)
        loss = loss + jnp.sum(mask_ref[at, :] * -picked, axis=0, keepdims=True)
        d = (jnp.exp(log_prob) - is_label.astype(F32)) * mask_ref[at, :] / count_ref[...]
        d_bf = d.astype(BF16)
        d_ref[at, :] = d_bf
        weighted_ref[at, :] = split_halves(join_halves(d_bf.astype(F32) * inv))
        return loss, d_bias + jnp.sum(d, axis=0, keepdims=True)

    loss, d_bias = over_rows(h_ref.shape[0], step, (jnp.zeros((1, 1), F32), jnp.zeros((1, LANES), F32)))
    small_ref[0:1, :] = d_bias
    small_ref[1:2, :] = jnp.broadcast_to(loss / count_ref[...], (1, LANES))
    small_ref[2:, :] = jnp.zeros((small_ref.shape[0] - 2, LANES), F32)
    exchange.send_spread(weighted_ref)
    exchange.own_back(weighted_ref, out_ref)
    g_self_ref[...] = t_dot(d_ref[...], h_ref[...])
    exchange.arrive_back(out_ref)


def back_2_kernel(group, list_ref, sums_ref, d_next_ref, h_ref, inv_ref, x_ref, mean_ref, w_self_next_ref,
                  w_neigh_next_ref, w_neigh_ref, own_hbm, rec_hbm, d_ref, weighted_ref, g_neigh_next_ref, g_self_ref,
                  g_neigh_ref, d_bias_ref, out_ref, projected_ref, *scratch):
    exchange = Exchange(group, list_ref, own_hbm, rec_hbm, *scratch, back=True)
    lane = lax.broadcasted_iota(jnp.int32, (ROWS, LANES), 1)

    def step(i, d_bias):
        at = rows_at(i)
        projected = jnp.where(lane < HALF, join_halves(sums_ref[at, :]), 0.0).astype(BF16)
        projected_ref[at, :] = projected
        d = dot(d_next_ref[at, :], w_self_next_ref[...]) + dot(projected, w_neigh_next_ref[...])
        d = jnp.where(h_ref[at, :].astype(F32) > 0, d, 0.0)
        d_bf = d.astype(BF16)
        d_ref[at, :] = d_bf
        weighted_ref[at, :] = (dot_t(d_bf, w_neigh_ref[...]) * inv_ref[at, :]).astype(BF16)
        return d_bias + jnp.sum(d, axis=0, keepdims=True)

    d_bias_ref[0:1, :] = over_rows(h_ref.shape[0], step, jnp.zeros((1, h_ref.shape[1]), F32))
    d_bias_ref[1:, :] = jnp.zeros((d_bias_ref.shape[0] - 1, h_ref.shape[1]), F32)
    exchange.send_spread(weighted_ref)
    exchange.own_back(weighted_ref, out_ref)
    g_neigh_next_ref[...] = t_dot(projected_ref[...], h_ref[...])
    g_self_ref[...] = t_dot(x_ref[...], d_ref[...])
    g_neigh_ref[...] = t_dot(mean_ref[...], d_ref[...])
    exchange.arrive_back(out_ref)


def exchange_call(body, which, name, lists, arrays, adj_own, adj_rec, outs, width, more_scratch=()):
    group = lists.shape[0]
    n_rows = adj_own.shape[0]
    planes = group // PLANE
    vmem, anywhere = pl.BlockSpec(memory_space=pltpu.VMEM), pl.BlockSpec(memory_space=pl.ANY)
    box = pltpu.VMEM((group, LANES, width), BF16)
    return pl.pallas_call(
        body,
        in_specs=[vmem] * (1 + len(arrays)) + [anywhere] * 2, out_specs=[vmem] * len(outs),
        out_shape=[jax.ShapeDtypeStruct(shape, dtype) for shape, dtype in outs],
        scratch_shapes=list(more_scratch) + [
            box, box, pltpu.VMEM(adj_own.shape, BF16),
            pltpu.VMEM((planes, n_rows, adj_rec.shape[1] // planes), BF16),
            pltpu.SemaphoreType.DMA((group,)), pltpu.SemaphoreType.DMA((group,)),
            pltpu.SemaphoreType.DMA((planes + 1,))],
        compiler_params=pltpu.CompilerParams(collective_id=which, has_side_effects=True, vmem_limit_bytes=VMEM_BYTES),
        cost_estimate=pl.CostEstimate(flops=2 * 2 * n_rows * adj_rec.shape[1] * width, bytes_accessed=30 * 10**6,
                                      transcendentals=0),
        name=name,
    )(lists, *arrays, adj_own, adj_rec)


def add_up_kernel(n_chips, rows, classes, sums_ref, d_next_ref, h_ref, x_ref, mean_ref, w_self_next_ref, g_self_2_ref,
                  g_neigh_2_ref, g_self_3_ref, g_neigh_3_ref, d_bias_2_ref, small_ref, out_ref, d_ref, packed,
                  partner_half, mine, inbox, total, gathered, send, recv):
    me = lax.axis_index(GROUP_AXIS)
    core, chip = lax.rem(me, 2), lax.div(me, 2)
    partner = me + 1 - 2 * core

    def twin(step):
        return 2 * lax.rem(chip + step, n_chips) + core

    barrier = pltpu.get_barrier_semaphore()
    pl.semaphore_signal(barrier, inc=1, device_id=(partner,), device_id_type=MESH)
    for step in range(1, n_chips):
        pl.semaphore_signal(barrier, inc=1, device_id=(twin(step),), device_id_type=MESH)

    def row_step(i, d_bias):
        at = rows_at(i)
        d = dot_t(d_next_ref[at, :], w_self_next_ref[...]) + sums_ref[at, :]
        d = jnp.where(h_ref[at, :].astype(F32) > 0, d, 0.0)
        d_ref[at, :] = d.astype(BF16)
        return d_bias + jnp.sum(d, axis=0, keepdims=True)

    d_bias_1 = over_rows(h_ref.shape[0], row_step, jnp.zeros((1, h_ref.shape[1]), F32))
    at = 0
    for value in (t_dot(x_ref[...], d_ref[...]), t_dot(mean_ref[...], d_ref[...]), g_self_2_ref[...],
                  g_neigh_2_ref[...], g_self_3_ref[:classes, :], g_neigh_3_ref[:classes, :], d_bias_1,
                  d_bias_2_ref[0:1, :], small_ref[0:2, :]):
        count, width = value.shape
        for j in range(width // LANES):
            packed[at:at + count, :] = value[:, j * LANES:(j + 1) * LANES]
            at += count
    packed[at:, :] = jnp.zeros((packed.shape[0] - at, LANES), F32)
    half = n_chips * rows

    def half_of(which):
        return pl.ds(pl.multiple_of(which * half, 8), half)

    def copy(src, dst, slot, device):
        return pltpu.make_async_remote_copy(
            src_ref=src, dst_ref=dst, send_sem=send.at[slot], recv_sem=recv.at[slot],
            device_id=(device,), device_id_type=MESH)

    pl.semaphore_wait(barrier, n_chips)
    first = copy(packed.at[half_of(1 - core)], partner_half, 0, partner)
    first.start()
    first.wait()
    mine[...] = (packed[half_of(core), :] + partner_half[...]).reshape(n_chips, rows, LANES)
    sends = []
    for step in range(1, n_chips):
        sends.append(copy(mine.at[lax.rem(chip + step, n_chips)], inbox.at[step], step, twin(step)))
        sends[-1].start()
    value = mine[chip]
    for step in range(1, n_chips):
        sends[step - 1].wait_recv()
        value = value + inbox[step]
    total[...] = value
    for item in sends:
        item.wait_send()
    spread = []
    for step in range(1, n_chips):
        spread.append(copy(total, gathered.at[core, chip], n_chips + step, twin(step)))
        spread[-1].start()
    gathered[core, chip] = value
    for item in spread:
        item.wait()
    last = copy(gathered.at[core], gathered.at[core], 2 * n_chips, partner)
    last.start()
    last.wait()
    out_ref[...] = gathered[...].reshape(2 * half, LANES)


def add_up(parts, group, classes):
    n_chips = group // 2
    n_rows, hidden = parts[0].shape
    x_width = parts[3].shape[1]
    used = (2 * x_width + 2 * hidden + 2 * classes + 2) * hidden // LANES + 2
    rows = -(-used // (group * 8)) * 8
    total = group * rows
    chunk = (rows, LANES)
    return pl.pallas_call(
        functools.partial(add_up_kernel, n_chips, rows, classes),
        in_specs=[pl.BlockSpec(memory_space=pltpu.VMEM)] * len(parts),
        out_specs=pl.BlockSpec(memory_space=pltpu.VMEM),
        out_shape=jax.ShapeDtypeStruct((total, LANES), F32),
        scratch_shapes=[pltpu.VMEM((n_rows, hidden), BF16),
                        pltpu.VMEM((total, LANES), F32), pltpu.VMEM((total // 2, LANES), F32),
                        pltpu.VMEM((n_chips,) + chunk, F32), pltpu.VMEM((n_chips,) + chunk, F32),
                        pltpu.VMEM(chunk, F32), pltpu.VMEM((2, n_chips) + chunk, F32),
                        pltpu.SemaphoreType.DMA((2 * n_chips + 1,)), pltpu.SemaphoreType.DMA((2 * n_chips + 1,))],
        compiler_params=pltpu.CompilerParams(collective_id=0, has_side_effects=True, vmem_limit_bytes=VMEM_BYTES),
        name='add_up',
    )(*parts)


def unpack_kernel(packed_ref, *out_refs):
    at = 0
    for ref in out_refs[:-1]:
        count, width = ref.shape
        pieces = []
        for j in range(width // LANES):
            pieces.append(packed_ref[at:at + count, :])
            at += count
        ref[...] = jnp.concatenate(pieces, axis=1)
    out_refs[-1][...] = packed_ref[at:at + out_refs[-1].shape[0], :]


def unpack(packed, shapes):
    return pl.pallas_call(
        unpack_kernel,
        in_specs=[pl.BlockSpec(memory_space=pltpu.VMEM)],
        out_specs=[pl.BlockSpec(memory_space=pltpu.VMEM)] * (len(shapes) + 1),
        out_shape=[jax.ShapeDtypeStruct(shape, F32) for shape in shapes + ((8, LANES),)],
        name='unpack',
    )(packed)


def before(count):
    index = jnp.arange(count, dtype=jnp.int32)
    return index[:, None] < index[None, :]


def rank_in_row(flags):
    tri = before(flags.shape[1]).astype(BF16)
    return jnp.dot(flags.astype(BF16), tri, preferred_element_type=F32).astype(jnp.int32)


def exchange_plan(send_idx, src_idx, train_mask, n_own):
    group, slots = send_idx.shape
    halo = src_idx - n_own
    peer, slot = halo // slots, halo % slots
    from_peer = ((halo >= 0)[:, None] & (peer[:, None] == jnp.arange(group, dtype=jnp.int32)[None, :])).astype(BF16)
    at_slot = (slot[:, None] == jnp.arange(slots, dtype=jnp.int32)[None, :]).astype(BF16)
    needed = jnp.einsum('eg,es->gs', from_peer, at_slot, preferred_element_type=F32) > 0
    rank = rank_in_row(needed)
    my_rounds = (jnp.max(jnp.where(needed, rank, 0)) // LANES + 1).astype(jnp.int32)
    upper = rank // LANES * group + jnp.arange(group, dtype=jnp.int32)[:, None]
    split = jnp.concatenate([upper, rank % LANES], axis=1).astype(BF16)
    found = jnp.dot(from_peer, split, preferred_element_type=F32)
    found = jnp.sum((found[:, :slots] * LANES + found[:, slots:]) * at_slot.astype(F32), axis=1).astype(jnp.int32)
    columns = jnp.where(halo >= 0, n_own + found, src_idx)
    my_count = jnp.sum(train_mask).astype(jnp.int32)
    extras = jnp.where(jnp.arange(LANES) == 0, my_rounds, my_count)
    message = jnp.concatenate([jnp.where(needed, rank, -1), jnp.broadcast_to(extras, (group, LANES))], axis=1)
    message = lax.all_to_all(message, GROUP_AXIS, 0, 0, tiled=True)
    asked, rounds = message[:, :slots], jnp.max(message[:, slots])
    count = jnp.sum(message[:, slots + 1]).astype(F32)

    def list_of(part):
        k = part * LANES + jnp.arange(LANES, dtype=jnp.int32)
        chosen = asked[:, None, :] == k[None, :, None]
        return jnp.sum(jnp.where(chosen, send_idx[:, None, :] + 1, 0), axis=2) - 1

    return columns, rounds, count, list_of


def solution(mesh):
    def device_step(features, labels, train_mask, send_idx, src_idx, dst_idx, inv_deg,
                    w_self_1, w_neigh_1, bias_1, w_self_2, w_neigh_2, bias_2,
                    w_self_3, w_neigh_3, bias_3):
        n_own, n_in = features.shape
        hidden = w_self_1.shape[1]
        classes = w_self_3.shape[1]
        group = send_idx.shape[0]
        n_recv = group * LANES
        columns, rounds, count, list_of = exchange_plan(send_idx, src_idx, train_mask, n_own)
        lists = list_of(0)
        starts = jnp.sum(dst_idx[None, :] < (jnp.arange(n_own // DST_TILE + 1) * DST_TILE)[:, None],
                         axis=1, dtype=jnp.int32)

        def adjacency_of(part):
            return adjacency(part, starts, dst_idx, columns, n_own, n_recv)

        adj_own, adj_rec = adjacency_of(0)

        def trade(rows):
            return lax.all_to_all(rows, GROUP_AXIS, 0, 0, tiled=True)

        def rest_in(rows, total):
            def more(part, total):
                received = trade(pick(list_of(part), rows))
                return gather_in(adjacency_of(part)[1], received.reshape(n_recv, -1), total)

            return lax.fori_loop(1, rounds, more, total)

        def rest_back(rows, total):
            def more(part, total):
                returned = trade(spread_out(adjacency_of(part)[1], rows).reshape(group, LANES, -1))
                return put_back(list_of(part), returned, total)

            return lax.fori_loop(1, rounds, more, total)

        def call(body, which, arrays, outs, width, more_scratch=()):
            return exchange_call(functools.partial(body, group), which, body.__name__, lists, arrays,
                                 adj_own, adj_rec, outs, width, more_scratch)

        inv = inv_deg.reshape(-1, 1)
        w_self_t, w_neigh_t = w_self_3.T, w_neigh_3.T
        to_half = jnp.pad(w_neigh_t, ((0, HALF - classes), (0, 0)))
        w_twice = jnp.concatenate([to_half, to_half], axis=0)
        w_self_t, w_neigh_t = (jnp.pad(w, ((0, LANES - classes), (0, 0))) for w in (w_self_t, w_neigh_t))
        bias_row = jnp.pad(bias_3, (0, LANES - classes)).reshape(1, -1)
        rows_f32 = lambda width: ((n_own, width), F32)
        rows_bf16 = lambda width: ((n_own, width), BF16)
        square = ((hidden, hidden), F32)
        tall = ((LANES, hidden), F32)

        sums_1, = call(edges_1_kernel, 1, (features,), [rows_f32(n_in)], n_in)
        sums_1 = rest_in(features, sums_1)
        mean_1, hidden_1, sums_2 = call(
            edges_2_kernel, 2, (sums_1, features, inv, w_self_1, w_neigh_1, bias_1.reshape(1, -1)),
            [rows_bf16(n_in), rows_bf16(hidden), rows_f32(hidden)], hidden)
        sums_2 = rest_in(hidden_1, sums_2)
        mean_2, hidden_2, projected, sums_3 = call(
            edges_3_kernel, 3, (sums_2, hidden_1, inv, w_self_2, w_neigh_2, bias_2.reshape(1, -1), w_twice),
            [rows_bf16(hidden), rows_bf16(hidden), rows_bf16(LANES), rows_f32(LANES)], LANES)
        sums_3 = rest_in(projected, sums_3)
        d_3, weighted_3, g_self_3, small, back_3 = exchange_call(
            functools.partial(back_3_kernel, classes, group), 4, 'back_3', lists,
            (sums_3, hidden_2, inv, w_self_t, bias_row, labels.reshape(-1, 1), train_mask.reshape(-1, 1),
             count.reshape(1, 1)),
            adj_own, adj_rec, [rows_bf16(LANES), rows_bf16(LANES), tall, ((8, LANES), F32), rows_f32(LANES)], LANES)
        back_3 = rest_back(weighted_3, back_3)
        d_2, weighted_2, g_neigh_3, g_self_2, g_neigh_2, d_bias_2, back_2 = call(
            back_2_kernel, 5, (back_3, d_3, hidden_2, inv, hidden_1, mean_2, w_self_t, w_neigh_t, w_neigh_2),
            [rows_bf16(hidden), rows_bf16(hidden), tall, square, square, ((8, hidden), F32), rows_f32(hidden)], hidden,
            (pltpu.VMEM((n_own, LANES), BF16),))
        back_2 = rest_back(weighted_2, back_2)
        summed = add_up((back_2, d_2, hidden_1, features, mean_1, w_self_2, g_self_2, g_neigh_2, g_self_3, g_neigh_3,
                         d_bias_2, small), group, classes)
        gs_1, gn_1, gs_2, gn_2, gs_3, gn_3, small = unpack(
            summed, ((n_in, hidden), (n_in, hidden), (hidden, hidden), (hidden, hidden), (classes, hidden),
                     (classes, hidden)))
        small = small.reshape(-1)
        return (small[2 * hidden + LANES], gs_1, gn_1, small[:hidden], gs_2, gn_2, small[hidden:2 * hidden],
                gs_3.T, gn_3.T, small[2 * hidden:2 * hidden + classes])

    sharded = P(GROUP_AXIS)
    whole = P()
    return jax.shard_map(device_step, mesh=mesh,
                         in_specs=(sharded,) * 7 + (whole,) * 9,
                         out_specs=(whole,) * 10, check_vma=False)
```

```python
import functools

import jax
import jax.numpy as jnp
from jax import lax
from jax.experimental import pallas as pl
from jax.experimental.pallas import tpu as pltpu
from jax.sharding import PartitionSpec as P

GROUP_AXIS = 'gp'
LANES = 128
HALF = 64
DST_TILE = 256
WINDOW = 8
COLS = 1024
BATCH = 8
PLANE = 8
ROWS = 512
COUNT_ROW = 13
VMEM_BYTES = 60 * 1024 * 1024
MESH = pl.DeviceIdType.MESH
F32 = jnp.float32
IDX = jnp.int16
BF16 = jnp.bfloat16


def as_columns(row):
    return jnp.broadcast_to(row, (LANES, LANES)).T


def adjacency_kernel(n_own, starts, parts, dst_ref, col_ref, own_ref, rec_ref):
    part, tile = parts[0], pl.program_id(0)
    first = lax.div(starts[tile], LANES)
    last = lax.div(starts[tile + 1] + LANES - 1, LANES)
    n_recv = rec_ref.shape[1]
    dst_iota = lax.broadcasted_iota(jnp.int32, (DST_TILE, LANES), 0) + tile * DST_TILE
    lanes = lax.broadcasted_iota(jnp.int32, (WINDOW * LANES, LANES), 1).astype(IDX)

    def window_step(w, add):
        rows = first + w * WINDOW
        dst = dst_ref[pl.ds(rows, WINDOW), :]
        col = col_ref[pl.ds(rows, WINDOW), :]
        mine = (col >= n_own + part * n_recv) & (col < n_own + (part + 1) * n_recv)
        col = jnp.where(col < n_own, col, jnp.where(mine, col - part * n_recv, -1))
        to_dst = jnp.concatenate([(dst_iota == dst[k:k + 1, :]).astype(BF16) for k in range(WINDOW)], axis=1)
        columns = jnp.concatenate([as_columns(col[k:k + 1, :]) for k in range(WINDOW)], axis=0).astype(IDX)

        def fill(out_ref, base):
            def block_step(b, carry):
                offset = b * COLS
                shifted = columns - (base + offset).astype(IDX)
                for c in range(0, COLS, 2 * LANES):
                    hot = jnp.concatenate([jnp.where(shifted == lanes + IDX(c + j * LANES), BF16(1), BF16(0))
                                           for j in range(2)], axis=1)
                    counts = jnp.dot(to_dst, hot, preferred_element_type=F32)
                    at = (slice(None), pl.ds(pl.multiple_of(offset + c, 2 * LANES), 2 * LANES))
                    if add:
                        counts = counts + out_ref[at].astype(F32)
                    out_ref[at] = counts.astype(BF16)
                return carry

            lax.fori_loop(0, out_ref.shape[1] // COLS, block_step, 0)

        fill(own_ref, 0)
        fill(rec_ref, n_own)

    window_step(0, False)

    def more(w, carry):
        window_step(w, True)
        return carry

    lax.fori_loop(1, lax.div(last - first + WINDOW - 1, WINDOW), more, 0)


def adjacency(part, starts, dst_rows, col_rows, n_own, n_recv):
    rows = dst_rows.shape[0]
    grid_spec = pltpu.PrefetchScalarGridSpec(
        num_scalar_prefetch=2, grid=(n_own // DST_TILE,),
        in_specs=[pl.BlockSpec((rows, LANES), lambda i, *_: (0, 0))] * 2,
        out_specs=[pl.BlockSpec((DST_TILE, n_own), lambda i, *_: (i, 0)),
                   pl.BlockSpec((DST_TILE, n_recv), lambda i, *_: (i, 0))])
    return pl.pallas_call(
        functools.partial(adjacency_kernel, n_own), grid_spec=grid_spec,
        out_shape=[jax.ShapeDtypeStruct((n_own, n_own), BF16), jax.ShapeDtypeStruct((n_own, n_recv), BF16)],
        compiler_params=pltpu.CompilerParams(vmem_limit_bytes=VMEM_BYTES),
        cost_estimate=pl.CostEstimate(flops=30 * 10**9, bytes_accessed=40 * 10**6, transcendentals=0),
        name='adjacency',
    )(starts, jnp.reshape(part, (1,)).astype(jnp.int32), dst_rows, col_rows)


def pick_kernel(list_ref, rows_ref, out_ref):
    n_rows = rows_ref.shape[0]
    lane_iota = lax.broadcasted_iota(jnp.int32, (LANES, LANES), 1)

    def hot(row):
        columns = as_columns(row)
        return jnp.concatenate(
            [(columns == lane_iota + j * LANES).astype(BF16) for j in range(n_rows // LANES)], axis=1)

    all_hot = jnp.concatenate([hot(list_ref[b:b + 1, :]) for b in range(BATCH)], axis=0)
    picked = jnp.dot(all_hot, rows_ref[...], preferred_element_type=F32).astype(BF16)
    for b in range(BATCH):
        out_ref[b] = picked[b * LANES:(b + 1) * LANES]


def pick(lists, rows):
    group, _ = lists.shape
    n_rows, width = rows.shape
    return pl.pallas_call(
        pick_kernel, grid=(group // BATCH,),
        in_specs=[pl.BlockSpec((BATCH, LANES), lambda i: (i, 0)),
                  pl.BlockSpec((n_rows, width), lambda i: (0, 0))],
        out_specs=pl.BlockSpec((BATCH, LANES, width), lambda i: (i, 0, 0)),
        out_shape=jax.ShapeDtypeStruct((group, LANES, width), BF16),
        compiler_params=pltpu.CompilerParams(vmem_limit_bytes=VMEM_BYTES),
        cost_estimate=pl.CostEstimate(flops=2 * group * LANES * n_rows * width, bytes_accessed=4 * 10**6,
                                      transcendentals=0),
        name='pick',
    )(lists, rows)


def put_back_kernel(list_ref, sent_ref, add_ref, out_ref):
    n_rows = out_ref.shape[0]
    row_iota = lax.broadcasted_iota(jnp.int32, (n_rows, LANES), 0)

    @pl.when(pl.program_id(0) == 0)
    def _():
        out_ref[...] = add_ref[...]

    hot = jnp.concatenate([(row_iota == list_ref[b:b + 1, :]).astype(BF16) for b in range(BATCH)], axis=1)
    rows = jnp.concatenate([sent_ref[b] for b in range(BATCH)], axis=0)
    out_ref[...] += jnp.dot(hot, rows, preferred_element_type=F32)


def put_back(lists, sent, add):
    group, _ = lists.shape
    n_rows, width = add.shape
    return pl.pallas_call(
        put_back_kernel, grid=(group // BATCH,),
        in_specs=[pl.BlockSpec((BATCH, LANES), lambda i: (i, 0)),
                  pl.BlockSpec((BATCH, LANES, width), lambda i: (i, 0, 0)),
                  pl.BlockSpec((n_rows, width), lambda i: (0, 0))],
        out_specs=pl.BlockSpec((n_rows, width), lambda i: (0, 0)),
        out_shape=jax.ShapeDtypeStruct((n_rows, width), F32),
        compiler_params=pltpu.CompilerParams(vmem_limit_bytes=VMEM_BYTES),
        cost_estimate=pl.CostEstimate(flops=2 * group * LANES * n_rows * width, bytes_accessed=8 * 10**6,
                                      transcendentals=0),
        name='put_back',
    )(lists, sent, add)


def gather_in_kernel(adj_ref, rows_ref, add_ref, out_ref):
    out_ref[...] = add_ref[...] + jnp.dot(adj_ref[...], rows_ref[...], preferred_element_type=F32)


def gather_in(adj_rec, rows, add):
    n_own, n_recv = adj_rec.shape
    width = rows.shape[1]
    return pl.pallas_call(
        gather_in_kernel, grid=(n_own // DST_TILE,),
        in_specs=[pl.BlockSpec((DST_TILE, n_recv), lambda i: (i, 0)),
                  pl.BlockSpec((n_recv, width), lambda i: (0, 0)),
                  pl.BlockSpec((DST_TILE, width), lambda i: (i, 0))],
        out_specs=pl.BlockSpec((DST_TILE, width), lambda i: (i, 0)),
        out_shape=jax.ShapeDtypeStruct((n_own, width), F32),
        compiler_params=pltpu.CompilerParams(vmem_limit_bytes=VMEM_BYTES),
        cost_estimate=pl.CostEstimate(flops=2 * n_own * n_recv * width, bytes_accessed=20 * 10**6, transcendentals=0),
        name='gather_in',
    )(adj_rec, rows, add)


def spread_out_kernel(adj_ref, rows_ref, out_ref):
    out_ref[...] = lax.dot_general(adj_ref[...], rows_ref[...], (((0,), (0,)), ((), ())),
                                   preferred_element_type=F32).astype(BF16)


def spread_out(adj_rec, rows):
    n_own, n_recv = adj_rec.shape
    width = rows.shape[1]
    return pl.pallas_call(
        spread_out_kernel, grid=(n_recv // 512,),
        in_specs=[pl.BlockSpec((n_own, 512), lambda i: (0, i)),
                  pl.BlockSpec((n_own, width), lambda i: (0, 0))],
        out_specs=pl.BlockSpec((512, width), lambda i: (i, 0)),
        out_shape=jax.ShapeDtypeStruct((n_recv, width), BF16),
        compiler_params=pltpu.CompilerParams(vmem_limit_bytes=VMEM_BYTES),
        cost_estimate=pl.CostEstimate(flops=2 * n_own * n_recv * width, bytes_accessed=20 * 10**6, transcendentals=0),
        name='spread_out',
    )(adj_rec, rows)


def plane_order(me):
    z = lax.div(me, PLANE)
    near, far, mirror = z + 1 - 2 * lax.rem(z, 2), lax.rem(z + 2, 4), 3 - z
    inner = lax.div(lax.rem(z, 3) + 1, 2)
    sending = [inner * far + (1 - inner) * near, inner * mirror + (1 - inner) * far,
               inner * near + (1 - inner) * mirror, z]
    return sending, [z, near, far, mirror]


def meet_all(barrier, me, group):
    def signal(step, carry):
        pl.semaphore_signal(barrier, inc=1, device_id=(lax.rem(me + step, group),), device_id_type=MESH)
        return carry

    lax.fori_loop(1, group, signal, 0)


class Swap:
    def __init__(self, me, outbox, inbox, send, recv):
        self.me, self.outbox, self.inbox, self.send, self.recv = me, outbox, inbox, send, recv

    def copy(self, peer, slot):
        return pltpu.make_async_remote_copy(
            src_ref=self.outbox.at[peer], dst_ref=self.inbox.at[slot], send_sem=self.send.at[peer],
            recv_sem=self.recv.at[slot], device_id=(peer,), device_id_type=MESH)

    def others(self, plane, own):
        if own:
            return [plane * PLANE + lax.rem(self.me + step, PLANE) for step in range(1, PLANE)]
        return [plane * PLANE + step for step in range(PLANE)]

    def send_plane(self, plane, own):
        for peer in self.others(plane, own):
            self.copy(peer, self.me).start()
        if own:
            self.inbox[self.me] = self.outbox[self.me]

    def receive_plane(self, plane, own):
        for peer in self.others(plane, own):
            self.copy(peer, peer).wait_recv()
        block = self.inbox[pl.ds(plane * PLANE, PLANE)]
        return block.reshape(block.shape[0] * block.shape[1], block.shape[2])

    def finish(self, planes):
        for k, plane in enumerate(planes):
            for peer in self.others(plane, k == len(planes) - 1):
                self.copy(peer, self.me).wait_send()


def rows_at(i):
    return pl.ds(pl.multiple_of(i * ROWS, ROWS), ROWS)


def over_rows(n_rows, step, carry=0):
    return lax.fori_loop(0, n_rows // ROWS, step, carry)


def dot(a, b):
    return jnp.dot(a, b, preferred_element_type=F32)


def dot_t(a, b):
    return lax.dot_general(a, b, (((1,), (1,)), ((), ())), preferred_element_type=F32)


def t_dot(a, b):
    return lax.dot_general(a, b, (((0,), (0,)), ((), ())), preferred_element_type=F32)


def split_halves(twice):
    high = twice.astype(BF16)
    low = (twice - high.astype(F32)).astype(BF16)
    return jnp.where(lax.broadcasted_iota(jnp.int32, twice.shape, 1) < HALF, high, low)


def join_halves(x):
    return x + pltpu.roll(x, HALF, 1)


class Exchange:
    def __init__(self, group, list_ref, own_hbm, rec_hbm, outbox, inbox, own_ref, rec_ref, send, recv, sems, back):
        self.me = lax.axis_index(GROUP_AXIS)
        self.group, self.list_ref, self.own_ref, self.rec_ref, self.outbox = group, list_ref, own_ref, rec_ref, outbox
        self.planes, self.arriving = plane_order(self.me)
        self.barrier = pltpu.get_barrier_semaphore()
        meet_all(self.barrier, self.me, group)
        order = self.planes if back else self.arriving
        span = rec_ref.shape[2]
        self.own_copy = pltpu.make_async_copy(own_hbm, own_ref, sems.at[len(order)])
        self.rec_copies = [
            pltpu.make_async_copy(rec_hbm.at[:, pl.ds(pl.multiple_of(plane * span, span), span)], rec_ref.at[k],
                                  sems.at[k]) for k, plane in enumerate(order)]
        for item in self.rec_copies + [self.own_copy] if back else [self.own_copy] + self.rec_copies:
            item.start()
        self.swap = Swap(self.me, outbox, inbox, send, recv)

    def fill(self, k, plane, rows):
        self.outbox[pl.ds(plane * PLANE, PLANE)] = rows.astype(BF16).reshape(PLANE, LANES, rows.shape[1])
        if k == 0:
            pl.semaphore_wait(self.barrier, self.group - 1)
        self.swap.send_plane(plane, k == len(self.planes) - 1)

    def send_picked(self, rows_ref):
        n_rows = rows_ref.shape[0]
        lanes = lax.broadcasted_iota(jnp.int32, (LANES, LANES), 1).astype(IDX)
        for k, plane in enumerate(self.planes):
            hot = []
            for b in range(PLANE):
                columns = as_columns(self.list_ref[pl.ds(plane * PLANE + b, 1), :]).astype(IDX)
                hot.append(jnp.concatenate([jnp.where(columns == lanes + IDX(j * LANES), BF16(1), BF16(0))
                                            for j in range(n_rows // LANES)], axis=1))
            self.fill(k, plane, dot(jnp.concatenate(hot, axis=0), rows_ref[...]))

    def send_spread(self, grad_ref):
        for k, plane in enumerate(self.planes):
            self.rec_copies[k].wait()
            self.fill(k, plane, t_dot(self.rec_ref[k], grad_ref[...]))

    def own_in(self, rows_ref, out_ref):
        self.own_copy.wait()

        def step(i, carry):
            out_ref[rows_at(i), :] = dot(self.own_ref[rows_at(i), :], rows_ref[...])
            return carry

        over_rows(out_ref.shape[0], step)

    def own_back(self, grad_ref, out_ref):
        self.own_copy.wait()

        def step(i, carry):
            out_ref[rows_at(i), :] = t_dot(self.own_ref[:, rows_at(i)], grad_ref[...])
            return carry

        over_rows(out_ref.shape[0], step)

    def arrive_in(self, out_ref):
        for k, plane in enumerate(self.arriving):
            self.rec_copies[k].wait()
            block = self.swap.receive_plane(plane, k == 0)

            def step(i, carry):
                out_ref[rows_at(i), :] += dot(self.rec_ref[k, rows_at(i), :], block)
                return carry

            over_rows(out_ref.shape[0], step)
        self.swap.finish(self.planes)

    def arrive_back(self, out_ref):
        row_iota = lax.broadcasted_iota(jnp.int32, (ROWS, LANES), 0)
        for k, plane in enumerate(self.arriving):
            block = self.swap.receive_plane(plane, k == 0)
            names = self.list_ref[pl.ds(pl.multiple_of(plane * PLANE, PLANE), PLANE), :]

            def step(i, carry):
                rows = (row_iota + i * ROWS).astype(IDX)
                hot = jnp.concatenate(
                    [jnp.where(rows == jnp.broadcast_to(names[b:b + 1, :], (ROWS, LANES)).astype(IDX),
                               BF16(1), BF16(0)) for b in range(PLANE)], axis=1)
                out_ref[rows_at(i), :] += dot(hot, block)
                return carry

            over_rows(out_ref.shape[0], step)
        self.swap.finish(self.planes)


def first_kernel(group, starts_ref, src_ref, dst_ref, send_ref, mask_ref, x_ref,
                 list_ref, heard_ref, stats_ref, col_ref, got_ref, out_ref, own_hbm, rec_hbm,
                 uses, ask, heard, outbox, inbox, own_ref, rec_ref, ask_send, ask_recv, send, recv, sems):
    n_own = x_ref.shape[0]
    slots = send_ref.shape[1] * LANES
    n_planes, _, span = rec_ref.shape
    me = lax.axis_index(GROUP_AXIS)
    planes, arriving = plane_order(me)
    barrier = pltpu.get_barrier_semaphore()
    meet_all(barrier, me, group)
    step_edges = WINDOW * LANES
    chunks = src_ref.shape[0] // WINDOW - 1
    peer_iota = lax.broadcasted_iota(jnp.int32, (group, step_edges), 0)
    slot_iota = lax.broadcasted_iota(jnp.int32, (slots, step_edges), 0).astype(IDX)

    def in_line(rows):
        return jnp.concatenate([rows[k:k + 1, :] for k in range(WINDOW)], axis=1)

    def hot_pair(c):
        rows = src_ref[pl.ds(pl.multiple_of(c * WINDOW, WINDOW), WINDOW), :]
        halo = in_line(rows) - n_own
        peer = lax.div(halo + slots, slots) - 1
        slot = jnp.broadcast_to(halo - peer * slots, (slots, step_edges)).astype(IDX)
        by_peer = jnp.where(peer_iota == peer, BF16(1), BF16(0))
        by_slot = slot_iota == slot
        return rows, halo, by_peer, by_slot

    uses[...] = jnp.zeros_like(uses)

    def use_step(c, carry):
        _, _, by_peer, by_slot = hot_pair(c)
        uses[...] += dot_t(by_peer, jnp.where(by_slot, BF16(1), BF16(0)))
        return carry

    lax.fori_loop(0, chunks, use_step, 0)
    needed = uses[...] > 0
    tri = lax.broadcasted_iota(jnp.int32, (slots, slots), 0) < lax.broadcasted_iota(jnp.int32, (slots, slots), 1)
    rank = dot(jnp.where(needed, 1.0, 0.0).astype(BF16), jnp.where(tri, 1.0, 0.0).astype(BF16)).astype(jnp.int32)
    part = lax.div(rank, LANES)
    wanted = jnp.where(needed, rank, -1)
    rounds = jnp.max(jnp.max(jnp.where(needed, part, 0).astype(F32), axis=1, keepdims=True), axis=0, keepdims=True) + 1
    count = jnp.sum(jnp.sum(mask_ref[...], axis=1, keepdims=True), axis=0, keepdims=True)
    extras = [jnp.broadcast_to(v, (1, LANES)).astype(jnp.int32) for v in (rounds, count)]
    quarter = slots // LANES
    tail = jnp.concatenate(extras + [jnp.zeros((8 - quarter - 2, LANES), jnp.int32)], axis=0)
    for p in range(group):
        lines = [wanted[p:p + 1, r * LANES:(r + 1) * LANES] for r in range(quarter)]
        ask[p] = jnp.concatenate(lines + [tail], axis=0)
    pl.semaphore_wait(barrier, group - 1)

    def ask_copy(peer, slot):
        return pltpu.make_async_remote_copy(
            src_ref=ask.at[peer], dst_ref=heard.at[slot], send_sem=ask_send.at[peer], recv_sem=ask_recv.at[slot],
            device_id=(peer,), device_id_type=MESH)

    for step in range(1, group):
        ask_copy(lax.rem(me + step, group), me).start()
    heard[me] = ask[me]

    upper = (part * group + lax.broadcasted_iota(jnp.int32, rank.shape, 0)).astype(F32).astype(BF16)
    lower = (rank - part * LANES).astype(F32).astype(BF16)

    def column_step(c, carry):
        rows, halo, by_peer, by_slot = hot_pair(c)
        place = t_dot(upper, by_peer) * LANES + t_dot(lower, by_peer)
        found = jnp.sum(jnp.where(by_slot, place, 0.0), axis=0, keepdims=True).astype(jnp.int32)
        found = jnp.where(halo >= 0, found + n_own, halo + n_own)
        col_ref[pl.ds(pl.multiple_of(c * WINDOW, WINDOW), WINDOW), :] = jnp.concatenate(
            [found[:, k * LANES:(k + 1) * LANES] for k in range(WINDOW)], axis=0)
        return carry

    lax.fori_loop(0, chunks, column_step, 0)
    col_ref[chunks * WINDOW:, :] = jnp.full((WINDOW, LANES), -1, jnp.int32)

    for step in range(1, group):
        peer = lax.rem(me + step, group)
        ask_copy(peer, peer).wait_recv()
    most, total = heard[0], heard[0]
    for p in range(1, group):
        most, total = jnp.maximum(most, heard[p]), total + heard[p]
    stats_ref[...] = jnp.concatenate([most, total], axis=0)
    heard_ref[...] = heard[...]

    swap = Swap(me, outbox, inbox, send, recv)
    places = lax.broadcasted_iota(jnp.int32, (LANES, LANES), 0)
    lanes = lax.broadcasted_iota(jnp.int32, (LANES, LANES), 1).astype(IDX)
    for k, plane in enumerate(planes):
        hot, names = [], []
        for b in range(PLANE):
            asked, rows = heard[plane * PLANE + b], send_ref[plane * PLANE + b]
            named = jnp.zeros((LANES, LANES), jnp.int32)
            for r in range(quarter):
                named = named + jnp.where(asked[r:r + 1, :] == places, rows[r:r + 1, :] + 1, 0)
            named = jnp.broadcast_to(jnp.sum(named.astype(F32), axis=1, keepdims=True) - 1, (LANES, LANES))
            names.append(named.T[0:1, :].astype(jnp.int32))
            columns = named.astype(jnp.int32).astype(IDX)
            hot.append(jnp.concatenate([jnp.where(columns == lanes + IDX(j * LANES), BF16(1), BF16(0))
                                        for j in range(n_own // LANES)], axis=1))
        list_ref[pl.ds(pl.multiple_of(plane * PLANE, PLANE), PLANE), :] = jnp.concatenate(names, axis=0)
        picked = dot(jnp.concatenate(hot, axis=0), x_ref[...]).astype(BF16)
        outbox[pl.ds(plane * PLANE, PLANE)] = picked.reshape(PLANE, LANES, picked.shape[1])
        swap.send_plane(plane, k == n_planes - 1)

    dst_iota = lax.broadcasted_iota(jnp.int32, (DST_TILE, LANES), 0)
    edge_lanes = lax.broadcasted_iota(jnp.int32, (step_edges, LANES), 1).astype(IDX)

    def own_out(tile):
        at = pl.ds(pl.multiple_of(tile * DST_TILE, DST_TILE), DST_TILE)
        return pltpu.make_async_copy(own_ref.at[at], own_hbm.at[at], sems.at[n_planes, tile])

    def rec_out(tile, p):
        at = pl.ds(pl.multiple_of(tile * DST_TILE, DST_TILE), DST_TILE)
        return pltpu.make_async_copy(rec_ref.at[p, at], rec_hbm.at[at, pl.ds(p * span, span)], sems.at[p, tile])

    def tile_step(tile, carry):
        first = lax.div(starts_ref[tile], LANES)
        dst = dst_ref[pl.ds(first, WINDOW), :]
        col = col_ref[pl.ds(first, WINDOW), :]
        at = pl.ds(pl.multiple_of(tile * DST_TILE, DST_TILE), DST_TILE)
        to_dst = jnp.concatenate([(dst_iota + tile * DST_TILE == dst[k:k + 1, :]).astype(BF16)
                                  for k in range(WINDOW)], axis=1)
        columns = jnp.concatenate([as_columns(col[k:k + 1, :]) for k in range(WINDOW)], axis=0).astype(IDX)

        def counts(base, c):
            hot = jnp.concatenate([jnp.where(columns - base == edge_lanes + IDX(c + j * LANES), BF16(1), BF16(0))
                                   for j in range(2)], axis=1)
            return dot(to_dst, hot).astype(BF16)

        def own_step(b, carry):
            for c in range(0, span, 2 * LANES):
                own_ref[at, pl.ds(pl.multiple_of(b * span + c, 2 * LANES), 2 * LANES)] = counts(
                    (b * span).astype(IDX), c)
            return carry

        def rec_step(p, carry):
            for c in range(0, span, 2 * LANES):
                rec_ref[p, at, c:c + 2 * LANES] = counts((n_own + p * span).astype(IDX), c)
            return carry

        lax.fori_loop(0, n_own // span, own_step, 0)
        own_out(tile).start()
        lax.fori_loop(0, n_planes, rec_step, 0)
        for p in range(n_planes):
            rec_out(tile, p).start()
        return carry

    tiles = n_own // DST_TILE
    lax.fori_loop(0, tiles, tile_step, 0)

    def own_sum(i, carry):
        out_ref[rows_at(i), :] = dot(own_ref[rows_at(i), :], x_ref[...])
        return carry

    over_rows(n_own, own_sum)
    for k, plane in enumerate(arriving):
        block = swap.receive_plane(plane, k == 0)

        def rec_sum(i, carry):
            out_ref[rows_at(i), :] += dot(rec_ref[plane, rows_at(i), :], block)
            return carry

        over_rows(n_own, rec_sum)
    got_ref[...] = inbox[...]
    swap.finish(planes)
    for step in range(1, group):
        ask_copy(lax.rem(me + step, group), me).wait_send()

    def drain(tile, carry):
        own_out(tile).wait()
        for p in range(n_planes):
            rec_out(tile, p).wait()
        return carry

    lax.fori_loop(0, tiles, drain, 0)


def edge_rows(index):
    return jnp.concatenate([index, jnp.full((WINDOW * LANES,), -1, jnp.int32)]).reshape(-1, LANES)


def first_exchange(starts, src_idx, dst_idx, send_idx, train_mask, x):
    group, slots = send_idx.shape
    n_own, width = x.shape
    n_recv = group * LANES
    planes = group // PLANE
    src, dst = edge_rows(src_idx), edge_rows(dst_idx)
    vmem, anywhere = pl.BlockSpec(memory_space=pltpu.VMEM), pl.BlockSpec(memory_space=pl.ANY)
    box = pltpu.VMEM((group, LANES, width), BF16)
    note = pltpu.VMEM((group, 8, LANES), jnp.int32)
    signals = pltpu.SemaphoreType.DMA((group,))
    shape = jax.ShapeDtypeStruct
    return pl.pallas_call(
        functools.partial(first_kernel, group),
        in_specs=[pl.BlockSpec(memory_space=pltpu.SMEM)] + [vmem] * 5, out_specs=[vmem] * 6 + [anywhere] * 2,
        out_shape=[shape((group, LANES), jnp.int32), shape((group, 8, LANES), jnp.int32), shape((16, LANES), jnp.int32),
                   shape(src.shape, jnp.int32), shape((group, LANES, width), BF16), shape((n_own, width), F32),
                   shape((n_own, n_own), BF16), shape((n_own, n_recv), BF16)],
        scratch_shapes=[pltpu.VMEM((group, slots), F32), note, note, box, box, pltpu.VMEM((n_own, n_own), BF16),
                        pltpu.VMEM((planes, n_own, n_recv // planes), BF16), signals, signals, signals, signals,
                        pltpu.SemaphoreType.DMA((planes + 1, n_own // DST_TILE))],
        compiler_params=pltpu.CompilerParams(collective_id=1, has_side_effects=True, vmem_limit_bytes=VMEM_BYTES),
        cost_estimate=pl.CostEstimate(flops=40 * 10**9, bytes_accessed=30 * 10**6, transcendentals=0),
        name='first',
    )(starts, src, dst, send_idx.reshape(group, slots // LANES, LANES), train_mask.reshape(-1, LANES), x)


def layer_step(sums, x, inv, w_self, w_neigh, bias):
    mean = (sums * inv).astype(BF16)
    pre_act = dot(x, w_self) + dot(mean, w_neigh) + bias
    return mean, jnp.maximum(pre_act, 0.0).astype(BF16)


def edges_2_kernel(group, list_ref, sums_ref, x_ref, inv_ref, w_self_ref, w_neigh_ref, bias_ref, own_hbm, rec_hbm,
                   mean_ref, h_ref, out_ref, *scratch):
    exchange = Exchange(group, list_ref, own_hbm, rec_hbm, *scratch, back=False)

    def step(i, carry):
        at = rows_at(i)
        mean_ref[at, :], h_ref[at, :] = layer_step(sums_ref[at, :], x_ref[at, :], inv_ref[at, :], w_self_ref[...],
                                                   w_neigh_ref[...], bias_ref[...])
        return carry

    over_rows(x_ref.shape[0], step)
    exchange.send_picked(h_ref)
    exchange.own_in(h_ref, out_ref)
    exchange.arrive_in(out_ref)


def edges_3_kernel(group, list_ref, sums_ref, x_ref, inv_ref, w_self_ref, w_neigh_ref, bias_ref, w_twice_ref,
                   own_hbm, rec_hbm, mean_ref, h_ref, y_ref, out_ref, *scratch):
    exchange = Exchange(group, list_ref, own_hbm, rec_hbm, *scratch, back=False)

    def step(i, carry):
        at = rows_at(i)
        mean, h = layer_step(sums_ref[at, :], x_ref[at, :], inv_ref[at, :], w_self_ref[...], w_neigh_ref[...],
                             bias_ref[...])
        mean_ref[at, :], h_ref[at, :] = mean, h
        y_ref[at, :] = split_halves(dot_t(h, w_twice_ref[...]))
        return carry

    over_rows(x_ref.shape[0], step)
    exchange.send_picked(y_ref)
    exchange.own_in(y_ref, out_ref)
    exchange.arrive_in(out_ref)


def back_3_kernel(classes, group, list_ref, sums_ref, h_ref, inv_ref, w_self_ref, bias_ref, label_ref, mask_ref,
                  stats_ref, own_hbm, rec_hbm, d_ref, weighted_ref, g_self_ref, small_ref, out_ref, *scratch):
    exchange = Exchange(group, list_ref, own_hbm, rec_hbm, *scratch, back=True)
    lane = lax.broadcasted_iota(jnp.int32, (ROWS, LANES), 1)
    count = stats_ref[COUNT_ROW:COUNT_ROW + 1, :].astype(F32)

    def step(i, carry):
        loss, d_bias = carry
        at = rows_at(i)
        inv = inv_ref[at, :]
        logits = dot_t(h_ref[at, :], w_self_ref[...]) + join_halves(sums_ref[at, :]) * inv + bias_ref[...]
        logits = jnp.where(lane < classes, logits, -1e30)
        shifted = logits - jnp.max(logits, axis=1, keepdims=True)
        log_prob = shifted - jnp.log(jnp.sum(jnp.exp(shifted), axis=1, keepdims=True))
        is_label = lane == label_ref[at, :]
        picked = jnp.sum(jnp.where(is_label, log_prob, 0.0), axis=1, keepdims=True)
        loss = loss + jnp.sum(mask_ref[at, :] * -picked, axis=0, keepdims=True)
        d = (jnp.exp(log_prob) - is_label.astype(F32)) * mask_ref[at, :] / count
        d_bf = d.astype(BF16)
        d_ref[at, :] = d_bf
        weighted_ref[at, :] = split_halves(join_halves(d_bf.astype(F32) * inv))
        return loss, d_bias + jnp.sum(d, axis=0, keepdims=True)

    loss, d_bias = over_rows(h_ref.shape[0], step, (jnp.zeros((1, 1), F32), jnp.zeros((1, LANES), F32)))
    small_ref[0:1, :] = d_bias
    small_ref[1:2, :] = jnp.broadcast_to(loss, (1, LANES)) / count
    small_ref[2:, :] = jnp.zeros((small_ref.shape[0] - 2, LANES), F32)
    exchange.send_spread(weighted_ref)
    exchange.own_back(weighted_ref, out_ref)
    g_self_ref[...] = t_dot(d_ref[...], h_ref[...])
    exchange.arrive_back(out_ref)


def back_2_kernel(group, list_ref, sums_ref, d_next_ref, h_ref, inv_ref, x_ref, mean_ref, w_self_next_ref,
                  w_neigh_next_ref, w_neigh_ref, own_hbm, rec_hbm, d_ref, weighted_ref, g_neigh_next_ref, g_self_ref,
                  g_neigh_ref, d_bias_ref, out_ref, projected_ref, *scratch):
    exchange = Exchange(group, list_ref, own_hbm, rec_hbm, *scratch, back=True)
    lane = lax.broadcasted_iota(jnp.int32, (ROWS, LANES), 1)

    def step(i, d_bias):
        at = rows_at(i)
        projected = jnp.where(lane < HALF, join_halves(sums_ref[at, :]), 0.0).astype(BF16)
        projected_ref[at, :] = projected
        d = dot(d_next_ref[at, :], w_self_next_ref[...]) + dot(projected, w_neigh_next_ref[...])
        d = jnp.where(h_ref[at, :].astype(F32) > 0, d, 0.0)
        d_bf = d.astype(BF16)
        d_ref[at, :] = d_bf
        weighted_ref[at, :] = (dot_t(d_bf, w_neigh_ref[...]) * inv_ref[at, :]).astype(BF16)
        return d_bias + jnp.sum(d, axis=0, keepdims=True)

    d_bias_ref[0:1, :] = over_rows(h_ref.shape[0], step, jnp.zeros((1, h_ref.shape[1]), F32))
    d_bias_ref[1:, :] = jnp.zeros((d_bias_ref.shape[0] - 1, h_ref.shape[1]), F32)
    exchange.send_spread(weighted_ref)
    exchange.own_back(weighted_ref, out_ref)
    g_neigh_next_ref[...] = t_dot(projected_ref[...], h_ref[...])
    g_self_ref[...] = t_dot(x_ref[...], d_ref[...])
    g_neigh_ref[...] = t_dot(mean_ref[...], d_ref[...])
    exchange.arrive_back(out_ref)


def exchange_call(body, which, name, lists, arrays, adj_own, adj_rec, outs, width, more_scratch=()):
    group = lists.shape[0]
    n_rows = adj_own.shape[0]
    planes = group // PLANE
    vmem, anywhere = pl.BlockSpec(memory_space=pltpu.VMEM), pl.BlockSpec(memory_space=pl.ANY)
    box = pltpu.VMEM((group, LANES, width), BF16)
    return pl.pallas_call(
        body,
        in_specs=[vmem] * (1 + len(arrays)) + [anywhere] * 2, out_specs=[vmem] * len(outs),
        out_shape=[jax.ShapeDtypeStruct(shape, dtype) for shape, dtype in outs],
        scratch_shapes=list(more_scratch) + [
            box, box, pltpu.VMEM(adj_own.shape, BF16),
            pltpu.VMEM((planes, n_rows, adj_rec.shape[1] // planes), BF16),
            pltpu.SemaphoreType.DMA((group,)), pltpu.SemaphoreType.DMA((group,)),
            pltpu.SemaphoreType.DMA((planes + 1,))],
        compiler_params=pltpu.CompilerParams(collective_id=which, has_side_effects=True, vmem_limit_bytes=VMEM_BYTES),
        cost_estimate=pl.CostEstimate(flops=2 * 2 * n_rows * adj_rec.shape[1] * width, bytes_accessed=30 * 10**6,
                                      transcendentals=0),
        name=name,
    )(lists, *arrays, adj_own, adj_rec)


def add_up_kernel(n_chips, rows, classes, sums_ref, d_next_ref, h_ref, x_ref, mean_ref, w_self_next_ref, g_self_2_ref,
                  g_neigh_2_ref, g_self_3_ref, g_neigh_3_ref, d_bias_2_ref, small_ref, out_ref, d_ref, packed,
                  partner_half, mine, inbox, total, gathered, send, recv):
    me = lax.axis_index(GROUP_AXIS)
    core, chip = lax.rem(me, 2), lax.div(me, 2)
    partner = me + 1 - 2 * core

    def twin(step):
        return 2 * lax.rem(chip + step, n_chips) + core

    barrier = pltpu.get_barrier_semaphore()
    pl.semaphore_signal(barrier, inc=1, device_id=(partner,), device_id_type=MESH)
    for step in range(1, n_chips):
        pl.semaphore_signal(barrier, inc=1, device_id=(twin(step),), device_id_type=MESH)

    def row_step(i, d_bias):
        at = rows_at(i)
        d = dot_t(d_next_ref[at, :], w_self_next_ref[...]) + sums_ref[at, :]
        d = jnp.where(h_ref[at, :].astype(F32) > 0, d, 0.0)
        d_ref[at, :] = d.astype(BF16)
        return d_bias + jnp.sum(d, axis=0, keepdims=True)

    d_bias_1 = over_rows(h_ref.shape[0], row_step, jnp.zeros((1, h_ref.shape[1]), F32))
    at = 0
    for value in (t_dot(x_ref[...], d_ref[...]), t_dot(mean_ref[...], d_ref[...]), g_self_2_ref[...],
                  g_neigh_2_ref[...], g_self_3_ref[:classes, :], g_neigh_3_ref[:classes, :], d_bias_1,
                  d_bias_2_ref[0:1, :], small_ref[0:2, :]):
        count, width = value.shape
        for j in range(width // LANES):
            packed[at:at + count, :] = value[:, j * LANES:(j + 1) * LANES]
            at += count
    packed[at:, :] = jnp.zeros((packed.shape[0] - at, LANES), F32)
    half = n_chips * rows

    def half_of(which):
        return pl.ds(pl.multiple_of(which * half, 8), half)

    def copy(src, dst, slot, device):
        return pltpu.make_async_remote_copy(
            src_ref=src, dst_ref=dst, send_sem=send.at[slot], recv_sem=recv.at[slot],
            device_id=(device,), device_id_type=MESH)

    pl.semaphore_wait(barrier, n_chips)
    first = copy(packed.at[half_of(1 - core)], partner_half, 0, partner)
    first.start()
    first.wait()
    mine[...] = (packed[half_of(core), :] + partner_half[...]).reshape(n_chips, rows, LANES)
    sends = []
    for step in range(1, n_chips):
        sends.append(copy(mine.at[lax.rem(chip + step, n_chips)], inbox.at[step], step, twin(step)))
        sends[-1].start()
    value = mine[chip]
    for step in range(1, n_chips):
        sends[step - 1].wait_recv()
        value = value + inbox[step]
    total[...] = value
    for item in sends:
        item.wait_send()
    spread = []
    for step in range(1, n_chips):
        spread.append(copy(total, gathered.at[core, chip], n_chips + step, twin(step)))
        spread[-1].start()
    gathered[core, chip] = value
    for item in spread:
        item.wait()
    last = copy(gathered.at[core], gathered.at[core], 2 * n_chips, partner)
    last.start()
    last.wait()
    out_ref[...] = gathered[...].reshape(2 * half, LANES)


def add_up(parts, group, classes):
    n_chips = group // 2
    n_rows, hidden = parts[0].shape
    x_width = parts[3].shape[1]
    used = (2 * x_width + 2 * hidden + 2 * classes + 2) * hidden // LANES + 2
    rows = -(-used // (group * 8)) * 8
    total = group * rows
    chunk = (rows, LANES)
    return pl.pallas_call(
        functools.partial(add_up_kernel, n_chips, rows, classes),
        in_specs=[pl.BlockSpec(memory_space=pltpu.VMEM)] * len(parts),
        out_specs=pl.BlockSpec(memory_space=pltpu.VMEM),
        out_shape=jax.ShapeDtypeStruct((total, LANES), F32),
        scratch_shapes=[pltpu.VMEM((n_rows, hidden), BF16),
                        pltpu.VMEM((total, LANES), F32), pltpu.VMEM((total // 2, LANES), F32),
                        pltpu.VMEM((n_chips,) + chunk, F32), pltpu.VMEM((n_chips,) + chunk, F32),
                        pltpu.VMEM(chunk, F32), pltpu.VMEM((2, n_chips) + chunk, F32),
                        pltpu.SemaphoreType.DMA((2 * n_chips + 1,)), pltpu.SemaphoreType.DMA((2 * n_chips + 1,))],
        compiler_params=pltpu.CompilerParams(collective_id=0, has_side_effects=True, vmem_limit_bytes=VMEM_BYTES),
        name='add_up',
    )(*parts)


def unpack_kernel(packed_ref, *out_refs):
    at = 0
    for ref in out_refs[:-1]:
        count, width = ref.shape
        pieces = []
        for j in range(width // LANES):
            pieces.append(packed_ref[at:at + count, :])
            at += count
        ref[...] = jnp.concatenate(pieces, axis=1)
    out_refs[-1][...] = packed_ref[at:at + out_refs[-1].shape[0], :]


def unpack(packed, shapes):
    return pl.pallas_call(
        unpack_kernel,
        in_specs=[pl.BlockSpec(memory_space=pltpu.VMEM)],
        out_specs=[pl.BlockSpec(memory_space=pltpu.VMEM)] * (len(shapes) + 1),
        out_shape=[jax.ShapeDtypeStruct(shape, F32) for shape in shapes + ((8, LANES),)],
        name='unpack',
    )(packed)


def solution(mesh):
    def device_step(features, labels, train_mask, send_idx, src_idx, dst_idx, inv_deg,
                    w_self_1, w_neigh_1, bias_1, w_self_2, w_neigh_2, bias_2,
                    w_self_3, w_neigh_3, bias_3):
        n_own, n_in = features.shape
        hidden = w_self_1.shape[1]
        classes = w_self_3.shape[1]
        group = send_idx.shape[0]
        n_recv = group * LANES
        starts = jnp.sum(dst_idx[None, :] < (jnp.arange(n_own // DST_TILE + 1) * DST_TILE)[:, None],
                         axis=1, dtype=jnp.int32)
        lists, heard, stats, columns, received_1, sums_1, adj_own, adj_rec = first_exchange(
            starts, src_idx, dst_idx, send_idx, train_mask, features)
        quarter = send_idx.shape[1] // LANES
        rounds = stats[quarter, 0]

        def list_of(part):
            asked = heard[:, :quarter].reshape(send_idx.shape)
            k = part * LANES + jnp.arange(LANES, dtype=jnp.int32)
            chosen = asked[:, None, :] == k[None, :, None]
            return jnp.sum(jnp.where(chosen, send_idx[:, None, :] + 1, 0), axis=2) - 1

        def adjacency_of(part):
            return adjacency(part, starts, edge_rows(dst_idx), columns, n_own, n_recv)

        def count_again(_, carry):
            own, rec = adjacency_of(0)
            own_sums = jnp.dot(own, features, preferred_element_type=F32)
            return own, rec, gather_in(rec, received_1.reshape(n_recv, -1), own_sums)

        spans = (starts[1:] + LANES - 1) // LANES - starts[:-1] // LANES
        outside = (jnp.max(spans) > WINDOW).astype(jnp.int32)
        adj_own, adj_rec, sums_1 = lax.fori_loop(0, outside, count_again, (adj_own, adj_rec, sums_1))

        def trade(rows):
            return lax.all_to_all(rows, GROUP_AXIS, 0, 0, tiled=True)

        def rest_in(rows, total):
            def more(part, total):
                received = trade(pick(list_of(part), rows))
                return gather_in(adjacency_of(part)[1], received.reshape(n_recv, -1), total)

            return lax.fori_loop(1, rounds, more, total)

        def rest_back(rows, total):
            def more(part, total):
                returned = trade(spread_out(adjacency_of(part)[1], rows).reshape(group, LANES, -1))
                return put_back(list_of(part), returned, total)

            return lax.fori_loop(1, rounds, more, total)

        def call(body, which, arrays, outs, width, more_scratch=()):
            return exchange_call(functools.partial(body, group), which, body.__name__, lists, arrays,
                                 adj_own, adj_rec, outs, width, more_scratch)

        inv = inv_deg.reshape(-1, 1)
        w_self_t, w_neigh_t = w_self_3.T, w_neigh_3.T
        to_half = jnp.pad(w_neigh_t, ((0, HALF - classes), (0, 0)))
        w_twice = jnp.concatenate([to_half, to_half], axis=0)
        w_self_t, w_neigh_t = (jnp.pad(w, ((0, LANES - classes), (0, 0))) for w in (w_self_t, w_neigh_t))
        bias_row = jnp.pad(bias_3, (0, LANES - classes)).reshape(1, -1)
        rows_f32 = lambda width: ((n_own, width), F32)
        rows_bf16 = lambda width: ((n_own, width), BF16)
        square = ((hidden, hidden), F32)
        tall = ((LANES, hidden), F32)

        sums_1 = rest_in(features, sums_1)
        mean_1, hidden_1, sums_2 = call(
            edges_2_kernel, 2, (sums_1, features, inv, w_self_1, w_neigh_1, bias_1.reshape(1, -1)),
            [rows_bf16(n_in), rows_bf16(hidden), rows_f32(hidden)], hidden)
        sums_2 = rest_in(hidden_1, sums_2)
        mean_2, hidden_2, projected, sums_3 = call(
            edges_3_kernel, 3, (sums_2, hidden_1, inv, w_self_2, w_neigh_2, bias_2.reshape(1, -1), w_twice),
            [rows_bf16(hidden), rows_bf16(hidden), rows_bf16(LANES), rows_f32(LANES)], LANES)
        sums_3 = rest_in(projected, sums_3)
        d_3, weighted_3, g_self_3, small, back_3 = exchange_call(
            functools.partial(back_3_kernel, classes, group), 4, 'back_3', lists,
            (sums_3, hidden_2, inv, w_self_t, bias_row, labels.reshape(-1, 1), train_mask.reshape(-1, 1),
             stats),
            adj_own, adj_rec, [rows_bf16(LANES), rows_bf16(LANES), tall, ((8, LANES), F32), rows_f32(LANES)], LANES)
        back_3 = rest_back(weighted_3, back_3)
        d_2, weighted_2, g_neigh_3, g_self_2, g_neigh_2, d_bias_2, back_2 = call(
            back_2_kernel, 5, (back_3, d_3, hidden_2, inv, hidden_1, mean_2, w_self_t, w_neigh_t, w_neigh_2),
            [rows_bf16(hidden), rows_bf16(hidden), tall, square, square, ((8, hidden), F32), rows_f32(hidden)], hidden,
            (pltpu.VMEM((n_own, LANES), BF16),))
        back_2 = rest_back(weighted_2, back_2)
        summed = add_up((back_2, d_2, hidden_1, features, mean_1, w_self_2, g_self_2, g_neigh_2, g_self_3, g_neigh_3,
                         d_bias_2, small), group, classes)
        gs_1, gn_1, gs_2, gn_2, gs_3, gn_3, small = unpack(
            summed, ((n_in, hidden), (n_in, hidden), (hidden, hidden), (hidden, hidden), (classes, hidden),
                     (classes, hidden)))
        small = small.reshape(-1)
        return (small[2 * hidden + LANES], gs_1, gn_1, small[:hidden], gs_2, gn_2, small[hidden:2 * hidden],
                gs_3.T, gn_3.T, small[2 * hidden:2 * hidden + classes])

    sharded = P(GROUP_AXIS)
    whole = P()
    return jax.shard_map(device_step, mesh=mesh,
                         in_specs=(sharded,) * 7 + (whole,) * 9,
                         out_specs=(whole,) * 10, check_vma=False)
```
